32 devices in a mesh: dp: 2 (over x), ep: 16 (over z, y, core).
Axes of the slice: x: 2, y: 2, z: 4, core: 2. Of those that a mesh axis runs over, the one named last changes fastest.
Arguments:
- x_tokens: bfloat16 [4096, 2048], P(('dp', 'ep')), parts along dimension 0
- dy_tokens: bfloat16 [4096, 2048], P(('dp', 'ep')), parts along dimension 0
- expert_ids: int32 [4096, 10], P(('dp', 'ep')), parts along dimension 0
- gate_vals: float32 [4096, 10], P(('dp', 'ep')), parts along dimension 0
- slot_pos: int32 [4096, 10], P(('dp', 'ep')), parts along dimension 0
- w_gate: bfloat16 [32, 2048, 512], P('ep')
- w_up: bfloat16 [32, 2048, 512], P('ep')
- w_down: bfloat16 [32, 512, 2048], P('ep')
- shared_gate: bfloat16 [2048, 512], replicated
- shared_up: bfloat16 [2048, 512], replicated
- shared_down: bfloat16 [512, 2048], replicated
Outputs:
- output 1: bfloat16 [4096, 2048], P(('dp', 'ep')), parts along dimension 0
- output 2: float32 [64, 2048, 512], P(('dp', 'ep')), parts along dimension 0
- output 3: float32 [64, 2048, 512], P(('dp', 'ep')), parts along dimension 0
- output 4: float32 [64, 512, 2048], P(('dp', 'ep')), parts along dimension 0
- output 5: float32 [32, 2048, 512], P(('dp', 'ep')), parts along dimension 0
- output 6: float32 [32, 2048, 512], P(('dp', 'ep')), parts along dimension 0
- output 7: float32 [32, 512, 2048], P(('dp', 'ep')), parts along dimension 0
There are 2 independent parts. The reference program is written for one: setup_inputs(seed, part) draws one part's arguments, and reference() takes and returns one part's arrays. A program takes and returns all parts, laid end to end along the dimension named above; an argument that names none is the same for every part.
All inputs are finite; a program needn't handle non-finite values.
Results may differ from the reference program's by a relative error of at most 0.0104941.
Values are sent between devices in bfloat16 or wider.
A program may use at most 1 GiB of HBM per device.

```python
import jax
import jax.numpy as jnp
from jax import lax

MODEL_DIM = 2048
EXPERT_FF = 512
SHARED_FF = 512
TOP_K = 10
TOK_DEV = 128
GROUP_SIZE = 16
NUM_EXPERTS = 32
CAPACITY = 60


def draw_routing(route_key):
    bias_key, hot_key, noise_key = jax.random.split(route_key, 3)
    expert_range = jnp.arange(NUM_EXPERTS, dtype=jnp.int32)
    expert_bias = jax.random.randint(bias_key, (NUM_EXPERTS,), 0, 256)
    hot_expert = jax.random.randint(hot_key, (GROUP_SIZE,), 0, NUM_EXPERTS)
    noise = jax.random.randint(noise_key, (GROUP_SIZE, TOK_DEV, NUM_EXPERTS), 0, 1024)
    forced = (jnp.arange(TOK_DEV)[None, :, None] < CAPACITY) & (expert_range[None, None, :] == hot_expert[:, None, None])
    score = (noise + expert_bias[None, None, :] + 4096 * forced.astype(jnp.int32)) * NUM_EXPERTS + expert_range
    choices = lax.top_k(score, TOP_K)[1]

    def source_slots(source_choices):
        flat_choices = source_choices.reshape(-1)
        onehot = (flat_choices[:, None] == expert_range[None, :]).astype(jnp.int32)
        earlier = jnp.cumsum(onehot, axis=0) - onehot
        slot_rank = jnp.sum(earlier * onehot, axis=1)
        return jnp.where(slot_rank < CAPACITY, slot_rank, -1).reshape(TOK_DEV, TOP_K)

    positions = lax.map(source_slots, choices)
    return choices.reshape(-1, TOP_K).astype(jnp.int32), positions.reshape(-1, TOP_K).astype(jnp.int32)


def setup_inputs(seed: int = 0, part: int = 0) -> dict:
    part_key = jax.random.fold_in(jax.random.key(seed), part)
    key_x, key_dy, key_gate, key_route = jax.random.split(part_key, 4)
    weight_keys = jax.random.split(jax.random.key(seed + 1), 6)
    tokens = GROUP_SIZE * TOK_DEV
    x_tokens = jax.random.normal(key_x, (tokens, MODEL_DIM), jnp.float32).astype(jnp.bfloat16)
    dy_tokens = jax.random.normal(key_dy, (tokens, MODEL_DIM), jnp.float32).astype(jnp.bfloat16)
    gate_vals = jax.random.uniform(key_gate, (tokens, TOP_K), jnp.float32, 0.25, 1.0)
    expert_ids, slot_pos = draw_routing(key_route)
    in_scale = MODEL_DIM ** -0.5
    ff_scale = EXPERT_FF ** -0.5
    shared_scale = SHARED_FF ** -0.5
    w_gate = (jax.random.normal(weight_keys[0], (NUM_EXPERTS, MODEL_DIM, EXPERT_FF), jnp.float32) * in_scale).astype(jnp.bfloat16)
    w_up = (jax.random.normal(weight_keys[1], (NUM_EXPERTS, MODEL_DIM, EXPERT_FF), jnp.float32) * in_scale).astype(jnp.bfloat16)
    w_down = (jax.random.normal(weight_keys[2], (NUM_EXPERTS, EXPERT_FF, MODEL_DIM), jnp.float32) * ff_scale).astype(jnp.bfloat16)
    shared_gate = (jax.random.normal(weight_keys[3], (MODEL_DIM, SHARED_FF), jnp.float32) * in_scale).astype(jnp.bfloat16)
    shared_up = (jax.random.normal(weight_keys[4], (MODEL_DIM, SHARED_FF), jnp.float32) * in_scale).astype(jnp.bfloat16)
    shared_down = (jax.random.normal(weight_keys[5], (SHARED_FF, MODEL_DIM), jnp.float32) * shared_scale).astype(jnp.bfloat16)
    return {'x_tokens': x_tokens, 'dy_tokens': dy_tokens, 'expert_ids': expert_ids, 'gate_vals': gate_vals, 'slot_pos': slot_pos, 'w_gate': w_gate, 'w_up': w_up, 'w_down': w_down, 'shared_gate': shared_gate, 'shared_up': shared_up, 'shared_down': shared_down}


def expert_grads(x_rows, dz_rows, gate_w, up_w, down_w):
    act_gate = jnp.dot(x_rows, gate_w, preferred_element_type=jnp.float32).astype(jnp.bfloat16)
    act_up = jnp.dot(x_rows, up_w, preferred_element_type=jnp.float32).astype(jnp.bfloat16)
    gate_f32 = act_gate.astype(jnp.float32)
    up_f32 = act_up.astype(jnp.float32)
    sigma = jax.nn.sigmoid(gate_f32)
    silu_gate = gate_f32 * sigma
    hidden = (silu_gate * up_f32).astype(jnp.bfloat16)
    grad_hidden = jnp.dot(dz_rows, down_w.T, preferred_element_type=jnp.float32)
    grad_gate = (grad_hidden * up_f32 * sigma * (1.0 + gate_f32 * (1.0 - sigma))).astype(jnp.bfloat16)
    grad_up = (grad_hidden * silu_gate).astype(jnp.bfloat16)
    grad_down_w = jnp.dot(hidden.T, dz_rows, preferred_element_type=jnp.float32)
    grad_gate_w = jnp.dot(x_rows.T, grad_gate, preferred_element_type=jnp.float32)
    grad_up_w = jnp.dot(x_rows.T, grad_up, preferred_element_type=jnp.float32)
    grad_rows = jnp.dot(grad_gate, gate_w.T, preferred_element_type=jnp.float32) + jnp.dot(grad_up, up_w.T, preferred_element_type=jnp.float32)
    return grad_rows, grad_gate_w, grad_up_w, grad_down_w


def reference(x_tokens, dy_tokens, expert_ids, gate_vals, slot_pos, w_gate, w_up, w_down, shared_gate, shared_up, shared_down):
    tokens = GROUP_SIZE * TOK_DEV
    slot_rows = GROUP_SIZE * CAPACITY
    total_rows = NUM_EXPERTS * slot_rows
    source = jnp.arange(tokens, dtype=jnp.int32)[:, None] // TOK_DEV
    target = jnp.where(slot_pos >= 0, expert_ids * slot_rows + source * CAPACITY + slot_pos, total_rows).reshape(-1)
    token_index = jnp.broadcast_to(jnp.arange(tokens, dtype=jnp.int32)[:, None], (tokens, TOP_K)).reshape(-1)
    row_token = jnp.full((total_rows + 1,), tokens, jnp.int32).at[target].set(token_index)[:total_rows].reshape(NUM_EXPERTS, slot_rows)
    row_gate = jnp.zeros((total_rows + 1,), jnp.float32).at[target].set(gate_vals.reshape(-1))[:total_rows].reshape(NUM_EXPERTS, slot_rows)

    def expert_step(routed_sum, expert_in):
        token_rows, gate_rows, gate_w, up_w, down_w = expert_in
        x_rows = jnp.take(x_tokens, token_rows, axis=0, mode='fill', fill_value=0)
        dy_rows = jnp.take(dy_tokens, token_rows, axis=0, mode='fill', fill_value=0)
        dz_rows = (dy_rows.astype(jnp.float32) * gate_rows[:, None]).astype(jnp.bfloat16)
        grad_rows, grad_gate_w, grad_up_w, grad_down_w = expert_grads(x_rows, dz_rows, gate_w, up_w, down_w)
        returned = grad_rows.astype(jnp.bfloat16).astype(jnp.float32)
        routed_sum = routed_sum.at[token_rows].add(returned, mode='drop')
        return routed_sum, (grad_gate_w, grad_up_w, grad_down_w)

    routed_sum, expert_w_grads = lax.scan(expert_step, jnp.zeros((tokens, MODEL_DIM), jnp.float32), (row_token, row_gate, w_gate, w_up, w_down))
    grad_w_gate, grad_w_up, grad_w_down = expert_w_grads

    def shared_step(source_in):
        x_rows, dy_rows = source_in
        return expert_grads(x_rows, dy_rows, shared_gate, shared_up, shared_down)

    shared_dx, grad_shared_gate, grad_shared_up, grad_shared_down = lax.map(shared_step, (x_tokens.reshape(GROUP_SIZE, TOK_DEV, MODEL_DIM), dy_tokens.reshape(GROUP_SIZE, TOK_DEV, MODEL_DIM)))
    grad_x = (routed_sum + shared_dx.reshape(tokens, MODEL_DIM)).astype(jnp.bfloat16)
    return (grad_x, grad_w_gate, grad_w_up, grad_w_down, grad_shared_gate, grad_shared_up, grad_shared_down)
```

```python
import jax
import jax.numpy as jnp
from jax import lax
from jax.sharding import PartitionSpec as P

F32 = jnp.float32
BF16 = jnp.bfloat16


def swiglu_parts(act_gate, act_up, grad_hidden):
    gate_f32 = act_gate.astype(F32)
    up_f32 = act_up.astype(F32)
    sigma = jax.nn.sigmoid(gate_f32)
    silu_gate = gate_f32 * sigma
    hidden = (silu_gate * up_f32).astype(BF16)
    grad_gate = (grad_hidden * up_f32 * sigma * (1.0 + gate_f32 * (1.0 - sigma))).astype(BF16)
    grad_up = (grad_hidden * silu_gate).astype(BF16)
    return hidden, grad_gate, grad_up


def dot32(spec, a, b):
    return jnp.einsum(spec, a, b, preferred_element_type=F32)


def shared_backward(x_tokens, dy_tokens, shared_gate, shared_up, shared_down):
    act_gate = dot32('td,df->tf', x_tokens, shared_gate).astype(BF16)
    act_up = dot32('td,df->tf', x_tokens, shared_up).astype(BF16)
    grad_hidden = dot32('td,fd->tf', dy_tokens, shared_down)
    hidden, grad_gate, grad_up = swiglu_parts(act_gate, act_up, grad_hidden)
    grad_gate_w = dot32('td,tf->df', x_tokens, grad_gate)
    grad_up_w = dot32('td,tf->df', x_tokens, grad_up)
    grad_down_w = dot32('tf,td->fd', hidden, dy_tokens)
    grad_input = dot32('tf,df->td', grad_gate, shared_gate) + dot32('tf,df->td', grad_up, shared_up)
    return grad_input, grad_gate_w, grad_up_w, grad_down_w


def solution(mesh):
    group = mesh.shape['ep']
    token_spec = P(('dp', 'ep'), None)
    expert_spec = P('ep', None, None)
    whole_spec = P(None, None)
    grad_spec = P(('dp', 'ep'), None, None)

    def local_backward(x_tokens, dy_tokens, expert_ids, gate_vals, slot_pos, w_gate, w_up, w_down, shared_gate, shared_up, shared_down):
        tok_count, top_k = expert_ids.shape
        local_experts, model_dim, expert_ff = w_gate.shape
        num_experts = local_experts * group
        capacity = (3 * tok_count * top_k + 2 * num_experts - 1) // (2 * num_experts)
        rows = (capacity + 15) // 16 * 16
        meta = jnp.concatenate([expert_ids.astype(F32), slot_pos.astype(F32), gate_vals], axis=1).T
        x_all = lax.all_gather(x_tokens, 'ep')
        dy_all = lax.all_gather(dy_tokens, 'ep')
        meta_all = lax.all_gather(meta, 'ep')
        ids_all, slot_all, gate_all = meta_all[:, :top_k], meta_all[:, top_k:2 * top_k], meta_all[:, 2 * top_k:]
        first = (lax.axis_index('ep') * local_experts).astype(F32)
        mine = first + jnp.arange(local_experts, dtype=F32)
        hit = (ids_all[:, None] == mine[None, :, None, None]) & (slot_all[:, None] >= 0)
        tok_slot = jnp.sum(jnp.where(hit, slot_all[:, None] + 1.0, 0.0), axis=2) - 1.0
        tok_gate = jnp.sum(jnp.where(hit, gate_all[:, None], 0.0), axis=2)
        pick = tok_slot[:, :, None, :] == jnp.arange(rows, dtype=F32)[None, None, :, None]
        row_gate = jnp.sum(jnp.where(pick, tok_gate[:, :, None, :], 0.0), axis=3)
        pick = pick.astype(BF16)
        x_exp = dot32('sert,std->esrd', pick, x_all).astype(BF16).reshape(local_experts, group * rows, model_dim)
        dz_exp = (dot32('sert,std->esrd', pick, dy_all) * row_gate.transpose(1, 0, 2)[..., None]).astype(BF16).reshape(local_experts, group * rows, model_dim)
        act_gate = dot32('erd,edf->erf', x_exp, w_gate).astype(BF16)
        act_up = dot32('erd,edf->erf', x_exp, w_up).astype(BF16)
        grad_hidden = dot32('erd,efd->erf', dz_exp, w_down)
        hidden, grad_gate, grad_up = swiglu_parts(act_gate, act_up, grad_hidden)
        grad_exp = (dot32('erf,edf->erd', grad_gate, w_gate) + dot32('erf,edf->erd', grad_up, w_up)).astype(BF16)
        partial = dot32('sert,esrd->std', pick, grad_exp.reshape(local_experts, group, rows, model_dim))
        routed_sum = lax.psum_scatter(partial, 'ep', scatter_dimension=0, tiled=True)[0]
        grad_w_gate = dot32('erd,erf->edf', x_exp, grad_gate)
        grad_w_up = dot32('erd,erf->edf', x_exp, grad_up)
        grad_w_down = dot32('erf,erd->efd', hidden, dz_exp)
        shared_dx, grad_shared_gate, grad_shared_up, grad_shared_down = shared_backward(x_tokens, dy_tokens, shared_gate, shared_up, shared_down)
        grad_x = (routed_sum + shared_dx).astype(BF16)
        return grad_x, grad_w_gate, grad_w_up, grad_w_down, grad_shared_gate[None], grad_shared_up[None], grad_shared_down[None]

    return jax.shard_map(local_backward, mesh=mesh, in_specs=(token_spec, token_spec, token_spec, token_spec, token_spec, expert_spec, expert_spec, expert_spec, whole_spec, whole_spec, whole_spec), out_specs=(token_spec, grad_spec, grad_spec, grad_spec, grad_spec, grad_spec, grad_spec), check_vma=False)
```

```python
import functools

import jax
import jax.numpy as jnp
from jax import lax
from jax.experimental import pallas as pl
from jax.experimental.pallas import tpu as pltpu
from jax.sharding import PartitionSpec as P

F32 = jnp.float32
BF16 = jnp.bfloat16
ANY = pl.BlockSpec(memory_space=pl.ANY)
VMEM = pl.BlockSpec(memory_space=pltpu.VMEM)
VMEM_LIMIT = 67_000_000


def dot_nn(a, b):
    return lax.dot_general(a, b, (((1,), (0,)), ((), ())), preferred_element_type=F32)


def dot_nt(a, b):
    return lax.dot_general(a, b, (((1,), (1,)), ((), ())), preferred_element_type=F32)


def dot_tn(a, b):
    return lax.dot_general(a, b, (((0,), (0,)), ((), ())), preferred_element_type=F32)


def swiglu_parts(act_gate, act_up, grad_hidden):
    gate_f32 = act_gate.astype(F32)
    up_f32 = act_up.astype(F32)
    sigma = jax.nn.sigmoid(gate_f32)
    silu_gate = gate_f32 * sigma
    hidden = (silu_gate * up_f32).astype(BF16)
    grad_gate = (grad_hidden * up_f32 * sigma * (1.0 + gate_f32 * (1.0 - sigma))).astype(BF16)
    grad_up = (grad_hidden * silu_gate).astype(BF16)
    return hidden, grad_gate, grad_up


def routed_kernel(x_in, dy_in, gate_tab, w_gate, w_up, w_down,
                  routed_out, x_all, z_all, act_all, hid_all,
                  xbuf, dybuf, gbuf, w13, w2, act, hst, zst,
                  sums, dsend, pbuf, ybuf, cbuf,
                  load_sem, out_sem, gs_sem, gr_sem, recv_sem, sy_sem, sd_sem, sown_sem, sz_sem,
                  ds_sem, dr_sem, ys_sem, yr_sem, cs_sem, cr_sem, credit):
    tok, dim = x_in.shape
    ff = w2.shape[1]
    me = lax.axis_index('ep')
    z = lax.div(me, 4)
    y = lax.rem(lax.div(me, 2), 2)
    c = lax.rem(me, 2)
    partner = me + 1 - 2 * c
    side = me + 2 - 4 * y
    bufs = (xbuf, dybuf)

    def bid(zz, yy, cc):
        return zz * 4 + yy * 2 + cc

    def order(k):
        near = lax.div(z * (3 - z), 2)
        flip = lax.div(z, 2)
        delta = lax.div((1 - k) * (2 - k) * (3 - k), 6) - lax.div(k * (2 - k) * (3 - k), 2)
        base = k + near * delta
        return base + flip * (3 - 2 * base)

    def visit(t):
        u = t + lax.div(t, 7)
        odd = lax.rem(u, 2)
        first = lax.div(7 - t, 7)
        k = odd * lax.div(u + 1, 2) + (1 - odd) * (lax.div(u, 2) - 1) + first
        col = 1 - odd - first
        return order(k), y + col * (1 - 2 * y), col

    def remote(src, dst, send, recv, dev):
        return pltpu.make_async_remote_copy(src_ref=src, dst_ref=dst, send_sem=send, recv_sem=recv, device_id={'ep': dev}, device_id_type=pl.DeviceIdType.MESH)

    own = [pltpu.make_async_copy(x_in, xbuf.at[me], load_sem.at[0]), pltpu.make_async_copy(dy_in, dybuf.at[me], load_sem.at[1])]
    loads = []
    for e in range(2):
        loads.append(pltpu.make_async_copy(w_gate.at[e], w13.at[e, :, pl.ds(0, ff)], load_sem.at[2 + 3 * e]))
        loads.append(pltpu.make_async_copy(w_up.at[e], w13.at[e, :, pl.ds(ff, ff)], load_sem.at[3 + 3 * e]))
        loads.append(pltpu.make_async_copy(w_down.at[e], w2.at[e], load_sem.at[4 + 3 * e]))
    for cp in own + loads:
        cp.start()

    barrier = pltpu.get_barrier_semaphore()

    @pl.loop(1, 16)
    def _(d):
        pl.semaphore_signal(barrier, inc=1, device_id={'ep': lax.rem(me + d, 16)}, device_id_type=pl.DeviceIdType.MESH)
    pl.semaphore_wait(barrier, 15)

    def send_y(q, zb, b):
        return remote(bufs[q].at[b], bufs[q].at[b], sy_sem.at[q, zb], recv_sem.at[q, b], side)

    def send_d(q, zb, yb, b):
        return remote(bufs[q].at[b], bufs[q].at[b], sd_sem.at[q, zb * 2 + yb], recv_sem.at[q, b], partner)

    def send_own(q, up):
        return remote(bufs[q].at[me], bufs[q].at[me], sown_sem.at[q, up], recv_sem.at[q, me], me + (4 if up else -4))

    def send_fwd(q, zb, b, up):
        return remote(bufs[q].at[b], bufs[q].at[b], sz_sem.at[q, zb], recv_sem.at[q, b], me + (4 if up else -4))

    for q in range(2):
        own[q].wait()
        send_y(q, z, me).start()

        @pl.when(z < 3)
        def _():
            send_own(q, 1).start()

        @pl.when(z > 0)
        def _():
            send_own(q, 0).start()
        send_d(q, z, y, me).start()

    def send_gate(d):
        dest = lax.rem(me + d, 16)
        return remote(gate_tab.at[dest], gbuf.at[me], gs_sem.at[d], gr_sem.at[me], dest)

    @pl.loop(1, 16)
    def _(d):
        send_gate(d).start()
    gbuf[me] = gate_tab[me]

    def arrive(t):
        zb, yb, col = visit(t)
        b = bid(zb, yb, c)
        for q in range(2):
            send_d(q, zb, yb, b).wait_recv()

            @pl.when(col == 0)
            def _():
                send_y(q, zb, b).start()

                @pl.when((zb > z) & (z > 0))
                def _():
                    send_fwd(q, zb, b, 0).start()

                @pl.when((zb < z) & (z < 3))
                def _():
                    send_fwd(q, zb, b, 1).start()
            send_d(q, zb, yb, b).start()

    def flush(t, start):
        zb, yb, _ = visit(t)
        b0 = bid(zb, yb, 0)
        two = pl.ds(b0, 2)
        cps = [pltpu.make_async_copy(xbuf.at[two], x_all.at[two], out_sem.at[0, t]),
               pltpu.make_async_copy(act.at[two], act_all.at[two], out_sem.at[1, t]),
               pltpu.make_async_copy(hst, hid_all.at[two], out_sem.at[2, t]),
               pltpu.make_async_copy(zst.at[0], z_all.at[0, two], out_sem.at[3, t]),
               pltpu.make_async_copy(zst.at[1], z_all.at[1, two], out_sem.at[4, t])]
        for cp in (cps if start else cps[2:]):
            if start:
                cp.start()
            else:
                cp.wait()

    def compute(t):
        zb, yb, _ = visit(t)
        b0 = bid(zb, yb, 0)
        bp = bid(zb, yb, 1 - c)
        for q in range(2):
            send_d(q, zb, yb, bp).wait_recv()
        for p in range(2):
            @pl.when(b0 + p != me)
            def _():
                remote(gate_tab.at[0], gbuf.at[b0 + p], gs_sem.at[0], gr_sem.at[b0 + p], partner).wait_recv()

        @pl.when(t > 0)
        def _():
            flush(t - 1, False)
        two = pl.ds(b0, 2)
        gates = jnp.concatenate([gbuf[b0].T, gbuf[b0 + 1].T], axis=0)
        for e in range(2):
            gate = gates[:, e:e + 1]
            zst[e] = (dybuf[two].reshape(2 * tok, dim).astype(F32) * gate).astype(BF16).reshape(2, tok, dim)
            ab = jnp.where(gate != 0.0, dot_nn(xbuf[two].reshape(2 * tok, dim), w13[e]), 0.0).astype(BF16)
            grad_hidden = dot_nt(zst[e].reshape(2 * tok, dim), w2[e])
            hidden, grad_gate, grad_up = swiglu_parts(ab[:, :ff], ab[:, ff:], grad_hidden)
            hst[:, :, e * ff:(e + 1) * ff] = hidden.reshape(2, tok, ff)
            act[two, :, 2 * e * ff:(2 * e + 1) * ff] = grad_gate.reshape(2, tok, ff)
            act[two, :, (2 * e + 1) * ff:(2 * e + 2) * ff] = grad_up.reshape(2, tok, ff)
        flush(t, True)

    for i, cp in enumerate(loads):
        cp.wait()

    @pl.loop(1, 9)
    def _(t):
        @pl.when(t < 8)
        def _():
            arrive(t)
        compute(t - 1)

    def rs_visit(j):
        half = lax.div(j, 4)
        zb = order(3 - lax.rem(j, 4))
        col = 1 - half
        return zb, y + col * (1 - 2 * y)

    def give(j):
        return remote(dsend.at[lax.rem(j, 2)], pbuf.at[lax.rem(j, 2)], ds_sem.at[lax.rem(j, 2)], dr_sem.at[lax.rem(j, 2)], partner)

    def rs_y(j):
        zb, _ = rs_visit(j)
        return remote(sums.at[j], ybuf.at[zb], ys_sem.at[zb], yr_sem.at[zb], side)

    tile = min(512, dim)

    def rs_compute(j):
        zb, yb = rs_visit(j)
        b = bid(zb, yb, c)
        bp = bid(zb, yb, 1 - c)

        @pl.when(j >= 2)
        def _():
            give(j).wait_send()

        @pl.loop(0, dim // tile)
        def _(n):
            cols = pl.ds(pl.multiple_of(n * tile, tile), tile)
            part = None
            for e in range(2):
                lanes = slice(2 * e * ff, (2 * e + 2) * ff)
                rows = jnp.concatenate([act[b, :, lanes], act[bp, :, lanes]], axis=0)
                r = dot_nt(rows, w13[e, cols, :]).astype(BF16).astype(F32)
                part = r if part is None else part + r
            sums[j, :, cols] = part[:tok]
            dsend[lax.rem(j, 2), :, cols] = part[tok:]

        @pl.when(j >= 2)
        def _():
            pl.semaphore_wait(credit, 1)
        give(j).start()

    def rs_finish(j):
        give(j).wait_recv()
        sums[j] = sums[j] + pbuf[lax.rem(j, 2)]

        @pl.when(j < 6)
        def _():
            pl.semaphore_signal(credit, inc=1, device_id={'ep': partner}, device_id_type=pl.DeviceIdType.MESH)

        @pl.when(j < 4)
        def _():
            rs_y(j).start()

    @pl.loop(0, 9)
    def _(j):
        @pl.when(j < 8)
        def _():
            rs_compute(j)

        @pl.when(j > 0)
        def _():
            rs_finish(j - 1)

    def chain(k, zb, up):
        j = 7 - k
        if up:
            return remote(sums.at[j], cbuf.at[0, zb - z - 1], cs_sem.at[k], cr_sem.at[0, zb - z - 1], me + 4)
        return remote(sums.at[j], cbuf.at[1, z - zb - 1], cs_sem.at[k], cr_sem.at[1, z - zb - 1], me - 4)

    def chain_in(j, up, gap):
        slot = 0 if up else 1
        remote(sums.at[j], cbuf.at[slot, gap], cs_sem.at[0], cr_sem.at[slot, gap], partner).wait_recv()
        sums[j] = sums[j] + cbuf[slot, gap]

    for k in (3, 2, 1, 0):
        zb = order(k)
        j = 7 - k
        remote(sums.at[j], ybuf.at[zb], ys_sem.at[zb], yr_sem.at[zb], side).wait_recv()
        sums[j] = sums[j] + ybuf[zb]
        if k:
            @pl.when(zb > z)
            def _():
                @pl.when(z > 0)
                def _():
                    chain_in(j, True, zb - z)
                chain(k, zb, True).start()

            @pl.when(zb < z)
            def _():
                @pl.when(z < 3)
                def _():
                    chain_in(j, False, z - zb)
                chain(k, zb, False).start()
        else:
            @pl.when(z > 0)
            def _():
                chain_in(7, True, 0)

            @pl.when(z < 3)
            def _():
                chain_in(7, False, 0)
            done = pltpu.make_async_copy(sums.at[7], routed_out, load_sem.at[0])
            done.start()

    done.wait()
    flush(7, False)
    for t in range(8):
        for i, ref in enumerate((xbuf, act)):
            pltpu.make_async_copy(ref.at[pl.ds(0, 2)], (x_all, act_all)[i].at[pl.ds(0, 2)], out_sem.at[i, t]).wait()
    for q in range(2):
        for zb in range(4):
            send_y(q, zb, 0).wait_send()
            for yb in range(2):
                send_d(q, zb, yb, 0).wait_send()

            @pl.when(((zb > z) & (z > 0)) | ((zb < z) & (z < 3)))
            def _():
                send_fwd(q, zb, 0, 1).wait_send()

        @pl.when(z < 3)
        def _():
            send_own(q, 1).wait_send()

        @pl.when(z > 0)
        def _():
            send_own(q, 0).wait_send()

    @pl.loop(1, 16)
    def _(d):
        send_gate(d).wait_send()
    for j in range(2):
        give(j).wait_send()
    for j in range(4):
        remote(sums.at[j], ybuf.at[j], ys_sem.at[j], yr_sem.at[j], side).wait_send()
    for k in range(1, 4):
        remote(sums.at[0], cbuf.at[0, 0], cs_sem.at[k], cr_sem.at[0, 0], partner).wait_send()


def routed(x_tokens, dy_tokens, gate_tab, w_gate, w_up, w_down):
    tok, dim = x_tokens.shape
    ff = w_gate.shape[2]
    dma = pltpu.SemaphoreType.DMA
    flops = 16 * tok * 2 * 2 * dim * ff * 5
    return pl.pallas_call(
        routed_kernel,
        name='routed',
        out_shape=(jax.ShapeDtypeStruct((tok, dim), F32), jax.ShapeDtypeStruct((16, tok, dim), BF16), jax.ShapeDtypeStruct((2, 16, tok, dim), BF16),
                   jax.ShapeDtypeStruct((16, tok, 4 * ff), BF16), jax.ShapeDtypeStruct((16, tok, 2 * ff), BF16)),
        in_specs=[ANY, ANY, VMEM, ANY, ANY, ANY],
        out_specs=(ANY,) * 5,
        scratch_shapes=[
            pltpu.VMEM((16, tok, dim), BF16), pltpu.VMEM((16, tok, dim), BF16), pltpu.VMEM((16, 8, tok), F32),
            pltpu.VMEM((2, dim, 2 * ff), BF16), pltpu.VMEM((2, ff, dim), BF16),
            pltpu.VMEM((16, tok, 4 * ff), BF16), pltpu.VMEM((2, tok, 2 * ff), BF16), pltpu.VMEM((2, 2, tok, dim), BF16),
            pltpu.VMEM((8, tok, dim), F32), pltpu.VMEM((2, tok, dim), F32), pltpu.VMEM((2, tok, dim), F32),
            pltpu.VMEM((4, tok, dim), F32), pltpu.VMEM((2, 3, tok, dim), F32),
            dma((8,)), dma((5, 8)), dma((16,)), dma((16,)), dma((2, 16)), dma((2, 4)), dma((2, 8)), dma((2, 2)), dma((2, 4)),
            dma((2,)), dma((2,)), dma((4,)), dma((4,)), dma((4,)), dma((2, 3)), pltpu.SemaphoreType.REGULAR,
        ],
        compiler_params=pltpu.CompilerParams(collective_id=0, has_side_effects=True, vmem_limit_bytes=VMEM_LIMIT),
        cost_estimate=pl.CostEstimate(flops=flops, bytes_accessed=80_000_000, transcendentals=0),
    )(x_tokens, dy_tokens, gate_tab, w_gate, w_up, w_down)


def shared_kernel(x, dy, w1, w3, w2, dx, g1, g3, g2):
    act_gate = dot_nn(x[...], w1[...]).astype(BF16)
    act_up = dot_nn(x[...], w3[...]).astype(BF16)
    grad_hidden = dot_nt(dy[...], w2[...])
    hidden, grad_gate, grad_up = swiglu_parts(act_gate, act_up, grad_hidden)
    dx[...] = dot_nt(grad_gate, w1[...]) + dot_nt(grad_up, w3[...])
    g1[0] = dot_tn(x[...], grad_gate)
    g3[0] = dot_tn(x[...], grad_up)
    g2[0] = dot_tn(hidden, dy[...])


def shared_backward(x, dy, w1, w3, w2):
    tok, dim = x.shape
    ff = w1.shape[1]
    return pl.pallas_call(
        shared_kernel,
        name='shared',
        out_shape=(jax.ShapeDtypeStruct((tok, dim), F32), jax.ShapeDtypeStruct((1, dim, ff), F32), jax.ShapeDtypeStruct((1, dim, ff), F32), jax.ShapeDtypeStruct((1, ff, dim), F32)),
        in_specs=[VMEM] * 5,
        out_specs=(VMEM,) * 4,
        compiler_params=pltpu.CompilerParams(vmem_limit_bytes=60_000_000),
        cost_estimate=pl.CostEstimate(flops=16 * tok * dim * ff, bytes_accessed=21_000_000, transcendentals=tok * ff),
    )(x, dy, w1, w3, w2)


def up_grad_kernel(x, act, g1, g3):
    ff = act.shape[1] // 2
    both = dot_tn(x[...], act[...])
    g1[0] = both[:, :ff]
    g3[0] = both[:, ff:]


def up_grads(x_all, act_all):
    rows, dim = x_all.shape
    ff = act_all.shape[1] // 4
    tile = min(512, dim)
    out = jax.ShapeDtypeStruct((2, dim, ff), F32)
    return pl.pallas_call(
        up_grad_kernel,
        name='up_grads',
        out_shape=(out, out),
        grid=(dim // tile, 2),
        in_specs=[pl.BlockSpec((rows, tile), lambda i, e: (0, i)), pl.BlockSpec((rows, 2 * ff), lambda i, e: (0, e))],
        out_specs=(pl.BlockSpec((1, tile, ff), lambda i, e: (e, i, 0)), pl.BlockSpec((1, tile, ff), lambda i, e: (e, i, 0))),
        compiler_params=pltpu.CompilerParams(vmem_limit_bytes=60_000_000),
        cost_estimate=pl.CostEstimate(flops=8 * rows * dim * ff, bytes_accessed=50_000_000, transcendentals=0),
    )(x_all, act_all)


def down_grad_kernel(hid, dz, g2):
    g2[0] = dot_tn(hid[...], dz[0])


def down_grads(hid_all, z_all):
    _, rows, dim = z_all.shape
    ff = hid_all.shape[1] // 2
    tile = min(512, dim)
    return pl.pallas_call(
        down_grad_kernel,
        name='down_grads',
        out_shape=jax.ShapeDtypeStruct((2, ff, dim), F32),
        grid=(2, dim // tile),
        in_specs=[pl.BlockSpec((rows, ff), lambda e, n: (0, e)), pl.BlockSpec((1, rows, tile), lambda e, n: (e, 0, n))],
        out_specs=pl.BlockSpec((1, ff, tile), lambda e, n: (e, 0, n)),
        compiler_params=pltpu.CompilerParams(vmem_limit_bytes=60_000_000),
        cost_estimate=pl.CostEstimate(flops=4 * rows * dim * ff, bytes_accessed=30_000_000, transcendentals=0),
    )(hid_all, z_all)


def solution(mesh):
    group = mesh.shape['ep']
    token_spec = P(('dp', 'ep'), None)
    expert_spec = P('ep', None, None)
    whole_spec = P(None, None)
    grad_spec = P(('dp', 'ep'), None, None)

    def local_backward(x_tokens, dy_tokens, expert_ids, gate_vals, slot_pos, w_gate, w_up, w_down, shared_gate, shared_up, shared_down):
        tok, dim = x_tokens.shape
        local_experts = w_gate.shape[0]
        experts = jnp.arange(group * local_experts, dtype=jnp.int32)
        hit = (expert_ids.T[None] == experts[:, None, None]) & (slot_pos.T[None] >= 0)
        table = jnp.sum(jnp.where(hit, gate_vals.T[None], 0.0), axis=1)
        gate_tab = jnp.pad(table.reshape(group, local_experts, tok), ((0, 0), (0, 8 - local_experts), (0, 0)))
        shared_dx, grad_shared_gate, grad_shared_up, grad_shared_down = shared_backward(x_tokens, dy_tokens, shared_gate, shared_up, shared_down)
        routed_sum, x_all, z_all, act_all, hid_all = routed(x_tokens, dy_tokens, gate_tab, w_gate, w_up, w_down)
        rows = group * tok
        grad_w_gate, grad_w_up = up_grads(x_all.reshape(rows, dim), act_all.reshape(rows, -1))
        grad_w_down = down_grads(hid_all.reshape(rows, -1), z_all.reshape(local_experts, rows, dim))
        grad_x = (routed_sum + shared_dx).astype(BF16)
        return grad_x, grad_w_gate, grad_w_up, grad_w_down, grad_shared_gate, grad_shared_up, grad_shared_down

    return jax.shard_map(local_backward, mesh=mesh, in_specs=(token_spec, token_spec, token_spec, token_spec, token_spec, expert_spec, expert_spec, expert_spec, whole_spec, whole_spec, whole_spec), out_specs=(token_spec, grad_spec, grad_spec, grad_spec, grad_spec, grad_spec, grad_spec), check_vma=False)
```

```python
import functools

import jax
import jax.numpy as jnp
from jax import lax
from jax.experimental import pallas as pl
from jax.experimental.pallas import tpu as pltpu
from jax.sharding import PartitionSpec as P

F32 = jnp.float32
BF16 = jnp.bfloat16
ANY = pl.BlockSpec(memory_space=pl.ANY)
VMEM = pl.BlockSpec(memory_space=pltpu.VMEM)
VMEM_LIMIT = 67_000_000


def dot_nn(a, b):
    return lax.dot_general(a, b, (((1,), (0,)), ((), ())), preferred_element_type=F32)


def dot_nt(a, b):
    return lax.dot_general(a, b, (((1,), (1,)), ((), ())), preferred_element_type=F32)


def dot_tn(a, b):
    return lax.dot_general(a, b, (((0,), (0,)), ((), ())), preferred_element_type=F32)


def swiglu_parts(act_gate, act_up, grad_hidden):
    gate_f32 = act_gate.astype(F32)
    up_f32 = act_up.astype(F32)
    sigma = jax.nn.sigmoid(gate_f32)
    silu_gate = gate_f32 * sigma
    hidden = (silu_gate * up_f32).astype(BF16)
    grad_gate = (grad_hidden * up_f32 * sigma * (1.0 + gate_f32 * (1.0 - sigma))).astype(BF16)
    grad_up = (grad_hidden * silu_gate).astype(BF16)
    return hidden, grad_gate, grad_up


def routed_kernel(x_in, dy_in, table, w_gate, w_up, w_down, s_gate, s_up, s_down,
                  grad_x, x_all, z_all, act_all, hid_all, sact_out, shid_out,
                  xbuf, dybuf, tbuf, pick, w13, w2, act, hst, xst, zst, sact, shid, sdx,
                  sums, dsend, pbuf, ybuf, cbuf, ebuf,
                  load_sem, out_sem, gs_sem, gr_sem, recv_sem, sy_sem, sd_sem, sown_sem, sz_sem, sx_sem,
                  ds_sem, dr_sem, ys_sem, yr_sem, cs_sem, cr_sem, es_sem, er_sem, credit):
    tok, dim = x_in.shape
    ff = w2.shape[1]
    cap = xst.shape[2]
    half = dim // 2
    tile = min(512, dim)
    me = lax.axis_index('ep')
    z = lax.div(me, 4)
    y = lax.rem(lax.div(me, 2), 2)
    c = lax.rem(me, 2)
    partner = me + 1 - 2 * c
    side = me + 2 - 4 * y
    inner = z * (3 - z)
    near_end = lax.div(z, 2)
    far_end = 1 - near_end
    bufs = (xbuf, dybuf)

    def bid(zz, yy, cc):
        return zz * 4 + yy * 2 + cc

    def order(k):
        near = lax.div(inner, 2)
        delta = lax.div((1 - k) * (2 - k) * (3 - k), 6) - lax.div(k * (2 - k) * (3 - k), 2)
        base = k + near * delta
        return base + near_end * (3 - 2 * base)

    def visit(t):
        u = t + lax.div(t, 7)
        odd = lax.rem(u, 2)
        first = lax.div(7 - t, 7)
        k = odd * lax.div(u + 1, 2) + (1 - odd) * (lax.div(u, 2) - 1) + first
        col = 1 - odd - first
        return order(k), y + col * (1 - 2 * y), col

    def remote(src, dst, send, recv, dev):
        return pltpu.make_async_remote_copy(src_ref=src, dst_ref=dst, send_sem=send, recv_sem=recv, device_id={'ep': dev}, device_id_type=pl.DeviceIdType.MESH)

    def weights(e, gate, up, down):
        return [pltpu.make_async_copy(gate, w13.at[e, :, pl.ds(0, ff)], load_sem.at[2 + 3 * e]),
                pltpu.make_async_copy(up, w13.at[e, :, pl.ds(ff, ff)], load_sem.at[3 + 3 * e]),
                pltpu.make_async_copy(down, w2.at[e], load_sem.at[4 + 3 * e])]

    own = [pltpu.make_async_copy(x_in, xbuf.at[me], load_sem.at[0]), pltpu.make_async_copy(dy_in, dybuf.at[me], load_sem.at[1])]
    shared_load = weights(1, s_gate, s_up, s_down)
    first_load = weights(0, w_gate.at[0], w_up.at[0], w_down.at[0])
    second_load = weights(1, w_gate.at[1], w_up.at[1], w_down.at[1])
    for cp in own + shared_load + first_load:
        cp.start()

    barrier = pltpu.get_barrier_semaphore()

    @pl.loop(1, 16)
    def _(d):
        pl.semaphore_signal(barrier, inc=1, device_id={'ep': lax.rem(me + d, 16)}, device_id_type=pl.DeviceIdType.MESH)
    pl.semaphore_wait(barrier, 15)

    def send_y(q, zb, b):
        return remote(bufs[q].at[b], bufs[q].at[b], sy_sem.at[q, zb], recv_sem.at[q, b], side)

    def send_d(q, zb, yb, b):
        return remote(bufs[q].at[b], bufs[q].at[b], sd_sem.at[q, zb * 2 + yb], recv_sem.at[q, b], partner)

    def send_own(q, up):
        return remote(bufs[q].at[me], bufs[q].at[me], sown_sem.at[q, up], recv_sem.at[q, me], me + (4 if up else -4))

    def send_fwd(q, zb, b, up):
        return remote(bufs[q].at[b], bufs[q].at[b], sz_sem.at[q, zb], recv_sem.at[q, b], me + (4 if up else -4))

    def send_end(b, up):
        return remote(xbuf.at[b], xbuf.at[b], sx_sem.at[1 - up], recv_sem.at[0, b], me + (4 if up else -4))

    for q in range(2):
        own[q].wait()
        send_y(q, z, me).start()

        @pl.when(z < 3)
        def _():
            send_own(q, 1).start()

        @pl.when(z > 0)
        def _():
            send_own(q, 0).start()
        send_d(q, z, y, me).start()

    def send_table(d):
        dest = lax.rem(me + d, 16)
        return remote(table.at[dest], tbuf.at[me], gs_sem.at[d], gr_sem.at[me], dest)

    @pl.loop(1, 16)
    def _(d):
        send_table(d).start()
    tbuf[me] = table[me]

    def arrive(t):
        zb, yb, col = visit(t)
        b = bid(zb, yb, c)
        middle = zb * (3 - zb)
        for q in range(2):
            send_d(q, zb, yb, b).wait_recv()

            @pl.when(col == 0)
            def _():
                if q:
                    send_y(q, zb, b).start()
                else:
                    @pl.when(middle > 0)
                    def _():
                        send_y(q, zb, b).start()

                @pl.when((zb > z) & (z > 0))
                def _():
                    send_fwd(q, zb, b, 0).start()

                @pl.when((zb < z) & (z < 3))
                def _():
                    send_fwd(q, zb, b, 1).start()
            if q == 0:
                @pl.when((col == 1) & (zb == 3) & (z > 0))
                def _():
                    send_end(b, 0).start()

                @pl.when((col == 1) & (zb == 0) & (z < 3))
                def _():
                    send_end(b, 1).start()
            send_d(q, zb, yb, b).start()

    def flush(t, start):
        zb, yb, _ = visit(t)
        two = pl.ds(bid(zb, yb, 0), 2)
        cps = [pltpu.make_async_copy(xst, x_all.at[:, two], out_sem.at[0, t]),
               pltpu.make_async_copy(zst, z_all.at[:, two], out_sem.at[1, t]),
               pltpu.make_async_copy(hst, hid_all.at[:, two], out_sem.at[2, t]),
               pltpu.make_async_copy(act.at[:, two], act_all.at[:, two], out_sem.at[3, t])]
        if start:
            for cp in cps:
                cp.start()
        else:
            for cp in cps[:3]:
                cp.wait()

    def compute(t):
        zb, yb, _ = visit(t)
        b0 = bid(zb, yb, 0)
        bp = bid(zb, yb, 1 - c)
        for q in range(2):
            send_d(q, zb, yb, bp).wait_recv()
        for p in range(2):
            @pl.when(b0 + p != me)
            def _():
                remote(table.at[0], tbuf.at[b0 + p], gs_sem.at[0], gr_sem.at[b0 + p], partner).wait_recv()

        @pl.when(t > 0)
        def _():
            flush(t - 1, False)
        row = lax.broadcasted_iota(jnp.int32, (2 * cap, tok), 0).astype(F32)
        for p in range(2):
            info = tbuf[b0 + p]
            top = row < cap
            chosen = jnp.where(top, info[2:3, :], info[3:4, :] + cap) == row
            gate = jnp.sum(jnp.where(chosen, jnp.where(top, info[0:1, :], info[1:2, :]), 0.0), axis=1, keepdims=True)
            sel = chosen.astype(BF16)
            pick[b0 + p] = sel
            for n in range(dim // tile):
                cols = slice(n * tile, (n + 1) * tile)
                xr = dot_nn(sel, xbuf[b0 + p, :, cols]).astype(BF16)
                zr = (dot_nn(sel, dybuf[b0 + p, :, cols]) * gate).astype(BF16)
                for e in range(2):
                    xst[e, p, :, cols] = xr[e * cap:(e + 1) * cap]
                    zst[e, p, :, cols] = zr[e * cap:(e + 1) * cap]
        two = pl.ds(b0, 2)
        for e in range(2):
            ab = dot_nn(xst[e].reshape(2 * cap, dim), w13[e]).astype(BF16)
            grad_hidden = dot_nt(zst[e].reshape(2 * cap, dim), w2[e])
            hidden, grad_gate, grad_up = swiglu_parts(ab[:, :ff], ab[:, ff:], grad_hidden)
            hst[e] = hidden.reshape(2, cap, ff)
            act[e, two, :, :ff] = grad_gate.reshape(2, cap, ff)
            act[e, two, :, ff:] = grad_up.reshape(2, cap, ff)
        flush(t, True)

    for cp in shared_load:
        cp.wait()
    ab = dot_nn(xbuf[me], w13[1]).astype(BF16)
    hidden, grad_gate, grad_up = swiglu_parts(ab[:, :ff], ab[:, ff:], dot_nt(dybuf[me], w2[1]))
    shid[...] = hidden
    sact[:, :ff] = grad_gate
    sact[:, ff:] = grad_up
    for n in range(dim // tile):
        cols = slice(n * tile, (n + 1) * tile)
        sdx[:, cols] = dot_nt(sact[...], w13[1, cols, :])
    shared_out = [pltpu.make_async_copy(sact, sact_out, load_sem.at[0]), pltpu.make_async_copy(shid, shid_out, load_sem.at[1])]
    for cp in shared_out + second_load:
        cp.start()
    for cp in first_load + second_load:
        cp.wait()
    compute(0)

    @pl.loop(1, 8)
    def _(t):
        arrive(t)
        compute(t)

    def rs_visit(j):
        late = lax.div(j, 4)
        zb = order(3 - lax.rem(j, 4))
        col = 1 - late
        return zb, y + col * (1 - 2 * y)

    def give(j):
        return remote(dsend.at[lax.rem(j, 2)], pbuf.at[lax.rem(j, 2)], ds_sem.at[lax.rem(j, 2)], dr_sem.at[lax.rem(j, 2)], partner)

    def part(h):
        return pl.ds(h * half, half)

    def rs_y(j, zb, h):
        return remote(sums.at[j, :, part(h)], ybuf.at[zb, :, part(h)], ys_sem.at[zb, h], yr_sem.at[zb, h], side)

    def rs_end(j, end):
        return remote(sums.at[j, :, part(0)], ebuf.at[end], es_sem.at[end], er_sem.at[end], me + 8 * end - 4)

    def rs_compute(j):
        zb, yb = rs_visit(j)
        b = bid(zb, yb, c)
        bp = bid(zb, yb, 1 - c)

        @pl.when(j >= 2)
        def _():
            give(j).wait_send()

        @pl.loop(0, dim // tile)
        def _(n):
            cols = pl.ds(pl.multiple_of(n * tile, tile), tile)
            r = [dot_nt(jnp.concatenate([act[e, b], act[e, bp]], axis=0), w13[e, cols, :]).astype(BF16) for e in range(2)]
            sums[j, :, cols] = dot_tn(pick[b], jnp.concatenate([r[0][:cap], r[1][:cap]], axis=0))
            dsend[lax.rem(j, 2), :, cols] = dot_tn(pick[bp], jnp.concatenate([r[0][cap:], r[1][cap:]], axis=0))

        @pl.when(j >= 2)
        def _():
            pl.semaphore_wait(credit, 1)
        give(j).start()

    def rs_finish(j):
        give(j).wait_recv()
        sums[j] = sums[j] + pbuf[lax.rem(j, 2)]

        @pl.when(j < 6)
        def _():
            pl.semaphore_signal(credit, inc=1, device_id={'ep': partner}, device_id_type=pl.DeviceIdType.MESH)

        @pl.when((j == 0) & (inner == 0))
        def _():
            rs_end(0, far_end).start()

        @pl.when(j < 4)
        def _():
            zb, _ = rs_visit(j)
            rs_y(j, zb, 1).start()

            @pl.when(zb * (3 - zb) > 0)
            def _():
                rs_y(j, zb, 0).start()

    @pl.loop(0, 9)
    def _(j):
        @pl.when(j < 8)
        def _():
            rs_compute(j)

        @pl.when(j > 0)
        def _():
            rs_finish(j - 1)

    def end_in(j, end):
        rs_end(j, end).wait_recv()
        sums[j, :, part(0)] = sums[j, :, part(0)] + ebuf[end]

    def chain(k, h, zb, up):
        j = 7 - k
        slot, gap = (0, zb - z - 1) if up else (1, z - zb - 1)
        return remote(sums.at[j, :, part(h)], cbuf.at[slot, gap, :, part(h)], cs_sem.at[k, h], cr_sem.at[slot, gap, h], me + (4 if up else -4))

    def chain_in(j, h, slot, gap):
        remote(sums.at[j, :, part(h)], cbuf.at[slot, gap, :, part(h)], cs_sem.at[0, h], cr_sem.at[slot, gap, h], partner).wait_recv()
        sums[j, :, part(h)] = sums[j, :, part(h)] + cbuf[slot, gap, :, part(h)]

    def y_in(j, zb, h):
        rs_y(0, zb, h).wait_recv()
        sums[j, :, part(h)] = sums[j, :, part(h)] + ybuf[zb, :, part(h)]

    def step(k, h):
        zb = order(k)
        j = 7 - k
        if h == 1 or k == 2:
            y_in(j, zb, h)
        elif k == 1:
            @pl.when(zb * (3 - zb) > 0)
            def _():
                y_in(j, zb, h)

        @pl.when(zb > z)
        def _():
            @pl.when(z > 0)
            def _():
                chain_in(j, h, 0, zb - z)
            chain(k, h, zb, True).start()

        @pl.when(zb < z)
        def _():
            @pl.when(z < 3)
            def _():
                chain_in(j, h, 1, z - zb)
            chain(k, h, zb, False).start()

    @pl.when(inner > 0)
    def _():
        end_in(0, far_end)
        rs_end(0, far_end).start()
    step(3, 0)

    @pl.when(inner > 0)
    def _():
        end_in(2, near_end)
        rs_end(2, near_end).start()
    step(3, 1)
    step(2, 0)

    @pl.when(inner == 0)
    def _():
        end_in(3, near_end)
        rs_y(3, z, 0).start()
    step(2, 1)
    step(1, 0)
    step(1, 1)
    flush(7, False)
    for h in range(2):
        @pl.when(z > 0)
        def _():
            chain_in(7, h, 0, 0)

        @pl.when(z < 3)
        def _():
            chain_in(7, h, 1, 0)
        rs_y(0, z, h).wait_recv()
        total = sums[7, :, part(h)] + ybuf[z, :, part(h)] + sdx[:, part(h)]
        xst[0, :, :, part(h)] = total.astype(BF16).reshape(2, cap, half)
    result = pltpu.make_async_copy(xst.at[0], grad_x, load_sem.at[2])
    result.start()

    for cp in shared_out:
        cp.wait()
    for t in range(8):
        pltpu.make_async_copy(act.at[:, pl.ds(0, 2)], act_all.at[:, pl.ds(0, 2)], out_sem.at[3, t]).wait()
    for zb in range(4):
        for q in range(2):
            if q or zb in (1, 2):
                send_y(q, zb, 0).wait_send()
            else:
                @pl.when(z == zb)
                def _():
                    send_y(q, zb, 0).wait_send()
            for yb in range(2):
                send_d(q, zb, yb, 0).wait_send()

            @pl.when(((zb > z) & (z > 0)) | ((zb < z) & (z < 3)))
            def _():
                send_fwd(q, zb, 0, 1).wait_send()
        for h in range(2):
            if h or zb in (1, 2):
                rs_y(0, zb, h).wait_send()
            else:
                @pl.when(z == zb)
                def _():
                    rs_y(0, zb, h).wait_send()
            if zb:
                remote(sums.at[0, :, part(h)], cbuf.at[0, 0, :, part(h)], cs_sem.at[zb, h], cr_sem.at[0, 0, h], partner).wait_send()

    @pl.when(z < 3)
    def _():
        send_end(0, 1).wait_send()
        for q in range(2):
            send_own(q, 1).wait_send()

    @pl.when(z > 0)
    def _():
        send_end(0, 0).wait_send()
        for q in range(2):
            send_own(q, 0).wait_send()
    rs_end(0, far_end).wait_send()

    @pl.when(inner > 0)
    def _():
        rs_end(0, near_end).wait_send()

    @pl.loop(1, 16)
    def _(d):
        send_table(d).wait_send()
    for j in range(2):
        give(j).wait_send()
    result.wait()


def routed(x_tokens, dy_tokens, table, w_gate, w_up, w_down, s_gate, s_up, s_down):
    tok, dim = x_tokens.shape
    ff = w_gate.shape[2]
    cap = tok // 2
    dma = pltpu.SemaphoreType.DMA
    shape = jax.ShapeDtypeStruct
    return pl.pallas_call(
        routed_kernel,
        name='routed',
        out_shape=(shape((2, cap, dim), BF16), shape((2, 16, cap, dim), BF16), shape((2, 16, cap, dim), BF16),
                   shape((2, 16, cap, 2 * ff), BF16), shape((2, 16, cap, ff), BF16), shape((tok, 2 * ff), BF16), shape((tok, ff), BF16)),
        in_specs=[ANY, ANY, VMEM] + [ANY] * 6,
        out_specs=(ANY,) * 7,
        scratch_shapes=[
            pltpu.VMEM((16, tok, dim), BF16), pltpu.VMEM((16, tok, dim), BF16), pltpu.VMEM((16, 8, tok), F32), pltpu.VMEM((16, 2 * cap, tok), BF16),
            pltpu.VMEM((2, dim, 2 * ff), BF16), pltpu.VMEM((2, ff, dim), BF16),
            pltpu.VMEM((2, 16, cap, 2 * ff), BF16), pltpu.VMEM((2, 2, cap, ff), BF16), pltpu.VMEM((2, 2, cap, dim), BF16), pltpu.VMEM((2, 2, cap, dim), BF16),
            pltpu.VMEM((tok, 2 * ff), BF16), pltpu.VMEM((tok, ff), BF16), pltpu.VMEM((tok, dim), F32),
            pltpu.VMEM((8, tok, dim), F32), pltpu.VMEM((2, tok, dim), F32), pltpu.VMEM((2, tok, dim), F32),
            pltpu.VMEM((4, tok, dim), F32), pltpu.VMEM((2, 3, tok, dim), F32), pltpu.VMEM((2, tok, dim // 2), F32),
            dma((8,)), dma((4, 8)), dma((16,)), dma((16,)), dma((2, 16)), dma((2, 4)), dma((2, 8)), dma((2, 2)), dma((2, 4)), dma((2,)),
            dma((2,)), dma((2,)), dma((4, 2)), dma((4, 2)), dma((4, 2)), dma((2, 3, 2)), dma((2,)), dma((2,)), pltpu.SemaphoreType.REGULAR,
        ],
        compiler_params=pltpu.CompilerParams(collective_id=0, has_side_effects=True, vmem_limit_bytes=VMEM_LIMIT),
        cost_estimate=pl.CostEstimate(flops=16 * tok * 2 * dim * ff * 5, bytes_accessed=80_000_000, transcendentals=0),
    )(x_tokens, dy_tokens, table, w_gate, w_up, w_down, s_gate, s_up, s_down)


def up_grad_kernel(x, act, g1, g3):
    ff = g1.shape[2]
    both = dot_tn(x[0], act[0])
    g1[0] = both[:, :ff]
    g3[0] = both[:, ff:]


def up_grads(x, act):
    experts, rows, dim = x.shape
    ff = act.shape[2] // 2
    tile = min(512, dim)
    out = jax.ShapeDtypeStruct((experts, dim, ff), F32)
    return pl.pallas_call(
        up_grad_kernel,
        name='up_grads',
        out_shape=(out, out),
        grid=(experts, dim // tile),
        in_specs=[pl.BlockSpec((1, rows, tile), lambda e, i: (e, 0, i)), pl.BlockSpec((1, rows, 2 * ff), lambda e, i: (e, 0, 0))],
        out_specs=(pl.BlockSpec((1, tile, ff), lambda e, i: (e, i, 0)),) * 2,
        compiler_params=pltpu.CompilerParams(vmem_limit_bytes=60_000_000),
        cost_estimate=pl.CostEstimate(flops=4 * experts * rows * dim * ff, bytes_accessed=8 * experts * dim * ff + 2 * x.size + 2 * act.size, transcendentals=0),
    )(x, act)


def down_grad_kernel(hid, dz, g2):
    g2[0] = dot_tn(hid[0], dz[0])


def down_grads(hid, dz):
    experts, rows, dim = dz.shape
    ff = hid.shape[2]
    tile = min(512, dim)
    return pl.pallas_call(
        down_grad_kernel,
        name='down_grads',
        out_shape=jax.ShapeDtypeStruct((experts, ff, dim), F32),
        grid=(experts, dim // tile),
        in_specs=[pl.BlockSpec((1, rows, ff), lambda e, n: (e, 0, 0)), pl.BlockSpec((1, rows, tile), lambda e, n: (e, 0, n))],
        out_specs=pl.BlockSpec((1, ff, tile), lambda e, n: (e, 0, n)),
        compiler_params=pltpu.CompilerParams(vmem_limit_bytes=60_000_000),
        cost_estimate=pl.CostEstimate(flops=2 * experts * rows * dim * ff, bytes_accessed=4 * experts * dim * ff + 2 * hid.size + 2 * dz.size, transcendentals=0),
    )(hid, dz)


def shared_grad_kernel(x, dy, act, hid, g1, g3, g2):
    ff = hid.shape[1]
    both = dot_tn(x[...], act[...])
    g1[0] = both[:, :ff]
    g3[0] = both[:, ff:]
    g2[0] = dot_tn(hid[...], dy[...])


def shared_grads(x, dy, act, hid):
    tok, dim = x.shape
    ff = hid.shape[1]
    tile = min(512, dim)
    out = jax.ShapeDtypeStruct((1, dim, ff), F32)
    return pl.pallas_call(
        shared_grad_kernel,
        name='shared_grads',
        out_shape=(out, out, jax.ShapeDtypeStruct((1, ff, dim), F32)),
        grid=(dim // tile,),
        in_specs=[pl.BlockSpec((tok, tile), lambda i: (0, i)), pl.BlockSpec((tok, tile), lambda i: (0, i)), pl.BlockSpec((tok, 2 * ff), lambda i: (0, 0)), pl.BlockSpec((tok, ff), lambda i: (0, 0))],
        out_specs=(pl.BlockSpec((1, tile, ff), lambda i: (0, i, 0)),) * 2 + (pl.BlockSpec((1, ff, tile), lambda i: (0, 0, i)),),
        compiler_params=pltpu.CompilerParams(vmem_limit_bytes=60_000_000),
        cost_estimate=pl.CostEstimate(flops=6 * tok * dim * ff, bytes_accessed=12 * dim * ff + 4 * x.size, transcendentals=0),
    )(x, dy, act, hid)


def solution(mesh):
    group = mesh.shape['ep']
    token_spec = P(('dp', 'ep'), None)
    expert_spec = P('ep', None, None)
    whole_spec = P(None, None)
    grad_spec = P(('dp', 'ep'), None, None)

    def local_backward(x_tokens, dy_tokens, expert_ids, gate_vals, slot_pos, w_gate, w_up, w_down, shared_gate, shared_up, shared_down):
        tok, dim = x_tokens.shape
        local_experts = w_gate.shape[0]
        experts = jnp.arange(group * local_experts, dtype=jnp.int32)
        hit = (expert_ids.T[None] == experts[:, None, None]) & (slot_pos.T[None] >= 0)
        gates = jnp.sum(jnp.where(hit, gate_vals.T[None], 0.0), axis=1)
        slots = jnp.sum(jnp.where(hit, slot_pos.T[None].astype(F32) + 1.0, 0.0), axis=1) - 1.0
        table = jnp.concatenate([gates.reshape(group, local_experts, tok), slots.reshape(group, local_experts, tok), jnp.zeros((group, 8 - 2 * local_experts, tok), F32)], axis=1)
        grad_x, x_all, z_all, act_all, hid_all, sact, shid = routed(x_tokens, dy_tokens, table, w_gate, w_up, w_down, shared_gate, shared_up, shared_down)
        x_all, z_all, act_all, hid_all = [a.reshape(local_experts, -1, a.shape[-1]) for a in (x_all, z_all, act_all, hid_all)]
        grad_w_gate, grad_w_up = up_grads(x_all, act_all)
        grad_w_down = down_grads(hid_all, z_all)
        grad_shared_gate, grad_shared_up, grad_shared_down = shared_grads(x_tokens, dy_tokens, sact, shid)
        grad_x = grad_x.reshape(tok, dim)
        return grad_x, grad_w_gate, grad_w_up, grad_w_down, grad_shared_gate, grad_shared_up, grad_shared_down

    return jax.shard_map(local_backward, mesh=mesh, in_specs=(token_spec, token_spec, token_spec, token_spec, token_spec, expert_spec, expert_spec, expert_spec, whole_spec, whole_spec, whole_spec), out_specs=(token_spec, grad_spec, grad_spec, grad_spec, grad_spec, grad_spec, grad_spec), check_vma=False)
```

```python
import functools

import jax
import jax.numpy as jnp
from jax import lax
from jax.experimental import pallas as pl
from jax.experimental.pallas import tpu as pltpu
from jax.sharding import PartitionSpec as P

F32 = jnp.float32
BF16 = jnp.bfloat16
ANY = pl.BlockSpec(memory_space=pl.ANY)
VMEM = pl.BlockSpec(memory_space=pltpu.VMEM)
VMEM_LIMIT = 67_000_000


def dot_nn(a, b):
    return lax.dot_general(a, b, (((1,), (0,)), ((), ())), preferred_element_type=F32)


def dot_nt(a, b):
    return lax.dot_general(a, b, (((1,), (1,)), ((), ())), preferred_element_type=F32)


def dot_tn(a, b):
    return lax.dot_general(a, b, (((0,), (0,)), ((), ())), preferred_element_type=F32)


def swiglu_parts(act_gate, act_up, grad_hidden):
    gate_f32 = act_gate.astype(F32)
    up_f32 = act_up.astype(F32)
    sigma = jax.nn.sigmoid(gate_f32)
    silu_gate = gate_f32 * sigma
    hidden = (silu_gate * up_f32).astype(BF16)
    grad_gate = (grad_hidden * up_f32 * sigma * (1.0 + gate_f32 * (1.0 - sigma))).astype(BF16)
    grad_up = (grad_hidden * silu_gate).astype(BF16)
    return hidden, grad_gate, grad_up


def routed_kernel(x_in, dy_in, table, w_gate, w_up, w_down, s_gate, s_up, s_down,
                  grad_x, x_all, z_all, act_all, hid_all, sact_out, shid_out,
                  xbuf, dybuf, tbuf, pick, w13, w2, act, hst, xst, zst, sact, shid, sdx,
                  sums, dsend, pbuf, ybuf, cbuf, ebuf,
                  load_sem, out_sem, gs_sem, gr_sem, recv_sem, sy_sem, sd_sem, sown_sem, sz_sem, sx_sem,
                  ds_sem, dr_sem, ys_sem, yr_sem, cs_sem, cr_sem, es_sem, er_sem, credit):
    tok, dim = x_in.shape
    ff = w2.shape[1]
    cap = xst.shape[2]
    half = dim // 2
    tile = min(512, dim)
    me = lax.axis_index('ep')
    z = lax.div(me, 4)
    y = lax.rem(lax.div(me, 2), 2)
    c = lax.rem(me, 2)
    partner = me + 1 - 2 * c
    side = me + 2 - 4 * y
    inner = z * (3 - z)
    near_end = lax.div(z, 2)
    far_end = 1 - near_end
    bufs = (xbuf, dybuf)

    def bid(zz, yy, cc):
        return zz * 4 + yy * 2 + cc

    def order(k):
        near = lax.div(inner, 2)
        delta = lax.div((1 - k) * (2 - k) * (3 - k), 6) - lax.div(k * (2 - k) * (3 - k), 2)
        base = k + near * delta
        return base + near_end * (3 - 2 * base)

    def visit(t):
        u = t + lax.div(t, 7)
        odd = lax.rem(u, 2)
        first = lax.div(7 - t, 7)
        k = odd * lax.div(u + 1, 2) + (1 - odd) * (lax.div(u, 2) - 1) + first
        col = 1 - odd - first
        return order(k), y + col * (1 - 2 * y), col

    def remote(src, dst, send, recv, dev):
        return pltpu.make_async_remote_copy(src_ref=src, dst_ref=dst, send_sem=send, recv_sem=recv, device_id={'ep': dev}, device_id_type=pl.DeviceIdType.MESH)

    def weights(e, gate, up, down):
        return [pltpu.make_async_copy(gate, w13.at[e, :, pl.ds(0, ff)], load_sem.at[2 + 3 * e]),
                pltpu.make_async_copy(up, w13.at[e, :, pl.ds(ff, ff)], load_sem.at[3 + 3 * e]),
                pltpu.make_async_copy(down, w2.at[e], load_sem.at[4 + 3 * e])]

    own = [pltpu.make_async_copy(x_in, xbuf.at[me], load_sem.at[0]), pltpu.make_async_copy(dy_in, dybuf.at[me], load_sem.at[1])]
    shared_load = weights(1, s_gate, s_up, s_down)
    first_load = weights(0, w_gate.at[0], w_up.at[0], w_down.at[0])
    second_load = weights(1, w_gate.at[1], w_up.at[1], w_down.at[1])
    for cp in own + shared_load + first_load:
        cp.start()

    barrier = pltpu.get_barrier_semaphore()

    @pl.loop(1, 16)
    def _(d):
        pl.semaphore_signal(barrier, inc=1, device_id={'ep': lax.rem(me + d, 16)}, device_id_type=pl.DeviceIdType.MESH)
    pl.semaphore_wait(barrier, 15)

    def send_y(q, zb, b):
        return remote(bufs[q].at[b], bufs[q].at[b], sy_sem.at[q, zb], recv_sem.at[q, b], side)

    def send_d(q, zb, yb, b):
        return remote(bufs[q].at[b], bufs[q].at[b], sd_sem.at[q, zb * 2 + yb], recv_sem.at[q, b], partner)

    def send_own(q, up):
        return remote(bufs[q].at[me], bufs[q].at[me], sown_sem.at[q, up], recv_sem.at[q, me], me + (4 if up else -4))

    def send_fwd(q, zb, b, up):
        return remote(bufs[q].at[b], bufs[q].at[b], sz_sem.at[q, zb], recv_sem.at[q, b], me + (4 if up else -4))

    def send_end(b, up):
        return remote(xbuf.at[b], xbuf.at[b], sx_sem.at[1 - up], recv_sem.at[0, b], me + (4 if up else -4))

    for q in range(2):
        own[q].wait()
        send_y(q, z, me).start()

        @pl.when(z < 3)
        def _():
            send_own(q, 1).start()

        @pl.when(z > 0)
        def _():
            send_own(q, 0).start()
        send_d(q, z, y, me).start()

    def send_table(d):
        dest = lax.rem(me + d, 16)
        return remote(table.at[dest], tbuf.at[me], gs_sem.at[d], gr_sem.at[me], dest)

    @pl.loop(1, 16)
    def _(d):
        send_table(d).start()
    tbuf[me] = table[me]

    def arrive(t):
        zb, yb, col = visit(t)
        b = bid(zb, yb, c)
        middle = zb * (3 - zb)
        for q in range(2):
            send_d(q, zb, yb, b).wait_recv()

            @pl.when(col == 0)
            def _():
                if q:
                    send_y(q, zb, b).start()
                else:
                    @pl.when(middle > 0)
                    def _():
                        send_y(q, zb, b).start()

                @pl.when((zb > z) & (z > 0))
                def _():
                    send_fwd(q, zb, b, 0).start()

                @pl.when((zb < z) & (z < 3))
                def _():
                    send_fwd(q, zb, b, 1).start()
            if q == 0:
                @pl.when((col == 1) & (zb == 3) & (z > 0))
                def _():
                    send_end(b, 0).start()

                @pl.when((col == 1) & (zb == 0) & (z < 3))
                def _():
                    send_end(b, 1).start()
            send_d(q, zb, yb, b).start()

    def flush(t, start):
        zb, yb, _ = visit(t)
        two = pl.ds(bid(zb, yb, 0), 2)
        cps = [pltpu.make_async_copy(xst, x_all.at[:, two], out_sem.at[0, t]),
               pltpu.make_async_copy(zst, z_all.at[:, two], out_sem.at[1, t]),
               pltpu.make_async_copy(hst, hid_all.at[:, two], out_sem.at[2, t]),
               pltpu.make_async_copy(act.at[:, two], act_all.at[:, two], out_sem.at[3, t])]
        if start:
            for cp in cps:
                cp.start()
        else:
            for cp in cps[:3]:
                cp.wait()

    def compute(t):
        zb, yb, _ = visit(t)
        b0 = bid(zb, yb, 0)
        bp = bid(zb, yb, 1 - c)
        for q in range(2):
            send_d(q, zb, yb, bp).wait_recv()
        for p in range(2):
            @pl.when(b0 + p != me)
            def _():
                remote(table.at[0], tbuf.at[b0 + p], gs_sem.at[0], gr_sem.at[b0 + p], partner).wait_recv()

        @pl.when(t > 0)
        def _():
            flush(t - 1, False)
        row = lax.broadcasted_iota(jnp.int32, (2 * cap, tok), 0).astype(F32)
        for p in range(2):
            info = tbuf[b0 + p]
            top = row < cap
            chosen = jnp.where(top, info[2:3, :], info[3:4, :] + cap) == row
            gate = jnp.sum(jnp.where(chosen, jnp.where(top, info[0:1, :], info[1:2, :]), 0.0), axis=1, keepdims=True)
            sel = chosen.astype(BF16)
            pick[b0 + p] = sel
            for n in range(dim // tile):
                cols = slice(n * tile, (n + 1) * tile)
                xr = dot_nn(sel, xbuf[b0 + p, :, cols]).astype(BF16)
                zr = (dot_nn(sel, dybuf[b0 + p, :, cols]) * gate).astype(BF16)
                for e in range(2):
                    xst[e, p, :, cols] = xr[e * cap:(e + 1) * cap]
                    zst[e, p, :, cols] = zr[e * cap:(e + 1) * cap]
        two = pl.ds(b0, 2)
        for e in range(2):
            ab = dot_nn(xst[e].reshape(2 * cap, dim), w13[e]).astype(BF16)
            grad_hidden = dot_nt(zst[e].reshape(2 * cap, dim), w2[e])
            hidden, grad_gate, grad_up = swiglu_parts(ab[:, :ff], ab[:, ff:], grad_hidden)
            hst[e] = hidden.reshape(2, cap, ff)
            act[e, two, :, :ff] = grad_gate.reshape(2, cap, ff)
            act[e, two, :, ff:] = grad_up.reshape(2, cap, ff)
        flush(t, True)

    for cp in shared_load:
        cp.wait()
    ab = dot_nn(xbuf[me], w13[1]).astype(BF16)
    hidden, grad_gate, grad_up = swiglu_parts(ab[:, :ff], ab[:, ff:], dot_nt(dybuf[me], w2[1]))
    shid[...] = hidden
    sact[:, :ff] = grad_gate
    sact[:, ff:] = grad_up
    for n in range(dim // tile):
        cols = slice(n * tile, (n + 1) * tile)
        sdx[:, cols] = dot_nt(sact[...], w13[1, cols, :])
    shared_out = [pltpu.make_async_copy(sact, sact_out, load_sem.at[0]), pltpu.make_async_copy(shid, shid_out, load_sem.at[1])]
    for cp in shared_out + second_load:
        cp.start()
    for cp in first_load + second_load:
        cp.wait()
    def give(j):
        return remote(dsend.at[lax.rem(j, 2)], pbuf.at[lax.rem(j, 2)], ds_sem.at[lax.rem(j, 2)], dr_sem.at[lax.rem(j, 2)], partner)

    def part(h):
        return pl.ds(h * half, half)

    def rs_y(j, zb, h):
        return remote(sums.at[j, :, part(h)], ybuf.at[zb, :, part(h)], ys_sem.at[zb, h], yr_sem.at[zb, h], side)

    def rs_end(j, end):
        return remote(sums.at[j, :, part(0)], ebuf.at[end], es_sem.at[end], er_sem.at[end], me + 8 * end - 4)

    def rs_compute(j):
        zb, yb, _ = visit(j)
        b = bid(zb, yb, c)
        bp = bid(zb, yb, 1 - c)

        @pl.when(j >= 2)
        def _():
            give(j).wait_send()

        @pl.loop(0, dim // tile)
        def _(n):
            cols = pl.ds(pl.multiple_of(n * tile, tile), tile)
            r = [dot_nt(jnp.concatenate([act[e, b], act[e, bp]], axis=0), w13[e, cols, :]).astype(BF16) for e in range(2)]
            sums[j, :, cols] = dot_tn(pick[b], jnp.concatenate([r[0][:cap], r[1][:cap]], axis=0))
            dsend[lax.rem(j, 2), :, cols] = dot_tn(pick[bp], jnp.concatenate([r[0][cap:], r[1][cap:]], axis=0))

        @pl.when(j >= 2)
        def _():
            pl.semaphore_wait(credit, 1)
        give(j).start()

    def rs_finish(j):
        give(j).wait_recv()
        sums[j] = sums[j] + pbuf[lax.rem(j, 2)]

        @pl.when(j < 6)
        def _():
            pl.semaphore_signal(credit, inc=1, device_id={'ep': partner}, device_id_type=pl.DeviceIdType.MESH)

    own_slot = (0, 1, 3, 5)
    other_slot = (2, 4, 6, 7)

    def end_in(j, end):
        rs_end(j, end).wait_recv()
        sums[j, :, part(0)] = sums[j, :, part(0)] + ebuf[end]

    def chain(k, h, zb, up):
        j = own_slot[k]
        slot, gap = (0, zb - z - 1) if up else (1, z - zb - 1)
        return remote(sums.at[j, :, part(h)], cbuf.at[slot, gap, :, part(h)], cs_sem.at[k, h], cr_sem.at[slot, gap, h], me + (4 if up else -4))

    def chain_in(j, h, slot, gap):
        remote(sums.at[j, :, part(h)], cbuf.at[slot, gap, :, part(h)], cs_sem.at[0, h], cr_sem.at[slot, gap, h], partner).wait_recv()
        sums[j, :, part(h)] = sums[j, :, part(h)] + cbuf[slot, gap, :, part(h)]

    def y_in(j, zb, h):
        rs_y(0, zb, h).wait_recv()
        sums[j, :, part(h)] = sums[j, :, part(h)] + ybuf[zb, :, part(h)]

    def step(k, h):
        zb = order(k)
        j = own_slot[k]
        if h == 1 or k == 2:
            y_in(j, zb, h)
        elif k == 1:
            @pl.when(zb * (3 - zb) > 0)
            def _():
                y_in(j, zb, h)

        @pl.when(zb > z)
        def _():
            @pl.when(z > 0)
            def _():
                chain_in(j, h, 0, zb - z)
            chain(k, h, zb, True).start()

        @pl.when(zb < z)
        def _():
            @pl.when(z < 3)
            def _():
                chain_in(j, h, 1, z - zb)
            chain(k, h, zb, False).start()

    def scatter_y(k):
        zb = order(k)
        rs_y(other_slot[k], zb, 1).start()
        if k == 2:
            rs_y(other_slot[k], zb, 0).start()
        elif k == 1:
            @pl.when(zb * (3 - zb) > 0)
            def _():
                rs_y(other_slot[k], zb, 0).start()
        elif k == 0:
            @pl.when(inner > 0)
            def _():
                rs_y(other_slot[k], zb, 0).start()

    @pl.loop(0, 8)
    def _(t):
        @pl.when(t > 0)
        def _():
            arrive(t)
        compute(t)
        rs_compute(t)
        rs_finish(t)

        @pl.when((t == 5) & (inner == 0))
        def _():
            step(3, 0)

        @pl.when(t == 6)
        def _():
            scatter_y(2)

    scatter_y(3)

    @pl.when(inner == 0)
    def _():
        rs_end(other_slot[3], far_end).start()
    scatter_y(1)
    scatter_y(0)

    @pl.when(inner > 0)
    def _():
        step(3, 0)
        step(1, 0)
        end_in(other_slot[3], far_end)
        rs_end(other_slot[3], far_end).start()
        end_in(other_slot[1], near_end)
        rs_end(other_slot[1], near_end).start()
    step(2, 1)
    step(2, 0)
    step(3, 1)

    @pl.when(inner == 0)
    def _():
        end_in(other_slot[0], near_end)
        rs_y(other_slot[0], z, 0).start()
    step(1, 1)

    @pl.when(inner == 0)
    def _():
        step(1, 0)
    flush(7, False)
    for h in range(2):
        @pl.when(z > 0)
        def _():
            chain_in(0, h, 0, 0)

        @pl.when(z < 3)
        def _():
            chain_in(0, h, 1, 0)
        rs_y(0, z, h).wait_recv()
        total = sums[0, :, part(h)] + ybuf[z, :, part(h)] + sdx[:, part(h)]
        xst[0, :, :, part(h)] = total.astype(BF16).reshape(2, cap, half)
    result = pltpu.make_async_copy(xst.at[0], grad_x, load_sem.at[2])
    result.start()

    for cp in shared_out:
        cp.wait()
    for t in range(8):
        pltpu.make_async_copy(act.at[:, pl.ds(0, 2)], act_all.at[:, pl.ds(0, 2)], out_sem.at[3, t]).wait()
    for zb in range(4):
        for q in range(2):
            if q or zb in (1, 2):
                send_y(q, zb, 0).wait_send()
            else:
                @pl.when(z == zb)
                def _():
                    send_y(q, zb, 0).wait_send()
            for yb in range(2):
                send_d(q, zb, yb, 0).wait_send()

            @pl.when(((zb > z) & (z > 0)) | ((zb < z) & (z < 3)))
            def _():
                send_fwd(q, zb, 0, 1).wait_send()
        for h in range(2):
            if h or zb in (1, 2):
                rs_y(0, zb, h).wait_send()
            else:
                @pl.when(z == zb)
                def _():
                    rs_y(0, zb, h).wait_send()
            if zb:
                remote(sums.at[0, :, part(h)], cbuf.at[0, 0, :, part(h)], cs_sem.at[zb, h], cr_sem.at[0, 0, h], partner).wait_send()

    @pl.when(z < 3)
    def _():
        send_end(0, 1).wait_send()
        for q in range(2):
            send_own(q, 1).wait_send()

    @pl.when(z > 0)
    def _():
        send_end(0, 0).wait_send()
        for q in range(2):
            send_own(q, 0).wait_send()
    rs_end(0, far_end).wait_send()

    @pl.when(inner > 0)
    def _():
        rs_end(0, near_end).wait_send()

    @pl.loop(1, 16)
    def _(d):
        send_table(d).wait_send()
    for j in range(2):
        give(j).wait_send()
    result.wait()


def routed(x_tokens, dy_tokens, table, w_gate, w_up, w_down, s_gate, s_up, s_down):
    tok, dim = x_tokens.shape
    ff = w_gate.shape[2]
    cap = tok // 2
    dma = pltpu.SemaphoreType.DMA
    shape = jax.ShapeDtypeStruct
    return pl.pallas_call(
        routed_kernel,
        name='routed',
        out_shape=(shape((2, cap, dim), BF16), shape((2, 16, cap, dim), BF16), shape((2, 16, cap, dim), BF16),
                   shape((2, 16, cap, 2 * ff), BF16), shape((2, 16, cap, ff), BF16), shape((tok, 2 * ff), BF16), shape((tok, ff), BF16)),
        in_specs=[ANY, ANY, VMEM] + [ANY] * 6,
        out_specs=(ANY,) * 7,
        scratch_shapes=[
            pltpu.VMEM((16, tok, dim), BF16), pltpu.VMEM((16, tok, dim), BF16), pltpu.VMEM((16, 8, tok), F32), pltpu.VMEM((16, 2 * cap, tok), BF16),
            pltpu.VMEM((2, dim, 2 * ff), BF16), pltpu.VMEM((2, ff, dim), BF16),
            pltpu.VMEM((2, 16, cap, 2 * ff), BF16), pltpu.VMEM((2, 2, cap, ff), BF16), pltpu.VMEM((2, 2, cap, dim), BF16), pltpu.VMEM((2, 2, cap, dim), BF16),
            pltpu.VMEM((tok, 2 * ff), BF16), pltpu.VMEM((tok, ff), BF16), pltpu.VMEM((tok, dim), F32),
            pltpu.VMEM((8, tok, dim), F32), pltpu.VMEM((2, tok, dim), F32), pltpu.VMEM((2, tok, dim), F32),
            pltpu.VMEM((4, tok, dim), F32), pltpu.VMEM((2, 3, tok, dim), F32), pltpu.VMEM((2, tok, dim // 2), F32),
            dma((8,)), dma((4, 8)), dma((16,)), dma((16,)), dma((2, 16)), dma((2, 4)), dma((2, 8)), dma((2, 2)), dma((2, 4)), dma((2,)),
            dma((2,)), dma((2,)), dma((4, 2)), dma((4, 2)), dma((4, 2)), dma((2, 3, 2)), dma((2,)), dma((2,)), pltpu.SemaphoreType.REGULAR,
        ],
        compiler_params=pltpu.CompilerParams(collective_id=0, has_side_effects=True, vmem_limit_bytes=VMEM_LIMIT),
        cost_estimate=pl.CostEstimate(flops=16 * tok * 2 * dim * ff * 5, bytes_accessed=80_000_000, transcendentals=0),
    )(x_tokens, dy_tokens, table, w_gate, w_up, w_down, s_gate, s_up, s_down)


def up_grad_kernel(x, act, g1, g3):
    ff = g1.shape[2]
    both = dot_tn(x[0], act[0])
    g1[0] = both[:, :ff]
    g3[0] = both[:, ff:]


def up_grads(x, act):
    experts, rows, dim = x.shape
    ff = act.shape[2] // 2
    tile = min(512, dim)
    out = jax.ShapeDtypeStruct((experts, dim, ff), F32)
    return pl.pallas_call(
        up_grad_kernel,
        name='up_grads',
        out_shape=(out, out),
        grid=(experts, dim // tile),
        in_specs=[pl.BlockSpec((1, rows, tile), lambda e, i: (e, 0, i)), pl.BlockSpec((1, rows, 2 * ff), lambda e, i: (e, 0, 0))],
        out_specs=(pl.BlockSpec((1, tile, ff), lambda e, i: (e, i, 0)),) * 2,
        compiler_params=pltpu.CompilerParams(vmem_limit_bytes=60_000_000),
        cost_estimate=pl.CostEstimate(flops=4 * experts * rows * dim * ff, bytes_accessed=8 * experts * dim * ff + 2 * x.size + 2 * act.size, transcendentals=0),
    )(x, act)


def down_grad_kernel(hid, dz, g2):
    g2[0] = dot_tn(hid[0], dz[0])


def down_grads(hid, dz):
    experts, rows, dim = dz.shape
    ff = hid.shape[2]
    tile = min(512, dim)
    return pl.pallas_call(
        down_grad_kernel,
        name='down_grads',
        out_shape=jax.ShapeDtypeStruct((experts, ff, dim), F32),
        grid=(experts, dim // tile),
        in_specs=[pl.BlockSpec((1, rows, ff), lambda e, n: (e, 0, 0)), pl.BlockSpec((1, rows, tile), lambda e, n: (e, 0, n))],
        out_specs=pl.BlockSpec((1, ff, tile), lambda e, n: (e, 0, n)),
        compiler_params=pltpu.CompilerParams(vmem_limit_bytes=60_000_000),
        cost_estimate=pl.CostEstimate(flops=2 * experts * rows * dim * ff, bytes_accessed=4 * experts * dim * ff + 2 * hid.size + 2 * dz.size, transcendentals=0),
    )(hid, dz)


def shared_grad_kernel(x, dy, act, hid, g1, g3, g2):
    ff = hid.shape[1]
    both = dot_tn(x[...], act[...])
    g1[0] = both[:, :ff]
    g3[0] = both[:, ff:]
    g2[0] = dot_tn(hid[...], dy[...])


def shared_grads(x, dy, act, hid):
    tok, dim = x.shape
    ff = hid.shape[1]
    tile = min(512, dim)
    out = jax.ShapeDtypeStruct((1, dim, ff), F32)
    return pl.pallas_call(
        shared_grad_kernel,
        name='shared_grads',
        out_shape=(out, out, jax.ShapeDtypeStruct((1, ff, dim), F32)),
        grid=(dim // tile,),
        in_specs=[pl.BlockSpec((tok, tile), lambda i: (0, i)), pl.BlockSpec((tok, tile), lambda i: (0, i)), pl.BlockSpec((tok, 2 * ff), lambda i: (0, 0)), pl.BlockSpec((tok, ff), lambda i: (0, 0))],
        out_specs=(pl.BlockSpec((1, tile, ff), lambda i: (0, i, 0)),) * 2 + (pl.BlockSpec((1, ff, tile), lambda i: (0, 0, i)),),
        compiler_params=pltpu.CompilerParams(vmem_limit_bytes=60_000_000),
        cost_estimate=pl.CostEstimate(flops=6 * tok * dim * ff, bytes_accessed=12 * dim * ff + 4 * x.size, transcendentals=0),
    )(x, dy, act, hid)


def solution(mesh):
    group = mesh.shape['ep']
    token_spec = P(('dp', 'ep'), None)
    expert_spec = P('ep', None, None)
    whole_spec = P(None, None)
    grad_spec = P(('dp', 'ep'), None, None)

    def local_backward(x_tokens, dy_tokens, expert_ids, gate_vals, slot_pos, w_gate, w_up, w_down, shared_gate, shared_up, shared_down):
        tok, dim = x_tokens.shape
        local_experts = w_gate.shape[0]
        experts = jnp.arange(group * local_experts, dtype=jnp.int32)
        hit = (expert_ids.T[None] == experts[:, None, None]) & (slot_pos.T[None] >= 0)
        gates = jnp.sum(jnp.where(hit, gate_vals.T[None], 0.0), axis=1)
        slots = jnp.sum(jnp.where(hit, slot_pos.T[None].astype(F32) + 1.0, 0.0), axis=1) - 1.0
        table = jnp.concatenate([gates.reshape(group, local_experts, tok), slots.reshape(group, local_experts, tok), jnp.zeros((group, 8 - 2 * local_experts, tok), F32)], axis=1)
        grad_x, x_all, z_all, act_all, hid_all, sact, shid = routed(x_tokens, dy_tokens, table, w_gate, w_up, w_down, shared_gate, shared_up, shared_down)
        x_all, z_all, act_all, hid_all = [a.reshape(local_experts, -1, a.shape[-1]) for a in (x_all, z_all, act_all, hid_all)]
        grad_w_gate, grad_w_up = up_grads(x_all, act_all)
        grad_w_down = down_grads(hid_all, z_all)
        grad_shared_gate, grad_shared_up, grad_shared_down = shared_grads(x_tokens, dy_tokens, sact, shid)
        grad_x = grad_x.reshape(tok, dim)
        return grad_x, grad_w_gate, grad_w_up, grad_w_down, grad_shared_gate, grad_shared_up, grad_shared_down

    return jax.shard_map(local_backward, mesh=mesh, in_specs=(token_spec, token_spec, token_spec, token_spec, token_spec, expert_spec, expert_spec, expert_spec, whole_spec, whole_spec, whole_spec), out_specs=(token_spec, grad_spec, grad_spec, grad_spec, grad_spec, grad_spec, grad_spec), check_vma=False)
```

```python
import functools

import jax
import jax.numpy as jnp
from jax import lax
from jax.experimental import pallas as pl
from jax.experimental.pallas import tpu as pltpu
from jax.sharding import PartitionSpec as P

F32 = jnp.float32
BF16 = jnp.bfloat16
ANY = pl.BlockSpec(memory_space=pl.ANY)
VMEM = pl.BlockSpec(memory_space=pltpu.VMEM)
VMEM_LIMIT = 67_000_000


def dot_nn(a, b):
    return lax.dot_general(a, b, (((1,), (0,)), ((), ())), preferred_element_type=F32)


def dot_nt(a, b):
    return lax.dot_general(a, b, (((1,), (1,)), ((), ())), preferred_element_type=F32)


def dot_tn(a, b):
    return lax.dot_general(a, b, (((0,), (0,)), ((), ())), preferred_element_type=F32)


def swiglu_parts(act_gate, act_up, grad_hidden):
    gate_f32 = act_gate.astype(F32)
    up_f32 = act_up.astype(F32)
    sigma = jax.nn.sigmoid(gate_f32)
    silu_gate = gate_f32 * sigma
    hidden = (silu_gate * up_f32).astype(BF16)
    grad_gate = (grad_hidden * up_f32 * sigma * (1.0 + gate_f32 * (1.0 - sigma))).astype(BF16)
    grad_up = (grad_hidden * silu_gate).astype(BF16)
    return hidden, grad_gate, grad_up


END_PLAN = (
    'F10F11F20C00F40R00C10F30R10F41X00F21X10C20R20F31C30R30F50X20',
    'X30C40F51F60R40C50X40Y11F61R50C60R60X50S30F70F71X60C70R70Y21',
    'X70Y31E00Y20Y10S21S31Y01S20S11S10N00',
)
MID_PLAN = (
    'C00F10F30F20R00F31F11C10F50X00F60R10F21C20R20X10F51C30F61F40',
    'X20F41R30C40R40F70C50X30X40R50F71C60R60Y01X50C70S30Y11X60R70',
    'X70Y21E00S10Y31N00Y20S21S31Y00S20S11',
)


def gaps(text):
    found = [[]]
    for i in range(0, len(text), 3):
        token = text[i:i + 3]
        if token[0] in 'CR':
            found.append([])
        else:
            found[-1].append(token)
    return found


def routed_kernel(x_in, dy_in, table, w_gate, w_up, w_down, s_gate, s_up, s_down,
                  grad_x, x_all, z_all, act_all, hid_all, sact_out, shid_out,
                  xbuf, dybuf, tbuf, pick, w13, w2, act, hst, xst, zst, sact, shid, sdx,
                  sums, dsend, pbuf, ybuf, cbuf, ebuf,
                  load_sem, out_sem, gs_sem, gr_sem, recv_sem, sy_sem, sd_sem, sown_sem, sz_sem, sx_sem,
                  ds_sem, dr_sem, ys_sem, yr_sem, cs_sem, cr_sem, es_sem, er_sem, credit):
    tok, dim = x_in.shape
    ff = w2.shape[1]
    cap = xst.shape[2]
    half = dim // 2
    tile = min(512, dim)
    me = lax.axis_index('ep')
    z = lax.div(me, 4)
    y = lax.rem(lax.div(me, 2), 2)
    c = lax.rem(me, 2)
    partner = me + 1 - 2 * c
    side = me + 2 - 4 * y
    inner = z * (3 - z)
    near_end = lax.div(z, 2)
    far_end = 1 - near_end
    bufs = (xbuf, dybuf)
    own_slot = (0, 1, 3, 5)
    other_slot = (2, 4, 6, 7)
    near_first = [(own_slot.index(t), 0) if t in own_slot else (other_slot.index(t), 1) for t in range(8)]

    def bid(zz, yy, cc):
        return zz * 4 + yy * 2 + cc

    def order(k):
        near = lax.div(inner, 2)
        delta = lax.div((1 - k) * (2 - k) * (3 - k), 6) - lax.div(k * (2 - k) * (3 - k), 2)
        base = k + near * delta
        return base + near_end * (3 - 2 * base)

    def visit(t):
        u = t + lax.div(t, 7)
        odd = lax.rem(u, 2)
        first = lax.div(7 - t, 7)
        k = odd * lax.div(u + 1, 2) + (1 - odd) * (lax.div(u, 2) - 1) + first
        col = 1 - odd - first
        return order(k), y + col * (1 - 2 * y), col

    def remote(src, dst, send, recv, dev):
        return pltpu.make_async_remote_copy(src_ref=src, dst_ref=dst, send_sem=send, recv_sem=recv, device_id={'ep': dev}, device_id_type=pl.DeviceIdType.MESH)

    def weights(e, gate, up, down):
        return [pltpu.make_async_copy(gate, w13.at[e, :, pl.ds(0, ff)], load_sem.at[2 + 3 * e]),
                pltpu.make_async_copy(up, w13.at[e, :, pl.ds(ff, ff)], load_sem.at[3 + 3 * e]),
                pltpu.make_async_copy(down, w2.at[e], load_sem.at[4 + 3 * e])]

    own = [pltpu.make_async_copy(x_in, xbuf.at[me], load_sem.at[0]), pltpu.make_async_copy(dy_in, dybuf.at[me], load_sem.at[1])]
    shared_load = weights(1, s_gate, s_up, s_down)
    first_load = weights(0, w_gate.at[0], w_up.at[0], w_down.at[0])
    second_load = weights(1, w_gate.at[1], w_up.at[1], w_down.at[1])
    for cp in own + shared_load + first_load:
        cp.start()

    barrier = pltpu.get_barrier_semaphore()

    @pl.loop(1, 16)
    def _(d):
        pl.semaphore_signal(barrier, inc=1, device_id={'ep': lax.rem(me + d, 16)}, device_id_type=pl.DeviceIdType.MESH)
    pl.semaphore_wait(barrier, 15)

    def send_y(q, zb, b):
        return remote(bufs[q].at[b], bufs[q].at[b], sy_sem.at[q, zb], recv_sem.at[q, b], side)

    def send_d(q, zb, yb, b):
        return remote(bufs[q].at[b], bufs[q].at[b], sd_sem.at[q, zb * 2 + yb], recv_sem.at[q, b], partner)

    def send_own(q, up):
        return remote(bufs[q].at[me], bufs[q].at[me], sown_sem.at[q, up], recv_sem.at[q, me], me + (4 if up else -4))

    def send_fwd(q, zb, b, up):
        return remote(bufs[q].at[b], bufs[q].at[b], sz_sem.at[q, zb], recv_sem.at[q, b], me + (4 if up else -4))

    def send_end(b, up):
        return remote(xbuf.at[b], xbuf.at[b], sx_sem.at[1 - up], recv_sem.at[0, b], me + (4 if up else -4))

    for q in range(2):
        own[q].wait()
        send_y(q, z, me).start()

        @pl.when(z < 3)
        def _():
            send_own(q, 1).start()

        @pl.when(z > 0)
        def _():
            send_own(q, 0).start()
        send_d(q, z, y, me).start()

    def send_table(d):
        dest = lax.rem(me + d, 16)
        return remote(table.at[dest], tbuf.at[me], gs_sem.at[d], gr_sem.at[me], dest)

    @pl.loop(1, 16)
    def _(d):
        send_table(d).start()
    tbuf[me] = table[me]

    def place(t):
        k, col = near_first[t]
        return order(k), y + col * (1 - 2 * y), col

    def pass_on(t, q):
        zb, yb, col = place(t)
        b = bid(zb, yb, c)
        send_d(q, zb, yb, b).wait_recv()
        if col == 0:
            if q:
                send_y(q, zb, b).start()
            else:
                @pl.when(zb * (3 - zb) > 0)
                def _():
                    send_y(q, zb, b).start()

            @pl.when((zb > z) & (z > 0))
            def _():
                send_fwd(q, zb, b, 0).start()

            @pl.when((zb < z) & (z < 3))
            def _():
                send_fwd(q, zb, b, 1).start()
        elif q == 0:
            @pl.when((zb == 3) & (z > 0))
            def _():
                send_end(b, 0).start()

            @pl.when((zb == 0) & (z < 3))
            def _():
                send_end(b, 1).start()
        send_d(q, zb, yb, b).start()

    def flush(t, start):
        zb, yb, _ = visit(t)
        two = pl.ds(bid(zb, yb, 0), 2)
        cps = [pltpu.make_async_copy(xst, x_all.at[:, two], out_sem.at[0, t]),
               pltpu.make_async_copy(zst, z_all.at[:, two], out_sem.at[1, t]),
               pltpu.make_async_copy(hst, hid_all.at[:, two], out_sem.at[2, t]),
               pltpu.make_async_copy(act.at[:, two], act_all.at[:, two], out_sem.at[3, t])]
        if start:
            for cp in cps:
                cp.start()
        else:
            for cp in cps[:3]:
                cp.wait()

    def compute(t):
        zb, yb, _ = visit(t)
        b0 = bid(zb, yb, 0)
        bp = bid(zb, yb, 1 - c)
        for q in range(2):
            send_d(q, zb, yb, bp).wait_recv()
        for p in range(2):
            @pl.when(b0 + p != me)
            def _():
                remote(table.at[0], tbuf.at[b0 + p], gs_sem.at[0], gr_sem.at[b0 + p], partner).wait_recv()

        @pl.when(t > 0)
        def _():
            flush(t - 1, False)
        row = lax.broadcasted_iota(jnp.int32, (2 * cap, tok), 0).astype(F32)
        for p in range(2):
            info = tbuf[b0 + p]
            top = row < cap
            chosen = jnp.where(top, info[2:3, :], info[3:4, :] + cap) == row
            gate = jnp.sum(jnp.where(chosen, jnp.where(top, info[0:1, :], info[1:2, :]), 0.0), axis=1, keepdims=True)
            sel = chosen.astype(BF16)
            pick[b0 + p] = sel
            for n in range(dim // tile):
                cols = slice(n * tile, (n + 1) * tile)
                xr = dot_nn(sel, xbuf[b0 + p, :, cols]).astype(BF16)
                zr = (dot_nn(sel, dybuf[b0 + p, :, cols]) * gate).astype(BF16)
                for e in range(2):
                    xst[e, p, :, cols] = xr[e * cap:(e + 1) * cap]
                    zst[e, p, :, cols] = zr[e * cap:(e + 1) * cap]
        two = pl.ds(b0, 2)
        for e in range(2):
            ab = dot_nn(xst[e].reshape(2 * cap, dim), w13[e]).astype(BF16)
            grad_hidden = dot_nt(zst[e].reshape(2 * cap, dim), w2[e])
            hidden, grad_gate, grad_up = swiglu_parts(ab[:, :ff], ab[:, ff:], grad_hidden)
            hst[e] = hidden.reshape(2, cap, ff)
            act[e, two, :, :ff] = grad_gate.reshape(2, cap, ff)
            act[e, two, :, ff:] = grad_up.reshape(2, cap, ff)
        flush(t, True)

    for cp in shared_load:
        cp.wait()
    ab = dot_nn(xbuf[me], w13[1]).astype(BF16)
    hidden, grad_gate, grad_up = swiglu_parts(ab[:, :ff], ab[:, ff:], dot_nt(dybuf[me], w2[1]))
    shid[...] = hidden
    sact[:, :ff] = grad_gate
    sact[:, ff:] = grad_up
    for n in range(dim // tile):
        cols = slice(n * tile, (n + 1) * tile)
        sdx[:, cols] = dot_nt(sact[...], w13[1, cols, :])
    shared_out = [pltpu.make_async_copy(sact, sact_out, load_sem.at[0]), pltpu.make_async_copy(shid, shid_out, load_sem.at[1])]
    for cp in shared_out + second_load:
        cp.start()
    for cp in first_load + second_load:
        cp.wait()
    def give(j):
        return remote(dsend.at[lax.rem(j, 2)], pbuf.at[lax.rem(j, 2)], ds_sem.at[lax.rem(j, 2)], dr_sem.at[lax.rem(j, 2)], partner)

    def part(h):
        return pl.ds(h * half, half)

    def rs_y(j, zb, h):
        return remote(sums.at[j, :, part(h)], ybuf.at[zb, :, part(h)], ys_sem.at[zb, h], yr_sem.at[zb, h], side)

    def rs_end(j, end):
        return remote(sums.at[j, :, part(0)], ebuf.at[end], es_sem.at[end], er_sem.at[end], me + 8 * end - 4)

    def rs_compute(j):
        zb, yb, _ = visit(j)
        b = bid(zb, yb, c)
        bp = bid(zb, yb, 1 - c)

        @pl.when(j >= 2)
        def _():
            give(j).wait_send()

        @pl.loop(0, dim // tile)
        def _(n):
            cols = pl.ds(pl.multiple_of(n * tile, tile), tile)
            r = [dot_nt(jnp.concatenate([act[e, b], act[e, bp]], axis=0), w13[e, cols, :]).astype(BF16) for e in range(2)]
            sums[j, :, cols] = dot_tn(pick[b], jnp.concatenate([r[0][:cap], r[1][:cap]], axis=0))
            dsend[lax.rem(j, 2), :, cols] = dot_tn(pick[bp], jnp.concatenate([r[0][cap:], r[1][cap:]], axis=0))

        @pl.when(j >= 2)
        def _():
            pl.semaphore_wait(credit, 1)
        give(j).start()

    def rs_finish(j):
        give(j).wait_recv()
        sums[j] = sums[j] + pbuf[j % 2]
        if j < 6:
            pl.semaphore_signal(credit, inc=1, device_id={'ep': partner}, device_id_type=pl.DeviceIdType.MESH)

    def end_in(j, end):
        rs_end(j, end).wait_recv()
        sums[j, :, part(0)] = sums[j, :, part(0)] + ebuf[end]

    def chain(k, h, zb, up):
        j = own_slot[k]
        slot, gap = (0, zb - z - 1) if up else (1, z - zb - 1)
        return remote(sums.at[j, :, part(h)], cbuf.at[slot, gap, :, part(h)], cs_sem.at[k, h], cr_sem.at[slot, gap, h], me + (4 if up else -4))

    def chain_in(j, h, slot, gap):
        remote(sums.at[j, :, part(h)], cbuf.at[slot, gap, :, part(h)], cs_sem.at[0, h], cr_sem.at[slot, gap, h], partner).wait_recv()
        sums[j, :, part(h)] = sums[j, :, part(h)] + cbuf[slot, gap, :, part(h)]

    def y_in(j, zb, h):
        rs_y(0, zb, h).wait_recv()
        sums[j, :, part(h)] = sums[j, :, part(h)] + ybuf[zb, :, part(h)]

    def step(k, h, mid):
        zb = order(k)
        j = own_slot[k]
        if h or k == 2 or (k == 1 and not mid):
            y_in(j, zb, h)

        @pl.when(zb > z)
        def _():
            if mid:
                chain_in(j, h, 0, zb - z)
            chain(k, h, zb, True).start()

        @pl.when(zb < z)
        def _():
            if mid:
                chain_in(j, h, 1, z - zb)
            chain(k, h, zb, False).start()

    def act_on(token, mid):
        kind, k, h = token[0], int(token[1]), int(token[2])
        if kind == 'F':
            pass_on(k, h)
        elif kind == 'X':
            rs_finish(k)
        elif kind == 'Y':
            rs_y(other_slot[k], order(k), h).start()
        elif kind == 'S':
            step(k, h, mid)
        elif kind == 'E':
            if mid:
                end_in(other_slot[3], far_end)
            rs_end(other_slot[3], far_end).start()
        elif mid:
            end_in(other_slot[1], near_end)
            rs_end(other_slot[1], near_end).start()
        else:
            end_in(other_slot[0], near_end)
            rs_y(other_slot[0], z, 0).start()

    plans = [gaps(''.join(rows)) for rows in (END_PLAN, MID_PLAN)]

    def between(t, gap):
        for mid in range(2):
            tokens = plans[mid][gap]
            if tokens:
                @pl.when((t == gap // 2) & ((inner > 0) if mid else (inner == 0)))
                def _():
                    for token in tokens:
                        act_on(token, mid)

    @pl.loop(0, 8)
    def _(t):
        for g in range(8):
            between(t, 2 * g)
        compute(t)
        for g in range(8):
            between(t, 2 * g + 1)
        rs_compute(t)

    between(8, 16)
    flush(7, False)
    for h in (1, 0):
        @pl.when(z > 0)
        def _():
            chain_in(0, h, 0, 0)

        @pl.when(z < 3)
        def _():
            chain_in(0, h, 1, 0)
        rs_y(0, z, h).wait_recv()
        total = sums[0, :, part(h)] + ybuf[z, :, part(h)] + sdx[:, part(h)]
        xst[0, :, :, part(h)] = total.astype(BF16).reshape(2, cap, half)
    result = pltpu.make_async_copy(xst.at[0], grad_x, load_sem.at[2])
    result.start()

    for cp in shared_out:
        cp.wait()
    for t in range(8):
        pltpu.make_async_copy(act.at[:, pl.ds(0, 2)], act_all.at[:, pl.ds(0, 2)], out_sem.at[3, t]).wait()
    for zb in range(4):
        for q in range(2):
            if q or zb in (1, 2):
                send_y(q, zb, 0).wait_send()
            else:
                @pl.when(z == zb)
                def _():
                    send_y(q, zb, 0).wait_send()
            for yb in range(2):
                send_d(q, zb, yb, 0).wait_send()

            @pl.when(((zb > z) & (z > 0)) | ((zb < z) & (z < 3)))
            def _():
                send_fwd(q, zb, 0, 1).wait_send()
        for h in range(2):
            if h or zb in (1, 2):
                rs_y(0, zb, h).wait_send()
            else:
                @pl.when(z == zb)
                def _():
                    rs_y(0, zb, h).wait_send()
            if zb:
                remote(sums.at[0, :, part(h)], cbuf.at[0, 0, :, part(h)], cs_sem.at[zb, h], cr_sem.at[0, 0, h], partner).wait_send()

    @pl.when(z < 3)
    def _():
        send_end(0, 1).wait_send()
        for q in range(2):
            send_own(q, 1).wait_send()

    @pl.when(z > 0)
    def _():
        send_end(0, 0).wait_send()
        for q in range(2):
            send_own(q, 0).wait_send()
    rs_end(0, far_end).wait_send()

    @pl.when(inner > 0)
    def _():
        rs_end(0, near_end).wait_send()

    @pl.loop(1, 16)
    def _(d):
        send_table(d).wait_send()
    for j in range(2):
        give(j).wait_send()
    result.wait()


def routed(x_tokens, dy_tokens, table, w_gate, w_up, w_down, s_gate, s_up, s_down):
    tok, dim = x_tokens.shape
    ff = w_gate.shape[2]
    cap = tok // 2
    dma = pltpu.SemaphoreType.DMA
    shape = jax.ShapeDtypeStruct
    return pl.pallas_call(
        routed_kernel,
        name='routed',
        out_shape=(shape((2, cap, dim), BF16), shape((2, 16, cap, dim), BF16), shape((2, 16, cap, dim), BF16),
                   shape((2, 16, cap, 2 * ff), BF16), shape((2, 16, cap, ff), BF16), shape((tok, 2 * ff), BF16), shape((tok, ff), BF16)),
        in_specs=[ANY, ANY, VMEM] + [ANY] * 6,
        out_specs=(ANY,) * 7,
        scratch_shapes=[
            pltpu.VMEM((16, tok, dim), BF16), pltpu.VMEM((16, tok, dim), BF16), pltpu.VMEM((16, 8, tok), F32), pltpu.VMEM((16, 2 * cap, tok), BF16),
            pltpu.VMEM((2, dim, 2 * ff), BF16), pltpu.VMEM((2, ff, dim), BF16),
            pltpu.VMEM((2, 16, cap, 2 * ff), BF16), pltpu.VMEM((2, 2, cap, ff), BF16), pltpu.VMEM((2, 2, cap, dim), BF16), pltpu.VMEM((2, 2, cap, dim), BF16),
            pltpu.VMEM((tok, 2 * ff), BF16), pltpu.VMEM((tok, ff), BF16), pltpu.VMEM((tok, dim), F32),
            pltpu.VMEM((8, tok, dim), F32), pltpu.VMEM((2, tok, dim), F32), pltpu.VMEM((2, tok, dim), F32),
            pltpu.VMEM((4, tok, dim), F32), pltpu.VMEM((2, 3, tok, dim), F32), pltpu.VMEM((2, tok, dim // 2), F32),
            dma((8,)), dma((4, 8)), dma((16,)), dma((16,)), dma((2, 16)), dma((2, 4)), dma((2, 8)), dma((2, 2)), dma((2, 4)), dma((2,)),
            dma((2,)), dma((2,)), dma((4, 2)), dma((4, 2)), dma((4, 2)), dma((2, 3, 2)), dma((2,)), dma((2,)), pltpu.SemaphoreType.REGULAR,
        ],
        compiler_params=pltpu.CompilerParams(collective_id=0, has_side_effects=True, vmem_limit_bytes=VMEM_LIMIT),
        cost_estimate=pl.CostEstimate(flops=16 * tok * 2 * dim * ff * 5, bytes_accessed=80_000_000, transcendentals=0),
    )(x_tokens, dy_tokens, table, w_gate, w_up, w_down, s_gate, s_up, s_down)


def up_grad_kernel(x, act, g1, g3):
    ff = g1.shape[2]
    both = dot_tn(x[0], act[0])
    g1[0] = both[:, :ff]
    g3[0] = both[:, ff:]


def up_grads(x, act):
    experts, rows, dim = x.shape
    ff = act.shape[2] // 2
    tile = min(512, dim)
    out = jax.ShapeDtypeStruct((experts, dim, ff), F32)
    return pl.pallas_call(
        up_grad_kernel,
        name='up_grads',
        out_shape=(out, out),
        grid=(experts, dim // tile),
        in_specs=[pl.BlockSpec((1, rows, tile), lambda e, i: (e, 0, i)), pl.BlockSpec((1, rows, 2 * ff), lambda e, i: (e, 0, 0))],
        out_specs=(pl.BlockSpec((1, tile, ff), lambda e, i: (e, i, 0)),) * 2,
        compiler_params=pltpu.CompilerParams(vmem_limit_bytes=60_000_000),
        cost_estimate=pl.CostEstimate(flops=4 * experts * rows * dim * ff, bytes_accessed=8 * experts * dim * ff + 2 * x.size + 2 * act.size, transcendentals=0),
    )(x, act)


def down_grad_kernel(hid, dz, g2):
    g2[0] = dot_tn(hid[0], dz[0])


def down_grads(hid, dz):
    experts, rows, dim = dz.shape
    ff = hid.shape[2]
    tile = min(512, dim)
    return pl.pallas_call(
        down_grad_kernel,
        name='down_grads',
        out_shape=jax.ShapeDtypeStruct((experts, ff, dim), F32),
        grid=(experts, dim // tile),
        in_specs=[pl.BlockSpec((1, rows, ff), lambda e, n: (e, 0, 0)), pl.BlockSpec((1, rows, tile), lambda e, n: (e, 0, n))],
        out_specs=pl.BlockSpec((1, ff, tile), lambda e, n: (e, 0, n)),
        compiler_params=pltpu.CompilerParams(vmem_limit_bytes=60_000_000),
        cost_estimate=pl.CostEstimate(flops=2 * experts * rows * dim * ff, bytes_accessed=4 * experts * dim * ff + 2 * hid.size + 2 * dz.size, transcendentals=0),
    )(hid, dz)


def shared_grad_kernel(x, dy, act, hid, g1, g3, g2):
    ff = hid.shape[1]
    both = dot_tn(x[...], act[...])
    g1[0] = both[:, :ff]
    g3[0] = both[:, ff:]
    g2[0] = dot_tn(hid[...], dy[...])


def shared_grads(x, dy, act, hid):
    tok, dim = x.shape
    ff = hid.shape[1]
    tile = min(512, dim)
    out = jax.ShapeDtypeStruct((1, dim, ff), F32)
    return pl.pallas_call(
        shared_grad_kernel,
        name='shared_grads',
        out_shape=(out, out, jax.ShapeDtypeStruct((1, ff, dim), F32)),
        grid=(dim // tile,),
        in_specs=[pl.BlockSpec((tok, tile), lambda i: (0, i)), pl.BlockSpec((tok, tile), lambda i: (0, i)), pl.BlockSpec((tok, 2 * ff), lambda i: (0, 0)), pl.BlockSpec((tok, ff), lambda i: (0, 0))],
        out_specs=(pl.BlockSpec((1, tile, ff), lambda i: (0, i, 0)),) * 2 + (pl.BlockSpec((1, ff, tile), lambda i: (0, 0, i)),),
        compiler_params=pltpu.CompilerParams(vmem_limit_bytes=60_000_000),
        cost_estimate=pl.CostEstimate(flops=6 * tok * dim * ff, bytes_accessed=12 * dim * ff + 4 * x.size, transcendentals=0),
    )(x, dy, act, hid)


def solution(mesh):
    group = mesh.shape['ep']
    token_spec = P(('dp', 'ep'), None)
    expert_spec = P('ep', None, None)
    whole_spec = P(None, None)
    grad_spec = P(('dp', 'ep'), None, None)

    def local_backward(x_tokens, dy_tokens, expert_ids, gate_vals, slot_pos, w_gate, w_up, w_down, shared_gate, shared_up, shared_down):
        tok, dim = x_tokens.shape
        local_experts = w_gate.shape[0]
        experts = jnp.arange(group * local_experts, dtype=jnp.int32)
        hit = (expert_ids.T[None] == experts[:, None, None]) & (slot_pos.T[None] >= 0)
        gates = jnp.sum(jnp.where(hit, gate_vals.T[None], 0.0), axis=1)
        slots = jnp.sum(jnp.where(hit, slot_pos.T[None].astype(F32) + 1.0, 0.0), axis=1) - 1.0
        table = jnp.concatenate([gates.reshape(group, local_experts, tok), slots.reshape(group, local_experts, tok), jnp.zeros((group, 8 - 2 * local_experts, tok), F32)], axis=1)
        grad_x, x_all, z_all, act_all, hid_all, sact, shid = routed(x_tokens, dy_tokens, table, w_gate, w_up, w_down, shared_gate, shared_up, shared_down)
        x_all, z_all, act_all, hid_all = [a.reshape(local_experts, -1, a.shape[-1]) for a in (x_all, z_all, act_all, hid_all)]
        grad_w_gate, grad_w_up = up_grads(x_all, act_all)
        grad_w_down = down_grads(hid_all, z_all)
        grad_shared_gate, grad_shared_up, grad_shared_down = shared_grads(x_tokens, dy_tokens, sact, shid)
        grad_x = grad_x.reshape(tok, dim)
        return grad_x, grad_w_gate, grad_w_up, grad_w_down, grad_shared_gate, grad_shared_up, grad_shared_down

    return jax.shard_map(local_backward, mesh=mesh, in_specs=(token_spec, token_spec, token_spec, token_spec, token_spec, expert_spec, expert_spec, expert_spec, whole_spec, whole_spec, whole_spec), out_specs=(token_spec, grad_spec, grad_spec, grad_spec, grad_spec, grad_spec, grad_spec), check_vma=False)
```

```python
import functools

import jax
import jax.numpy as jnp
from jax import lax
from jax.experimental import pallas as pl
from jax.experimental.pallas import tpu as pltpu
from jax.sharding import PartitionSpec as P

F32 = jnp.float32
BF16 = jnp.bfloat16
ANY = pl.BlockSpec(memory_space=pl.ANY)
VMEM = pl.BlockSpec(memory_space=pltpu.VMEM)
VMEM_LIMIT = 67_000_000


def dot_nn(a, b):
    return lax.dot_general(a, b, (((1,), (0,)), ((), ())), preferred_element_type=F32)


def dot_nt(a, b):
    return lax.dot_general(a, b, (((1,), (1,)), ((), ())), preferred_element_type=F32)


def dot_tn(a, b):
    return lax.dot_general(a, b, (((0,), (0,)), ((), ())), preferred_element_type=F32)


def swiglu_parts(act_gate, act_up, grad_hidden):
    gate_f32 = act_gate.astype(F32)
    up_f32 = act_up.astype(F32)
    sigma = jax.nn.sigmoid(gate_f32)
    silu_gate = gate_f32 * sigma
    hidden = (silu_gate * up_f32).astype(BF16)
    grad_gate = (grad_hidden * up_f32 * sigma * (1.0 + gate_f32 * (1.0 - sigma))).astype(BF16)
    grad_up = (grad_hidden * silu_gate).astype(BF16)
    return hidden, grad_gate, grad_up


END_PLAN = (
    'F10F11F20C00F40R00C10F30R10F41X00F21X10C20R20F31C30R30F50X20',
    'X30C40F51F60R40C50X40Y11F61R50C60R60X50S30F70F71X60C70R70Y21',
    'X70Y31E00Y20Y10S21S31Y01S20S11S10N00',
)
MID_PLAN = (
    'C00F10F30F20R00F31F11C10F50X00F60R10F21C20R20X10F51C30F61F40',
    'X20F41R30C40R40F70C50X30X40R50F71C60R60Y01X50C70S30Y11X60R70',
    'X70Y21E00S10Y31N00Y20S21S31Y00S20S11',
)


def gaps(text):
    found = [[]]
    for i in range(0, len(text), 3):
        token = text[i:i + 3]
        if token[0] in 'CR':
            found.append([])
        else:
            found[-1].append(token)
    return found


def routed_kernel(x_in, dy_in, ids, gates, slots, w_gate, w_up, w_down, s_gate, s_up, s_down,
                  grad_x, x_all, z_all, act_all, hid_all, sact_out, shid_out,
                  xbuf, dybuf, tbuf, table, pick, w13, w2, act, hst, xst, zst, sact, shid, sdx,
                  sums, dsend, pbuf, ybuf, cbuf, ebuf,
                  load_sem, out_sem, gs_sem, gr_sem, recv_sem, sy_sem, sd_sem, sown_sem, sz_sem, sx_sem,
                  ds_sem, dr_sem, ys_sem, yr_sem, cs_sem, cr_sem, es_sem, er_sem, credit):
    tok, dim = x_in.shape
    ff = w2.shape[1]
    cap = xst.shape[2]
    half = dim // 2
    tile = min(512, dim)
    me = lax.axis_index('ep')
    z = lax.div(me, 4)
    y = lax.rem(lax.div(me, 2), 2)
    c = lax.rem(me, 2)
    partner = me + 1 - 2 * c
    side = me + 2 - 4 * y
    inner = z * (3 - z)
    near_end = lax.div(z, 2)
    far_end = 1 - near_end
    bufs = (xbuf, dybuf)
    own_slot = (0, 1, 3, 5)
    other_slot = (2, 4, 6, 7)
    near_first = [(own_slot.index(t), 0) if t in own_slot else (other_slot.index(t), 1) for t in range(8)]

    def bid(zz, yy, cc):
        return zz * 4 + yy * 2 + cc

    def order(k):
        near = lax.div(inner, 2)
        delta = lax.div((1 - k) * (2 - k) * (3 - k), 6) - lax.div(k * (2 - k) * (3 - k), 2)
        base = k + near * delta
        return base + near_end * (3 - 2 * base)

    def visit(t):
        u = t + lax.div(t, 7)
        odd = lax.rem(u, 2)
        first = lax.div(7 - t, 7)
        k = odd * lax.div(u + 1, 2) + (1 - odd) * (lax.div(u, 2) - 1) + first
        col = 1 - odd - first
        return order(k), y + col * (1 - 2 * y), col

    def remote(src, dst, send, recv, dev):
        return pltpu.make_async_remote_copy(src_ref=src, dst_ref=dst, send_sem=send, recv_sem=recv, device_id={'ep': dev}, device_id_type=pl.DeviceIdType.MESH)

    def weights(e, gate, up, down):
        return [pltpu.make_async_copy(gate, w13.at[e, :, pl.ds(0, ff)], load_sem.at[2 + 3 * e]),
                pltpu.make_async_copy(up, w13.at[e, :, pl.ds(ff, ff)], load_sem.at[3 + 3 * e]),
                pltpu.make_async_copy(down, w2.at[e], load_sem.at[4 + 3 * e])]

    own = [pltpu.make_async_copy(x_in, xbuf.at[me], load_sem.at[0]), pltpu.make_async_copy(dy_in, dybuf.at[me], load_sem.at[1])]
    shared_load = weights(1, s_gate, s_up, s_down)
    first_load = weights(0, w_gate.at[0], w_up.at[0], w_down.at[0])
    second_load = weights(1, w_gate.at[1], w_up.at[1], w_down.at[1])
    for cp in own + shared_load + first_load:
        cp.start()

    barrier = pltpu.get_barrier_semaphore()

    @pl.loop(1, 16)
    def _(d):
        pl.semaphore_signal(barrier, inc=1, device_id={'ep': lax.rem(me + d, 16)}, device_id_type=pl.DeviceIdType.MESH)
    pl.semaphore_wait(barrier, 15)

    def send_y(q, zb, b):
        return remote(bufs[q].at[b], bufs[q].at[b], sy_sem.at[q, zb], recv_sem.at[q, b], side)

    def send_d(q, zb, yb, b):
        return remote(bufs[q].at[b], bufs[q].at[b], sd_sem.at[q, zb * 2 + yb], recv_sem.at[q, b], partner)

    def send_own(q, up):
        return remote(bufs[q].at[me], bufs[q].at[me], sown_sem.at[q, up], recv_sem.at[q, me], me + (4 if up else -4))

    def send_fwd(q, zb, b, up):
        return remote(bufs[q].at[b], bufs[q].at[b], sz_sem.at[q, zb], recv_sem.at[q, b], me + (4 if up else -4))

    def send_end(b, up):
        return remote(xbuf.at[b], xbuf.at[b], sx_sem.at[1 - up], recv_sem.at[0, b], me + (4 if up else -4))

    for q in range(2):
        own[q].wait()
        send_y(q, z, me).start()

        @pl.when(z < 3)
        def _():
            send_own(q, 1).start()

        @pl.when(z > 0)
        def _():
            send_own(q, 0).start()
        send_d(q, z, y, me).start()

    kept = jnp.where(slots[...] >= 0, ids[...], -1)
    slot_f32 = slots[...].astype(F32) + 1.0
    for dev in range(16):
        hits = [kept == 2 * dev + e for e in range(2)]
        rows = [jnp.sum(jnp.where(hit, gates[...], 0.0), axis=0, keepdims=True) for hit in hits]
        rows += [jnp.sum(jnp.where(hit, slot_f32, 0.0), axis=0, keepdims=True) - 1.0 for hit in hits]
        table[dev] = jnp.concatenate(rows + [jnp.zeros((4, tok), F32)], axis=0)

    def send_table(d):
        dest = lax.rem(me + d, 16)
        return remote(table.at[dest], tbuf.at[me], gs_sem.at[d], gr_sem.at[me], dest)

    @pl.loop(1, 16)
    def _(d):
        send_table(d).start()
    tbuf[me] = table[me]

    def place(t):
        k, col = near_first[t]
        return order(k), y + col * (1 - 2 * y), col

    def pass_on(t, q):
        zb, yb, col = place(t)
        b = bid(zb, yb, c)
        send_d(q, zb, yb, b).wait_recv()
        if col == 0:
            if q:
                send_y(q, zb, b).start()
            else:
                @pl.when(zb * (3 - zb) > 0)
                def _():
                    send_y(q, zb, b).start()

            @pl.when((zb > z) & (z > 0))
            def _():
                send_fwd(q, zb, b, 0).start()

            @pl.when((zb < z) & (z < 3))
            def _():
                send_fwd(q, zb, b, 1).start()
        elif q == 0:
            @pl.when((zb == 3) & (z > 0))
            def _():
                send_end(b, 0).start()

            @pl.when((zb == 0) & (z < 3))
            def _():
                send_end(b, 1).start()
        send_d(q, zb, yb, b).start()

    def flush(t, start):
        zb, yb, _ = visit(t)
        two = pl.ds(bid(zb, yb, 0), 2)
        cps = [pltpu.make_async_copy(xst, x_all.at[:, two], out_sem.at[0, t]),
               pltpu.make_async_copy(zst, z_all.at[:, two], out_sem.at[1, t]),
               pltpu.make_async_copy(hst, hid_all.at[:, two], out_sem.at[2, t]),
               pltpu.make_async_copy(act.at[:, two], act_all.at[:, two], out_sem.at[3, t])]
        if start:
            for cp in cps:
                cp.start()
        else:
            for cp in cps[:3]:
                cp.wait()

    def compute(t):
        zb, yb, _ = visit(t)
        b0 = bid(zb, yb, 0)
        bp = bid(zb, yb, 1 - c)
        for q in range(2):
            send_d(q, zb, yb, bp).wait_recv()
        for p in range(2):
            @pl.when(b0 + p != me)
            def _():
                remote(table.at[0], tbuf.at[b0 + p], gs_sem.at[0], gr_sem.at[b0 + p], partner).wait_recv()

        @pl.when(t > 0)
        def _():
            flush(t - 1, False)
        row = lax.broadcasted_iota(jnp.int32, (2 * cap, tok), 0).astype(F32)
        for p in range(2):
            info = tbuf[b0 + p]
            top = row < cap
            chosen = jnp.where(top, info[2:3, :], info[3:4, :] + cap) == row
            gate = jnp.sum(jnp.where(chosen, jnp.where(top, info[0:1, :], info[1:2, :]), 0.0), axis=1, keepdims=True)
            sel = chosen.astype(BF16)
            pick[b0 + p] = sel
            for n in range(dim // tile):
                cols = slice(n * tile, (n + 1) * tile)
                xr = dot_nn(sel, xbuf[b0 + p, :, cols]).astype(BF16)
                zr = (dot_nn(sel, dybuf[b0 + p, :, cols]) * gate).astype(BF16)
                for e in range(2):
                    xst[e, p, :, cols] = xr[e * cap:(e + 1) * cap]
                    zst[e, p, :, cols] = zr[e * cap:(e + 1) * cap]
        two = pl.ds(b0, 2)
        for e in range(2):
            ab = dot_nn(xst[e].reshape(2 * cap, dim), w13[e]).astype(BF16)
            grad_hidden = dot_nt(zst[e].reshape(2 * cap, dim), w2[e])
            hidden, grad_gate, grad_up = swiglu_parts(ab[:, :ff], ab[:, ff:], grad_hidden)
            hst[e] = hidden.reshape(2, cap, ff)
            act[e, two, :, :ff] = grad_gate.reshape(2, cap, ff)
            act[e, two, :, ff:] = grad_up.reshape(2, cap, ff)
        flush(t, True)

    for cp in shared_load:
        cp.wait()
    ab = dot_nn(xbuf[me], w13[1]).astype(BF16)
    hidden, grad_gate, grad_up = swiglu_parts(ab[:, :ff], ab[:, ff:], dot_nt(dybuf[me], w2[1]))
    shid[...] = hidden
    sact[:, :ff] = grad_gate
    sact[:, ff:] = grad_up
    for n in range(dim // tile):
        cols = slice(n * tile, (n + 1) * tile)
        sdx[:, cols] = dot_nt(sact[...], w13[1, cols, :])
    shared_out = [pltpu.make_async_copy(sact, sact_out, load_sem.at[0]), pltpu.make_async_copy(shid, shid_out, load_sem.at[1])]
    for cp in shared_out + second_load:
        cp.start()
    for cp in first_load + second_load:
        cp.wait()
    def give(j):
        return remote(dsend.at[lax.rem(j, 2)], pbuf.at[lax.rem(j, 2)], ds_sem.at[lax.rem(j, 2)], dr_sem.at[lax.rem(j, 2)], partner)

    def part(h):
        return pl.ds(h * half, half)

    def rs_y(j, zb, h):
        return remote(sums.at[j, :, part(h)], ybuf.at[zb, :, part(h)], ys_sem.at[zb, h], yr_sem.at[zb, h], side)

    def rs_end(j, end):
        return remote(sums.at[j, :, part(0)], ebuf.at[end], es_sem.at[end], er_sem.at[end], me + 8 * end - 4)

    def rs_compute(j):
        zb, yb, _ = visit(j)
        b = bid(zb, yb, c)
        bp = bid(zb, yb, 1 - c)

        @pl.when(j >= 2)
        def _():
            give(j).wait_send()

        @pl.loop(0, dim // tile)
        def _(n):
            cols = pl.ds(pl.multiple_of(n * tile, tile), tile)
            r = [dot_nt(jnp.concatenate([act[e, b], act[e, bp]], axis=0), w13[e, cols, :]).astype(BF16) for e in range(2)]
            sums[j, :, cols] = dot_tn(pick[b], jnp.concatenate([r[0][:cap], r[1][:cap]], axis=0))
            dsend[lax.rem(j, 2), :, cols] = dot_tn(pick[bp], jnp.concatenate([r[0][cap:], r[1][cap:]], axis=0))

        @pl.when(j >= 2)
        def _():
            pl.semaphore_wait(credit, 1)
        give(j).start()

    def rs_finish(j):
        give(j).wait_recv()
        sums[j] = sums[j] + pbuf[j % 2]
        if j < 6:
            pl.semaphore_signal(credit, inc=1, device_id={'ep': partner}, device_id_type=pl.DeviceIdType.MESH)

    def end_in(j, end):
        rs_end(j, end).wait_recv()
        sums[j, :, part(0)] = sums[j, :, part(0)] + ebuf[end]

    def chain(k, h, zb, up):
        j = own_slot[k]
        slot, gap = (0, zb - z - 1) if up else (1, z - zb - 1)
        return remote(sums.at[j, :, part(h)], cbuf.at[slot, gap, :, part(h)], cs_sem.at[k, h], cr_sem.at[slot, gap, h], me + (4 if up else -4))

    def chain_in(j, h, slot, gap):
        remote(sums.at[j, :, part(h)], cbuf.at[slot, gap, :, part(h)], cs_sem.at[0, h], cr_sem.at[slot, gap, h], partner).wait_recv()
        sums[j, :, part(h)] = sums[j, :, part(h)] + cbuf[slot, gap, :, part(h)]

    def y_in(j, zb, h):
        rs_y(0, zb, h).wait_recv()
        sums[j, :, part(h)] = sums[j, :, part(h)] + ybuf[zb, :, part(h)]

    def step(k, h, mid):
        zb = order(k)
        j = own_slot[k]
        if h or k == 2 or (k == 1 and not mid):
            y_in(j, zb, h)

        @pl.when(zb > z)
        def _():
            if mid:
                chain_in(j, h, 0, zb - z)
            chain(k, h, zb, True).start()

        @pl.when(zb < z)
        def _():
            if mid:
                chain_in(j, h, 1, z - zb)
            chain(k, h, zb, False).start()

    def act_on(token, mid):
        kind, k, h = token[0], int(token[1]), int(token[2])
        if kind == 'F':
            pass_on(k, h)
        elif kind == 'X':
            rs_finish(k)
        elif kind == 'Y':
            rs_y(other_slot[k], order(k), h).start()
        elif kind == 'S':
            step(k, h, mid)
        elif kind == 'E':
            if mid:
                end_in(other_slot[3], far_end)
            rs_end(other_slot[3], far_end).start()
        elif mid:
            end_in(other_slot[1], near_end)
            rs_end(other_slot[1], near_end).start()
        else:
            end_in(other_slot[0], near_end)
            rs_y(other_slot[0], z, 0).start()

    plans = [gaps(''.join(rows)) for rows in (END_PLAN, MID_PLAN)]

    def between(t, gap):
        for mid in range(2):
            tokens = plans[mid][gap]
            if tokens:
                @pl.when((t == gap // 2) & ((inner > 0) if mid else (inner == 0)))
                def _():
                    for token in tokens:
                        act_on(token, mid)

    @pl.loop(0, 8)
    def _(t):
        for g in range(8):
            between(t, 2 * g)
        compute(t)
        for g in range(8):
            between(t, 2 * g + 1)
        rs_compute(t)

    between(8, 16)
    flush(7, False)
    for h in (1, 0):
        @pl.when(z > 0)
        def _():
            chain_in(0, h, 0, 0)

        @pl.when(z < 3)
        def _():
            chain_in(0, h, 1, 0)
        rs_y(0, z, h).wait_recv()
        total = sums[0, :, part(h)] + ybuf[z, :, part(h)] + sdx[:, part(h)]
        xst[0, :, :, part(h)] = total.astype(BF16).reshape(2, cap, half)
    result = pltpu.make_async_copy(xst.at[0], grad_x, load_sem.at[2])
    result.start()

    for cp in shared_out:
        cp.wait()
    for t in range(8):
        pltpu.make_async_copy(act.at[:, pl.ds(0, 2)], act_all.at[:, pl.ds(0, 2)], out_sem.at[3, t]).wait()
    for zb in range(4):
        for q in range(2):
            if q or zb in (1, 2):
                send_y(q, zb, 0).wait_send()
            else:
                @pl.when(z == zb)
                def _():
                    send_y(q, zb, 0).wait_send()
            for yb in range(2):
                send_d(q, zb, yb, 0).wait_send()

            @pl.when(((zb > z) & (z > 0)) | ((zb < z) & (z < 3)))
            def _():
                send_fwd(q, zb, 0, 1).wait_send()
        for h in range(2):
            if h or zb in (1, 2):
                rs_y(0, zb, h).wait_send()
            else:
                @pl.when(z == zb)
                def _():
                    rs_y(0, zb, h).wait_send()
            if zb:
                remote(sums.at[0, :, part(h)], cbuf.at[0, 0, :, part(h)], cs_sem.at[zb, h], cr_sem.at[0, 0, h], partner).wait_send()

    @pl.when(z < 3)
    def _():
        send_end(0, 1).wait_send()
        for q in range(2):
            send_own(q, 1).wait_send()

    @pl.when(z > 0)
    def _():
        send_end(0, 0).wait_send()
        for q in range(2):
            send_own(q, 0).wait_send()
    rs_end(0, far_end).wait_send()

    @pl.when(inner > 0)
    def _():
        rs_end(0, near_end).wait_send()

    @pl.loop(1, 16)
    def _(d):
        send_table(d).wait_send()
    for j in range(2):
        give(j).wait_send()
    result.wait()


def routed(x_tokens, dy_tokens, ids, gates, slots, w_gate, w_up, w_down, s_gate, s_up, s_down):
    tok, dim = x_tokens.shape
    ff = w_gate.shape[2]
    cap = tok // 2
    dma = pltpu.SemaphoreType.DMA
    shape = jax.ShapeDtypeStruct
    return pl.pallas_call(
        routed_kernel,
        name='routed',
        out_shape=(shape((2, cap, dim), BF16), shape((2, 16, cap, dim), BF16), shape((2, 16, cap, dim), BF16),
                   shape((2, 16, cap, 2 * ff), BF16), shape((2, 16, cap, ff), BF16), shape((tok, 2 * ff), BF16), shape((tok, ff), BF16)),
        in_specs=[ANY, ANY] + [VMEM] * 3 + [ANY] * 6,
        out_specs=(ANY,) * 7,
        scratch_shapes=[
            pltpu.VMEM((16, tok, dim), BF16), pltpu.VMEM((16, tok, dim), BF16), pltpu.VMEM((16, 8, tok), F32), pltpu.VMEM((16, 8, tok), F32), pltpu.VMEM((16, 2 * cap, tok), BF16),
            pltpu.VMEM((2, dim, 2 * ff), BF16), pltpu.VMEM((2, ff, dim), BF16),
            pltpu.VMEM((2, 16, cap, 2 * ff), BF16), pltpu.VMEM((2, 2, cap, ff), BF16), pltpu.VMEM((2, 2, cap, dim), BF16), pltpu.VMEM((2, 2, cap, dim), BF16),
            pltpu.VMEM((tok, 2 * ff), BF16), pltpu.VMEM((tok, ff), BF16), pltpu.VMEM((tok, dim), F32),
            pltpu.VMEM((8, tok, dim), F32), pltpu.VMEM((2, tok, dim), F32), pltpu.VMEM((2, tok, dim), F32),
            pltpu.VMEM((4, tok, dim), F32), pltpu.VMEM((2, 3, tok, dim), F32), pltpu.VMEM((2, tok, dim // 2), F32),
            dma((8,)), dma((4, 8)), dma((16,)), dma((16,)), dma((2, 16)), dma((2, 4)), dma((2, 8)), dma((2, 2)), dma((2, 4)), dma((2,)),
            dma((2,)), dma((2,)), dma((4, 2)), dma((4, 2)), dma((4, 2)), dma((2, 3, 2)), dma((2,)), dma((2,)), pltpu.SemaphoreType.REGULAR,
        ],
        compiler_params=pltpu.CompilerParams(collective_id=0, has_side_effects=True, vmem_limit_bytes=VMEM_LIMIT),
        cost_estimate=pl.CostEstimate(flops=16 * tok * 2 * dim * ff * 5, bytes_accessed=80_000_000, transcendentals=0),
    )(x_tokens, dy_tokens, ids, gates, slots, w_gate, w_up, w_down, s_gate, s_up, s_down)


def grads_kernel(x_in, dy_in, sact_in, shid_in, xr_in, zr_in, act_in, hid_in,
                 s1, s3, s2, g1, g3, g2,
                 x, dy, sact, shid, xr, zr, act, hid, ring, load_sem, ring_sem):
    dim, ff = x.shape[1], shid.shape[1]
    tile = ff
    count = dim // tile
    small = [pltpu.make_async_copy(a, b, load_sem.at[i]) for i, (a, b) in enumerate(((x_in, x), (sact_in, sact), (shid_in, shid), (dy_in, dy)))]
    pairs = ((xr_in, xr), (act_in, act), (hid_in, hid), (zr_in, zr))

    def large(e):
        return [pltpu.make_async_copy(a.at[e], b.at[e], load_sem.at[4 * e + 4 + i]) for i, (a, b) in enumerate(pairs)]

    for cp in small + large(0) + large(1):
        cp.start()
    depth = ring.shape[0]

    def drain(slot):
        for i in range(3):
            pltpu.make_async_copy(ring.at[slot, i, pl.ds(0, ff), pl.ds(0, ff)], g1.at[0, pl.ds(0, ff), :], ring_sem.at[slot, i]).wait()

    def emit(job, rows, acts, hids, dzs, outs):
        slot = lax.rem(job, depth)

        @pl.when(job >= depth)
        def _():
            drain(slot)
        both = dot_tn(rows, acts)
        ring[slot, 0] = both[:, :ff]
        ring[slot, 1] = both[:, ff:]
        ring[slot, 2] = dot_tn(hids, dzs)
        for i in range(3):
            pltpu.make_async_copy(ring.at[slot, i], outs[i], ring_sem.at[slot, i]).start()

    for cp in small:
        cp.wait()

    @pl.loop(0, count)
    def _(i):
        part = pl.ds(pl.multiple_of(i * tile, tile), tile)
        emit(i, x[:, part], sact[...], shid[...], dy[:, part], (s1.at[0, part, :], s3.at[0, part, :], s2.at[0, :, part]))

    @pl.loop(0, 2 * count)
    def _(j):
        e = lax.div(j, count)
        i = lax.rem(j, count)

        @pl.when(i == 0)
        def _():
            for cp in large(e):
                cp.wait()
        part = pl.ds(pl.multiple_of(i * tile, tile), tile)
        emit(j + count, xr[e, :, part], act[e], hid[e], zr[e, :, part], (g1.at[e, part, :], g3.at[e, part, :], g2.at[e, :, part]))
    for slot in range(depth):
        drain(slot)


def weight_grads(x, dy, sact, shid, xr, zr, act, hid):
    dim, ff = x.shape[1], shid.shape[1]
    tile = ff
    shape = jax.ShapeDtypeStruct
    ins = (x, dy, sact, shid, xr, zr, act, hid)
    dma = pltpu.SemaphoreType.DMA
    return pl.pallas_call(
        grads_kernel,
        name='weight_grads',
        out_shape=tuple(shape((n,) + d, F32) for n in (1, 2) for d in ((dim, ff), (dim, ff), (ff, dim))),
        in_specs=[ANY] * 8,
        out_specs=(ANY,) * 6,
        scratch_shapes=[pltpu.VMEM(a.shape, a.dtype) for a in ins] + [pltpu.VMEM((4, 3, tile, ff), F32), dma((12,)), dma((4, 3))],
        compiler_params=pltpu.CompilerParams(vmem_limit_bytes=60_000_000),
        cost_estimate=pl.CostEstimate(flops=6 * dim * ff * (x.shape[0] + 2 * xr.shape[1]), bytes_accessed=2 * sum(a.size for a in ins) + 36 * dim * ff, transcendentals=0),
    )(*ins)


def solution(mesh):
    group = mesh.shape['ep']
    token_spec = P(('dp', 'ep'), None)
    expert_spec = P('ep', None, None)
    whole_spec = P(None, None)
    grad_spec = P(('dp', 'ep'), None, None)

    def local_backward(x_tokens, dy_tokens, expert_ids, gate_vals, slot_pos, w_gate, w_up, w_down, shared_gate, shared_up, shared_down):
        tok, dim = x_tokens.shape
        local_experts = w_gate.shape[0]
        grad_x, x_all, z_all, act_all, hid_all, sact, shid = routed(x_tokens, dy_tokens, expert_ids.T, gate_vals.T, slot_pos.T, w_gate, w_up, w_down, shared_gate, shared_up, shared_down)
        x_all, z_all, act_all, hid_all = [a.reshape(local_experts, -1, a.shape[-1]) for a in (x_all, z_all, act_all, hid_all)]
        grad_shared_gate, grad_shared_up, grad_shared_down, grad_w_gate, grad_w_up, grad_w_down = weight_grads(x_tokens, dy_tokens, sact, shid, x_all, z_all, act_all, hid_all)
        grad_x = grad_x.reshape(tok, dim)
        return grad_x, grad_w_gate, grad_w_up, grad_w_down, grad_shared_gate, grad_shared_up, grad_shared_down

    return jax.shard_map(local_backward, mesh=mesh, in_specs=(token_spec, token_spec, token_spec, token_spec, token_spec, expert_spec, expert_spec, expert_spec, whole_spec, whole_spec, whole_spec), out_specs=(token_spec, grad_spec, grad_spec, grad_spec, grad_spec, grad_spec, grad_spec), check_vma=False)
```

```python
import functools

import jax
import jax.numpy as jnp
from jax import lax
from jax.experimental import pallas as pl
from jax.experimental.pallas import tpu as pltpu
from jax.sharding import PartitionSpec as P

F32 = jnp.float32
BF16 = jnp.bfloat16
ANY = pl.BlockSpec(memory_space=pl.ANY)
VMEM = pl.BlockSpec(memory_space=pltpu.VMEM)
VMEM_LIMIT = 67_000_000


def dot_nn(a, b):
    return lax.dot_general(a, b, (((1,), (0,)), ((), ())), preferred_element_type=F32)


def dot_nt(a, b):
    return lax.dot_general(a, b, (((1,), (1,)), ((), ())), preferred_element_type=F32)


def dot_tn(a, b):
    return lax.dot_general(a, b, (((0,), (0,)), ((), ())), preferred_element_type=F32)


def swiglu_parts(act_gate, act_up, grad_hidden):
    gate_f32 = act_gate.astype(F32)
    up_f32 = act_up.astype(F32)
    sigma = jax.nn.sigmoid(gate_f32)
    silu_gate = gate_f32 * sigma
    hidden = (silu_gate * up_f32).astype(BF16)
    grad_gate = (grad_hidden * up_f32 * sigma * (1.0 + gate_f32 * (1.0 - sigma))).astype(BF16)
    grad_up = (grad_hidden * silu_gate).astype(BF16)
    return hidden, grad_gate, grad_up


END_PLAN = (
    'C00F20F10F11R00X00F21C10R10C20F40X10F30F31R20F41C30R30C40F60',
    'X20X30R40F50F51F61X40C50Y01R50C60X50F70F71S30R60C70R70X60Y20',
    'X70E00Y31Y21Y11Y10S20S31S21S11N00S10',
)
MID_PLAN = (
    'C00F20F10R00F30F11C10F31F50X00F21R10C20F60X10F51F40R20C30R30',
    'F41X20C40R40Y00X30F70C50F61R50X40Y11Y01X50F71C60R60C70R70X60',
    'X70Y20S30Y31E00S10S20N00Y21S31S21S11',
)


def gaps(text):
    found = [[]]
    for i in range(0, len(text), 3):
        token = text[i:i + 3]
        if token[0] in 'CR':
            found.append([])
        else:
            found[-1].append(token)
    return found


def routed_kernel(x_in, dy_in, ids, gates, slots, w_gate, w_up, w_down, s_gate, s_up, s_down,
                  grad_x, x_all, z_all, act_all, hid_all, sact_out, shid_out,
                  xbuf, dybuf, tbuf, table, pick, w13, w2, act, hst, xst, zst, sact, shid, sdx,
                  sums, dsend, pbuf, ybuf, cbuf, ebuf,
                  load_sem, out_sem, gs_sem, gr_sem, recv_sem, sy_sem, sd_sem, sown_sem, sz_sem, sx_sem,
                  ds_sem, dr_sem, ys_sem, yr_sem, cs_sem, cr_sem, es_sem, er_sem, credit):
    tok, dim = x_in.shape
    ff = w2.shape[1]
    cap = xst.shape[2]
    half = dim // 2
    tile = min(512, dim)
    me = lax.axis_index('ep')
    z = lax.div(me, 4)
    y = lax.rem(lax.div(me, 2), 2)
    c = lax.rem(me, 2)
    partner = me + 1 - 2 * c
    side = me + 2 - 4 * y
    inner = z * (3 - z)
    near_end = lax.div(z, 2)
    far_end = 1 - near_end
    bufs = (xbuf, dybuf)
    own_slot = (0, 1, 3, 5)
    other_slot = (2, 4, 6, 7)
    near_first = [(own_slot.index(t), 0) if t in own_slot else (other_slot.index(t), 1) for t in range(8)]

    def bid(zz, yy, cc):
        return zz * 4 + yy * 2 + cc

    def order(k):
        near = lax.div(inner, 2)
        delta = lax.div((1 - k) * (2 - k) * (3 - k), 6) - lax.div(k * (2 - k) * (3 - k), 2)
        base = k + near * delta
        return base + near_end * (3 - 2 * base)

    def visit(t):
        u = t + lax.div(t, 7)
        odd = lax.rem(u, 2)
        first = lax.div(7 - t, 7)
        k = odd * lax.div(u + 1, 2) + (1 - odd) * (lax.div(u, 2) - 1) + first
        col = 1 - odd - first
        return order(k), y + col * (1 - 2 * y), col

    def remote(src, dst, send, recv, dev):
        return pltpu.make_async_remote_copy(src_ref=src, dst_ref=dst, send_sem=send, recv_sem=recv, device_id={'ep': dev}, device_id_type=pl.DeviceIdType.MESH)

    def weights(e, gate, up, down):
        return [pltpu.make_async_copy(gate, w13.at[e, :, pl.ds(0, ff)], load_sem.at[2 + 3 * e]),
                pltpu.make_async_copy(up, w13.at[e, :, pl.ds(ff, ff)], load_sem.at[3 + 3 * e]),
                pltpu.make_async_copy(down, w2.at[e], load_sem.at[4 + 3 * e])]

    own = [pltpu.make_async_copy(x_in, xbuf.at[me], load_sem.at[0]), pltpu.make_async_copy(dy_in, dybuf.at[me], load_sem.at[1])]
    shared_load = weights(1, s_gate, s_up, s_down)
    first_load = weights(0, w_gate.at[0], w_up.at[0], w_down.at[0])
    second_load = weights(1, w_gate.at[1], w_up.at[1], w_down.at[1])
    for cp in own + shared_load + first_load:
        cp.start()

    barrier = pltpu.get_barrier_semaphore()

    @pl.loop(1, 16)
    def _(d):
        pl.semaphore_signal(barrier, inc=1, device_id={'ep': lax.rem(me + d, 16)}, device_id_type=pl.DeviceIdType.MESH)
    pl.semaphore_wait(barrier, 15)

    def send_y(q, zb, b):
        return remote(bufs[q].at[b], bufs[q].at[b], sy_sem.at[q, zb], recv_sem.at[q, b], side)

    def send_d(q, zb, yb, b):
        return remote(bufs[q].at[b], bufs[q].at[b], sd_sem.at[q, zb * 2 + yb], recv_sem.at[q, b], partner)

    def send_own(q, up):
        return remote(bufs[q].at[me], bufs[q].at[me], sown_sem.at[q, up], recv_sem.at[q, me], me + (4 if up else -4))

    def send_fwd(q, zb, b, up):
        return remote(bufs[q].at[b], bufs[q].at[b], sz_sem.at[q, zb], recv_sem.at[q, b], me + (4 if up else -4))

    def send_end(b, up):
        return remote(xbuf.at[b], xbuf.at[b], sx_sem.at[1 - up], recv_sem.at[0, b], me + (4 if up else -4))

    for q in range(2):
        own[q].wait()
        send_y(q, z, me).start()

        @pl.when(z < 3)
        def _():
            send_own(q, 1).start()

        @pl.when(z > 0)
        def _():
            send_own(q, 0).start()
        send_d(q, z, y, me).start()

    kept = jnp.where(slots[...] >= 0, ids[...], -1)
    slot_f32 = slots[...].astype(F32) + 1.0
    for dev in range(16):
        hits = [kept == 2 * dev + e for e in range(2)]
        rows = [jnp.sum(jnp.where(hit, gates[...], 0.0), axis=0, keepdims=True) for hit in hits]
        rows += [jnp.sum(jnp.where(hit, slot_f32, 0.0), axis=0, keepdims=True) - 1.0 for hit in hits]
        table[dev] = jnp.concatenate(rows + [jnp.zeros((4, tok), F32)], axis=0)

    def send_table(d):
        dest = lax.rem(me + d, 16)
        return remote(table.at[dest], tbuf.at[me], gs_sem.at[d], gr_sem.at[me], dest)

    @pl.loop(1, 16)
    def _(d):
        send_table(d).start()
    tbuf[me] = table[me]

    def place(t):
        k, col = near_first[t]
        return order(k), y + col * (1 - 2 * y), col

    def pass_on(t, q):
        zb, yb, col = place(t)
        b = bid(zb, yb, c)
        send_d(q, zb, yb, b).wait_recv()
        if col == 0:
            if q:
                send_y(q, zb, b).start()
            else:
                @pl.when(zb * (3 - zb) > 0)
                def _():
                    send_y(q, zb, b).start()

            @pl.when((zb > z) & (z > 0))
            def _():
                send_fwd(q, zb, b, 0).start()

            @pl.when((zb < z) & (z < 3))
            def _():
                send_fwd(q, zb, b, 1).start()
        elif q == 0:
            @pl.when((zb == 3) & (z > 0))
            def _():
                send_end(b, 0).start()

            @pl.when((zb == 0) & (z < 3))
            def _():
                send_end(b, 1).start()
        send_d(q, zb, yb, b).start()

    def flush(t, start):
        zb, yb, _ = visit(t)
        two = pl.ds(bid(zb, yb, 0), 2)
        cps = [pltpu.make_async_copy(xst, x_all.at[:, two], out_sem.at[0, t]),
               pltpu.make_async_copy(zst, z_all.at[:, two], out_sem.at[1, t]),
               pltpu.make_async_copy(hst, hid_all.at[:, two], out_sem.at[2, t]),
               pltpu.make_async_copy(act.at[:, two], act_all.at[:, two], out_sem.at[3, t])]
        if start:
            for cp in cps:
                cp.start()
        else:
            for cp in cps[:3]:
                cp.wait()

    def compute(t):
        zb, yb, _ = visit(t)
        b0 = bid(zb, yb, 0)
        bp = bid(zb, yb, 1 - c)
        for q in range(2):
            send_d(q, zb, yb, bp).wait_recv()
        for p in range(2):
            @pl.when(b0 + p != me)
            def _():
                remote(table.at[0], tbuf.at[b0 + p], gs_sem.at[0], gr_sem.at[b0 + p], partner).wait_recv()

        @pl.when(t > 0)
        def _():
            flush(t - 1, False)
        row = lax.broadcasted_iota(jnp.int32, (2 * cap, tok), 0).astype(F32)
        for p in range(2):
            info = tbuf[b0 + p]
            top = row < cap
            chosen = jnp.where(top, info[2:3, :], info[3:4, :] + cap) == row
            gate = jnp.sum(jnp.where(chosen, jnp.where(top, info[0:1, :], info[1:2, :]), 0.0), axis=1, keepdims=True)
            sel = chosen.astype(BF16)
            pick[b0 + p] = sel
            for n in range(dim // tile):
                cols = slice(n * tile, (n + 1) * tile)
                xr = dot_nn(sel, xbuf[b0 + p, :, cols]).astype(BF16)
                zr = (dot_nn(sel, dybuf[b0 + p, :, cols]) * gate).astype(BF16)
                for e in range(2):
                    xst[e, p, :, cols] = xr[e * cap:(e + 1) * cap]
                    zst[e, p, :, cols] = zr[e * cap:(e + 1) * cap]
        two = pl.ds(b0, 2)
        for e in range(2):
            ab = dot_nn(xst[e].reshape(2 * cap, dim), w13[e]).astype(BF16)
            grad_hidden = dot_nt(zst[e].reshape(2 * cap, dim), w2[e])
            hidden, grad_gate, grad_up = swiglu_parts(ab[:, :ff], ab[:, ff:], grad_hidden)
            hst[e] = hidden.reshape(2, cap, ff)
            act[e, two, :, :ff] = grad_gate.reshape(2, cap, ff)
            act[e, two, :, ff:] = grad_up.reshape(2, cap, ff)
        flush(t, True)

    for cp in shared_load:
        cp.wait()
    ab = dot_nn(xbuf[me], w13[1]).astype(BF16)
    hidden, grad_gate, grad_up = swiglu_parts(ab[:, :ff], ab[:, ff:], dot_nt(dybuf[me], w2[1]))
    shid[...] = hidden
    sact[:, :ff] = grad_gate
    sact[:, ff:] = grad_up
    for n in range(dim // tile):
        cols = slice(n * tile, (n + 1) * tile)
        sdx[:, cols] = dot_nt(sact[...], w13[1, cols, :])
    shared_out = [pltpu.make_async_copy(sact, sact_out, load_sem.at[0]), pltpu.make_async_copy(shid, shid_out, load_sem.at[1])]
    for cp in shared_out + second_load:
        cp.start()
    for cp in first_load + second_load:
        cp.wait()
    def give(j):
        return remote(dsend.at[lax.rem(j, 2)], pbuf.at[lax.rem(j, 2)], ds_sem.at[lax.rem(j, 2)], dr_sem.at[lax.rem(j, 2)], partner)

    def part(h):
        return pl.ds(h * half, half)

    def rs_y(j, zb, h):
        return remote(sums.at[j, :, part(h)], ybuf.at[zb, :, part(h)], ys_sem.at[zb, h], yr_sem.at[zb, h], side)

    def rs_end(j, end):
        return remote(sums.at[j, :, part(0)], ebuf.at[end], es_sem.at[end], er_sem.at[end], me + 8 * end - 4)

    def rs_compute(j):
        zb, yb, _ = visit(j)
        b = bid(zb, yb, c)
        bp = bid(zb, yb, 1 - c)

        @pl.when(j >= 2)
        def _():
            give(j).wait_send()

        @pl.loop(0, dim // tile)
        def _(n):
            cols = pl.ds(pl.multiple_of(n * tile, tile), tile)
            r = [dot_nt(jnp.concatenate([act[e, b], act[e, bp]], axis=0), w13[e, cols, :]).astype(BF16) for e in range(2)]
            sums[j, :, cols] = dot_tn(pick[b], jnp.concatenate([r[0][:cap], r[1][:cap]], axis=0))
            dsend[lax.rem(j, 2), :, cols] = dot_tn(pick[bp], jnp.concatenate([r[0][cap:], r[1][cap:]], axis=0))

        @pl.when(j >= 2)
        def _():
            pl.semaphore_wait(credit, 1)
        give(j).start()

    def rs_finish(j):
        give(j).wait_recv()
        sums[j] = sums[j] + pbuf[j % 2]
        if j < 6:
            pl.semaphore_signal(credit, inc=1, device_id={'ep': partner}, device_id_type=pl.DeviceIdType.MESH)

    def end_in(j, end):
        rs_end(j, end).wait_recv()
        sums[j, :, part(0)] = sums[j, :, part(0)] + ebuf[end]

    def chain(k, h, zb, up):
        j = own_slot[k]
        slot, gap = (0, zb - z - 1) if up else (1, z - zb - 1)
        return remote(sums.at[j, :, part(h)], cbuf.at[slot, gap, :, part(h)], cs_sem.at[k, h], cr_sem.at[slot, gap, h], me + (4 if up else -4))

    def chain_in(j, h, slot, gap):
        remote(sums.at[j, :, part(h)], cbuf.at[slot, gap, :, part(h)], cs_sem.at[0, h], cr_sem.at[slot, gap, h], partner).wait_recv()
        sums[j, :, part(h)] = sums[j, :, part(h)] + cbuf[slot, gap, :, part(h)]

    def y_in(j, zb, h):
        rs_y(0, zb, h).wait_recv()
        sums[j, :, part(h)] = sums[j, :, part(h)] + ybuf[zb, :, part(h)]

    def step(k, h, mid):
        zb = order(k)
        j = own_slot[k]
        if h or k == 2 or (k == 1 and not mid):
            y_in(j, zb, h)

        @pl.when(zb > z)
        def _():
            if mid:
                chain_in(j, h, 0, zb - z)
            chain(k, h, zb, True).start()

        @pl.when(zb < z)
        def _():
            if mid:
                chain_in(j, h, 1, z - zb)
            chain(k, h, zb, False).start()

    def act_on(token, mid):
        kind, k, h = token[0], int(token[1]), int(token[2])
        if kind == 'F':
            pass_on(k, h)
        elif kind == 'X':
            rs_finish(k)
        elif kind == 'Y':
            rs_y(other_slot[k], order(k), h).start()
        elif kind == 'S':
            step(k, h, mid)
        elif kind == 'E':
            if mid:
                end_in(other_slot[3], far_end)
            rs_end(other_slot[3], far_end).start()
        elif mid:
            end_in(other_slot[1], near_end)
            rs_end(other_slot[1], near_end).start()
        else:
            end_in(other_slot[0], near_end)
            rs_y(other_slot[0], z, 0).start()

    plans = [gaps(''.join(rows)) for rows in (END_PLAN, MID_PLAN)]

    def between(t, gap):
        for mid in range(2):
            tokens = plans[mid][gap]
            if tokens:
                @pl.when((t == gap // 2) & ((inner > 0) if mid else (inner == 0)))
                def _():
                    for token in tokens:
                        act_on(token, mid)

    @pl.loop(0, 8)
    def _(t):
        for g in range(8):
            between(t, 2 * g)
        compute(t)
        for g in range(8):
            between(t, 2 * g + 1)
        rs_compute(t)

    between(8, 16)
    flush(7, False)
    for h in (1, 0):
        @pl.when(z > 0)
        def _():
            chain_in(0, h, 0, 0)

        @pl.when(z < 3)
        def _():
            chain_in(0, h, 1, 0)
        rs_y(0, z, h).wait_recv()
        total = sums[0, :, part(h)] + ybuf[z, :, part(h)] + sdx[:, part(h)]
        xst[0, :, :, part(h)] = total.astype(BF16).reshape(2, cap, half)
    result = pltpu.make_async_copy(xst.at[0], grad_x, load_sem.at[2])
    result.start()

    for cp in shared_out:
        cp.wait()
    for t in range(8):
        pltpu.make_async_copy(act.at[:, pl.ds(0, 2)], act_all.at[:, pl.ds(0, 2)], out_sem.at[3, t]).wait()
    for zb in range(4):
        for q in range(2):
            if q or zb in (1, 2):
                send_y(q, zb, 0).wait_send()
            else:
                @pl.when(z == zb)
                def _():
                    send_y(q, zb, 0).wait_send()
            for yb in range(2):
                send_d(q, zb, yb, 0).wait_send()

            @pl.when(((zb > z) & (z > 0)) | ((zb < z) & (z < 3)))
            def _():
                send_fwd(q, zb, 0, 1).wait_send()
        for h in range(2):
            if h or zb in (1, 2):
                rs_y(0, zb, h).wait_send()
            else:
                @pl.when(z == zb)
                def _():
                    rs_y(0, zb, h).wait_send()
            if zb:
                remote(sums.at[0, :, part(h)], cbuf.at[0, 0, :, part(h)], cs_sem.at[zb, h], cr_sem.at[0, 0, h], partner).wait_send()

    @pl.when(z < 3)
    def _():
        send_end(0, 1).wait_send()
        for q in range(2):
            send_own(q, 1).wait_send()

    @pl.when(z > 0)
    def _():
        send_end(0, 0).wait_send()
        for q in range(2):
            send_own(q, 0).wait_send()
    rs_end(0, far_end).wait_send()

    @pl.when(inner > 0)
    def _():
        rs_end(0, near_end).wait_send()

    @pl.loop(1, 16)
    def _(d):
        send_table(d).wait_send()
    for j in range(2):
        give(j).wait_send()
    result.wait()


def routed(x_tokens, dy_tokens, ids, gates, slots, w_gate, w_up, w_down, s_gate, s_up, s_down):
    tok, dim = x_tokens.shape
    ff = w_gate.shape[2]
    cap = tok // 2
    dma = pltpu.SemaphoreType.DMA
    shape = jax.ShapeDtypeStruct
    return pl.pallas_call(
        routed_kernel,
        name='routed',
        out_shape=(shape((2, cap, dim), BF16), shape((2, 16, cap, dim), BF16), shape((2, 16, cap, dim), BF16),
                   shape((2, 16, cap, 2 * ff), BF16), shape((2, 16, cap, ff), BF16), shape((tok, 2 * ff), BF16), shape((tok, ff), BF16)),
        in_specs=[ANY, ANY] + [VMEM] * 3 + [ANY] * 6,
        out_specs=(ANY,) * 7,
        scratch_shapes=[
            pltpu.VMEM((16, tok, dim), BF16), pltpu.VMEM((16, tok, dim), BF16), pltpu.VMEM((16, 8, tok), F32), pltpu.VMEM((16, 8, tok), F32), pltpu.VMEM((16, 2 * cap, tok), BF16),
            pltpu.VMEM((2, dim, 2 * ff), BF16), pltpu.VMEM((2, ff, dim), BF16),
            pltpu.VMEM((2, 16, cap, 2 * ff), BF16), pltpu.VMEM((2, 2, cap, ff), BF16), pltpu.VMEM((2, 2, cap, dim), BF16), pltpu.VMEM((2, 2, cap, dim), BF16),
            pltpu.VMEM((tok, 2 * ff), BF16), pltpu.VMEM((tok, ff), BF16), pltpu.VMEM((tok, dim), F32),
            pltpu.VMEM((8, tok, dim), F32), pltpu.VMEM((2, tok, dim), F32), pltpu.VMEM((2, tok, dim), F32),
            pltpu.VMEM((4, tok, dim), F32), pltpu.VMEM((2, 3, tok, dim), F32), pltpu.VMEM((2, tok, dim // 2), F32),
            dma((8,)), dma((4, 8)), dma((16,)), dma((16,)), dma((2, 16)), dma((2, 4)), dma((2, 8)), dma((2, 2)), dma((2, 4)), dma((2,)),
            dma((2,)), dma((2,)), dma((4, 2)), dma((4, 2)), dma((4, 2)), dma((2, 3, 2)), dma((2,)), dma((2,)), pltpu.SemaphoreType.REGULAR,
        ],
        compiler_params=pltpu.CompilerParams(collective_id=0, has_side_effects=True, vmem_limit_bytes=VMEM_LIMIT),
        cost_estimate=pl.CostEstimate(flops=16 * tok * 2 * dim * ff * 5, bytes_accessed=80_000_000, transcendentals=0),
    )(x_tokens, dy_tokens, ids, gates, slots, w_gate, w_up, w_down, s_gate, s_up, s_down)


def grads_kernel(x_in, dy_in, sact_in, shid_in, xr_in, zr_in, act_in, hid_in,
                 s1, s3, s2, g1, g3, g2,
                 x, dy, sact, shid, xr, zr, act, hid, ring, load_sem, tile_sem, ring_sem):
    dim, ff = x.shape[1], shid.shape[1]
    tile = ff
    count = dim // tile
    small = [pltpu.make_async_copy(a, b, load_sem.at[i]) for i, (a, b) in enumerate(((x_in, x), (sact_in, sact), (shid_in, shid), (dy_in, dy)))]

    def part(i):
        return pl.ds(pl.multiple_of(i * tile, tile), tile)

    def whole(e):
        return [pltpu.make_async_copy(a.at[e], b.at[e], load_sem.at[2 * e + 4 + i]) for i, (a, b) in enumerate(((act_in, act), (hid_in, hid)))]

    def tiles(e, i):
        return [pltpu.make_async_copy(a.at[e, :, part(i)], b.at[e, :, part(i)], tile_sem.at[n, e, i]) for n, (a, b) in enumerate(((xr_in, xr), (zr_in, zr)))]

    def load(e):
        for cp in whole(e):
            cp.start()
        for i in range(count):
            for cp in tiles(e, i):
                cp.start()

    for cp in small:
        cp.start()
    load(0)
    depth = ring.shape[0]

    def drain(slot):
        for i in range(3):
            pltpu.make_async_copy(ring.at[slot, i, pl.ds(0, ff), pl.ds(0, ff)], g1.at[0, pl.ds(0, ff), :], ring_sem.at[slot, i]).wait()

    def emit(job, rows, acts, hids, dzs, outs):
        slot = lax.rem(job, depth)

        @pl.when(job >= depth)
        def _():
            drain(slot)
        both = dot_tn(rows, acts)
        ring[slot, 0] = both[:, :ff]
        ring[slot, 1] = both[:, ff:]
        ring[slot, 2] = dot_tn(hids, dzs)
        for i in range(3):
            pltpu.make_async_copy(ring.at[slot, i], outs[i], ring_sem.at[slot, i]).start()

    for cp in small:
        cp.wait()

    @pl.loop(0, count)
    def _(i):
        emit(i, x[:, part(i)], sact[...], shid[...], dy[:, part(i)], (s1.at[0, part(i), :], s3.at[0, part(i), :], s2.at[0, :, part(i)]))
    load(1)

    @pl.loop(0, 2 * count)
    def _(j):
        e = lax.div(j, count)
        i = lax.rem(j, count)

        @pl.when(i == 0)
        def _():
            for cp in whole(e):
                cp.wait()
        for cp in tiles(e, i):
            cp.wait()
        emit(j + count, xr[e, :, part(i)], act[e], hid[e], zr[e, :, part(i)], (g1.at[e, part(i), :], g3.at[e, part(i), :], g2.at[e, :, part(i)]))
    for slot in range(depth):
        drain(slot)


def weight_grads(x, dy, sact, shid, xr, zr, act, hid):
    dim, ff = x.shape[1], shid.shape[1]
    tile = ff
    shape = jax.ShapeDtypeStruct
    ins = (x, dy, sact, shid, xr, zr, act, hid)
    dma = pltpu.SemaphoreType.DMA
    return pl.pallas_call(
        grads_kernel,
        name='weight_grads',
        out_shape=tuple(shape((n,) + d, F32) for n in (1, 2) for d in ((dim, ff), (dim, ff), (ff, dim))),
        in_specs=[ANY] * 8,
        out_specs=(ANY,) * 6,
        scratch_shapes=[pltpu.VMEM(a.shape, a.dtype) for a in ins] + [pltpu.VMEM((4, 3, tile, ff), F32), dma((8,)), dma((2, 2, dim // tile)), dma((4, 3))],
        compiler_params=pltpu.CompilerParams(vmem_limit_bytes=60_000_000),
        cost_estimate=pl.CostEstimate(flops=6 * dim * ff * (x.shape[0] + 2 * xr.shape[1]), bytes_accessed=2 * sum(a.size for a in ins) + 36 * dim * ff, transcendentals=0),
    )(*ins)


def solution(mesh):
    group = mesh.shape['ep']
    token_spec = P(('dp', 'ep'), None)
    expert_spec = P('ep', None, None)
    whole_spec = P(None, None)
    grad_spec = P(('dp', 'ep'), None, None)

    def local_backward(x_tokens, dy_tokens, expert_ids, gate_vals, slot_pos, w_gate, w_up, w_down, shared_gate, shared_up, shared_down):
        tok, dim = x_tokens.shape
        local_experts = w_gate.shape[0]
        grad_x, x_all, z_all, act_all, hid_all, sact, shid = routed(x_tokens, dy_tokens, expert_ids.T, gate_vals.T, slot_pos.T, w_gate, w_up, w_down, shared_gate, shared_up, shared_down)
        x_all, z_all, act_all, hid_all = [a.reshape(local_experts, -1, a.shape[-1]) for a in (x_all, z_all, act_all, hid_all)]
        grad_shared_gate, grad_shared_up, grad_shared_down, grad_w_gate, grad_w_up, grad_w_down = weight_grads(x_tokens, dy_tokens, sact, shid, x_all, z_all, act_all, hid_all)
        grad_x = grad_x.reshape(tok, dim)
        return grad_x, grad_w_gate, grad_w_up, grad_w_down, grad_shared_gate, grad_shared_up, grad_shared_down

    return jax.shard_map(local_backward, mesh=mesh, in_specs=(token_spec, token_spec, token_spec, token_spec, token_spec, expert_spec, expert_spec, expert_spec, whole_spec, whole_spec, whole_spec), out_specs=(token_spec, grad_spec, grad_spec, grad_spec, grad_spec, grad_spec, grad_spec), check_vma=False)
```

```python
import functools

import jax
import jax.numpy as jnp
from jax import lax
from jax.experimental import pallas as pl
from jax.experimental.pallas import tpu as pltpu
from jax.sharding import PartitionSpec as P

F32 = jnp.float32
BF16 = jnp.bfloat16
ANY = pl.BlockSpec(memory_space=pl.ANY)
VMEM = pl.BlockSpec(memory_space=pltpu.VMEM)
VMEM_LIMIT = 67_000_000


def dot_nn(a, b):
    return lax.dot_general(a, b, (((1,), (0,)), ((), ())), preferred_element_type=F32)


def dot_nt(a, b):
    return lax.dot_general(a, b, (((1,), (1,)), ((), ())), preferred_element_type=F32)


def dot_tn(a, b):
    return lax.dot_general(a, b, (((0,), (0,)), ((), ())), preferred_element_type=F32)


def swiglu_parts(act_gate, act_up, grad_hidden):
    gate_f32 = act_gate.astype(F32)
    up_f32 = act_up.astype(F32)
    sigma = jax.nn.sigmoid(gate_f32)
    silu_gate = gate_f32 * sigma
    hidden = (silu_gate * up_f32).astype(BF16)
    grad_gate = (grad_hidden * up_f32 * sigma * (1.0 + gate_f32 * (1.0 - sigma))).astype(BF16)
    grad_up = (grad_hidden * silu_gate).astype(BF16)
    return hidden, grad_gate, grad_up


END_PLAN = (
    'C00F20F10F11R00X00F21C10R10C20F40X10F30F31R20F41C30R30C40F60',
    'X20X30R40F50F51F61X40C50Y01R50C60X50F70F71S30R60C70R70X60Y20',
    'X70E00Y31Y21Y11Y10S20S31S21S11N00S10',
)
MID_PLAN = (
    'C00F20F10R00F30F11C10F31F50X00F21R10C20F60X10F51F40R20C30R30',
    'F41X20C40R40Y00X30F70C50F61R50X40Y11Y01X50F71C60R60C70R70X60',
    'X70Y20S30Y31E00S10S20N00Y21S31S21S11',
)


def gaps(text):
    found = [[]]
    for i in range(0, len(text), 3):
        token = text[i:i + 3]
        if token[0] in 'CR':
            found.append([])
        else:
            found[-1].append(token)
    return found


def routed_kernel(x_in, dy_in, ids_in, gates_in, slots_in, w_gate, w_up, w_down, s_gate, s_up, s_down,
                  grad_x, x_all, z_all, act_all, hid_all, sact_out, shid_out,
                  xbuf, dybuf, ids, gates, slots, tbuf, table, pick, w13, w2, act, hst, xst, zst, sact, shid, sdx,
                  sums, dsend, pbuf, ybuf, cbuf, ebuf,
                  load_sem, out_sem, gs_sem, gr_sem, recv_sem, sy_sem, sd_sem, sown_sem, sz_sem, sx_sem,
                  ds_sem, dr_sem, ys_sem, yr_sem, cs_sem, cr_sem, es_sem, er_sem, credit):
    tok, dim = x_in.shape
    ff = w2.shape[1]
    cap = xst.shape[2]
    half = dim // 2
    tile = min(512, dim)
    me = lax.axis_index('ep')
    z = lax.div(me, 4)
    y = lax.rem(lax.div(me, 2), 2)
    c = lax.rem(me, 2)
    partner = me + 1 - 2 * c
    side = me + 2 - 4 * y
    inner = z * (3 - z)
    near_end = lax.div(z, 2)
    far_end = 1 - near_end
    bufs = (xbuf, dybuf)
    own_slot = (0, 1, 3, 5)
    other_slot = (2, 4, 6, 7)
    near_first = [(own_slot.index(t), 0) if t in own_slot else (other_slot.index(t), 1) for t in range(8)]

    def bid(zz, yy, cc):
        return zz * 4 + yy * 2 + cc

    def order(k):
        near = lax.div(inner, 2)
        delta = lax.div((1 - k) * (2 - k) * (3 - k), 6) - lax.div(k * (2 - k) * (3 - k), 2)
        base = k + near * delta
        return base + near_end * (3 - 2 * base)

    def visit(t):
        u = t + lax.div(t, 7)
        odd = lax.rem(u, 2)
        first = lax.div(7 - t, 7)
        k = odd * lax.div(u + 1, 2) + (1 - odd) * (lax.div(u, 2) - 1) + first
        col = 1 - odd - first
        return order(k), y + col * (1 - 2 * y), col

    def remote(src, dst, send, recv, dev):
        return pltpu.make_async_remote_copy(src_ref=src, dst_ref=dst, send_sem=send, recv_sem=recv, device_id={'ep': dev}, device_id_type=pl.DeviceIdType.MESH)

    def weights(e, gate, up, down):
        return [pltpu.make_async_copy(gate, w13.at[e, :, pl.ds(0, ff)], load_sem.at[2 + 3 * e]),
                pltpu.make_async_copy(up, w13.at[e, :, pl.ds(ff, ff)], load_sem.at[3 + 3 * e]),
                pltpu.make_async_copy(down, w2.at[e], load_sem.at[4 + 3 * e])]

    own = [pltpu.make_async_copy(x_in, xbuf.at[me], load_sem.at[0]), pltpu.make_async_copy(dy_in, dybuf.at[me], load_sem.at[1])]
    shared_load = weights(1, s_gate, s_up, s_down)
    first_load = weights(0, w_gate.at[0], w_up.at[0], w_down.at[0])
    second_load = weights(1, w_gate.at[1], w_up.at[1], w_down.at[1])
    routing = [pltpu.make_async_copy(a, b, load_sem.at[8 + i]) for i, (a, b) in enumerate(((ids_in, ids), (gates_in, gates), (slots_in, slots)))]
    for cp in own + routing + shared_load + first_load:
        cp.start()

    barrier = pltpu.get_barrier_semaphore()

    @pl.loop(1, 16)
    def _(d):
        pl.semaphore_signal(barrier, inc=1, device_id={'ep': lax.rem(me + d, 16)}, device_id_type=pl.DeviceIdType.MESH)
    pl.semaphore_wait(barrier, 15)

    def send_y(q, zb, b):
        return remote(bufs[q].at[b], bufs[q].at[b], sy_sem.at[q, zb], recv_sem.at[q, b], side)

    def send_d(q, zb, yb, b):
        return remote(bufs[q].at[b], bufs[q].at[b], sd_sem.at[q, zb * 2 + yb], recv_sem.at[q, b], partner)

    def send_own(q, up):
        return remote(bufs[q].at[me], bufs[q].at[me], sown_sem.at[q, up], recv_sem.at[q, me], me + (4 if up else -4))

    def send_fwd(q, zb, b, up):
        return remote(bufs[q].at[b], bufs[q].at[b], sz_sem.at[q, zb], recv_sem.at[q, b], me + (4 if up else -4))

    def send_end(b, up):
        return remote(xbuf.at[b], xbuf.at[b], sx_sem.at[1 - up], recv_sem.at[0, b], me + (4 if up else -4))

    for q in range(2):
        own[q].wait()
        send_y(q, z, me).start()

        @pl.when(z < 3)
        def _():
            send_own(q, 1).start()

        @pl.when(z > 0)
        def _():
            send_own(q, 0).start()
        send_d(q, z, y, me).start()

    for cp in routing:
        cp.wait()
    kept = jnp.where(slots[...] >= 0, ids[...], -1)
    slot_f32 = slots[...].astype(F32) + 1.0
    for dev in range(16):
        hits = [kept == 2 * dev + e for e in range(2)]
        rows = [jnp.sum(jnp.where(hit, gates[...], 0.0), axis=0, keepdims=True) for hit in hits]
        rows += [jnp.sum(jnp.where(hit, slot_f32, 0.0), axis=0, keepdims=True) - 1.0 for hit in hits]
        table[dev] = jnp.concatenate(rows + [jnp.zeros((4, tok), F32)], axis=0)

    def send_table(d):
        dest = lax.rem(me + d, 16)
        return remote(table.at[dest], tbuf.at[me], gs_sem.at[d], gr_sem.at[me], dest)

    @pl.loop(1, 16)
    def _(d):
        send_table(d).start()
    tbuf[me] = table[me]

    def place(t):
        k, col = near_first[t]
        return order(k), y + col * (1 - 2 * y), col

    def pass_on(t, q):
        zb, yb, col = place(t)
        b = bid(zb, yb, c)
        send_d(q, zb, yb, b).wait_recv()
        if col == 0:
            if q:
                send_y(q, zb, b).start()
            else:
                @pl.when(zb * (3 - zb) > 0)
                def _():
                    send_y(q, zb, b).start()

            @pl.when((zb > z) & (z > 0))
            def _():
                send_fwd(q, zb, b, 0).start()

            @pl.when((zb < z) & (z < 3))
            def _():
                send_fwd(q, zb, b, 1).start()
        elif q == 0:
            @pl.when((zb == 3) & (z > 0))
            def _():
                send_end(b, 0).start()

            @pl.when((zb == 0) & (z < 3))
            def _():
                send_end(b, 1).start()
        send_d(q, zb, yb, b).start()

    def flush(t, start):
        zb, yb, _ = visit(t)
        two = pl.ds(bid(zb, yb, 0), 2)
        cps = [pltpu.make_async_copy(xst, x_all.at[:, two], out_sem.at[0, t]),
               pltpu.make_async_copy(zst, z_all.at[:, two], out_sem.at[1, t]),
               pltpu.make_async_copy(hst, hid_all.at[:, two], out_sem.at[2, t]),
               pltpu.make_async_copy(act.at[:, two], act_all.at[:, two], out_sem.at[3, t])]
        if start:
            for cp in cps:
                cp.start()
        else:
            for cp in cps[:3]:
                cp.wait()

    def compute(t):
        zb, yb, _ = visit(t)
        b0 = bid(zb, yb, 0)
        bp = bid(zb, yb, 1 - c)
        for q in range(2):
            send_d(q, zb, yb, bp).wait_recv()
        for p in range(2):
            @pl.when(b0 + p != me)
            def _():
                remote(table.at[0], tbuf.at[b0 + p], gs_sem.at[0], gr_sem.at[b0 + p], partner).wait_recv()

        @pl.when(t > 0)
        def _():
            flush(t - 1, False)
        row = lax.broadcasted_iota(jnp.int32, (2 * cap, tok), 0).astype(F32)
        for p in range(2):
            info = tbuf[b0 + p]
            top = row < cap
            chosen = jnp.where(top, info[2:3, :], info[3:4, :] + cap) == row
            gate = jnp.sum(jnp.where(chosen, jnp.where(top, info[0:1, :], info[1:2, :]), 0.0), axis=1, keepdims=True)
            sel = chosen.astype(BF16)
            pick[b0 + p] = sel
            for n in range(dim // tile):
                cols = slice(n * tile, (n + 1) * tile)
                xr = dot_nn(sel, xbuf[b0 + p, :, cols]).astype(BF16)
                zr = (dot_nn(sel, dybuf[b0 + p, :, cols]) * gate).astype(BF16)
                for e in range(2):
                    xst[e, p, :, cols] = xr[e * cap:(e + 1) * cap]
                    zst[e, p, :, cols] = zr[e * cap:(e + 1) * cap]
        two = pl.ds(b0, 2)
        for e in range(2):
            ab = dot_nn(xst[e].reshape(2 * cap, dim), w13[e]).astype(BF16)
            grad_hidden = dot_nt(zst[e].reshape(2 * cap, dim), w2[e])
            hidden, grad_gate, grad_up = swiglu_parts(ab[:, :ff], ab[:, ff:], grad_hidden)
            hst[e] = hidden.reshape(2, cap, ff)
            act[e, two, :, :ff] = grad_gate.reshape(2, cap, ff)
            act[e, two, :, ff:] = grad_up.reshape(2, cap, ff)
        flush(t, True)

    for cp in shared_load:
        cp.wait()
    ab = dot_nn(xbuf[me], w13[1]).astype(BF16)
    hidden, grad_gate, grad_up = swiglu_parts(ab[:, :ff], ab[:, ff:], dot_nt(dybuf[me], w2[1]))
    shid[...] = hidden
    sact[:, :ff] = grad_gate
    sact[:, ff:] = grad_up
    for n in range(dim // tile):
        cols = slice(n * tile, (n + 1) * tile)
        sdx[:, cols] = dot_nt(sact[...], w13[1, cols, :])
    shared_out = [pltpu.make_async_copy(sact, sact_out, load_sem.at[0]), pltpu.make_async_copy(shid, shid_out, load_sem.at[1])]
    for cp in shared_out + second_load:
        cp.start()
    for cp in first_load + second_load:
        cp.wait()
    def give(j):
        return remote(dsend.at[lax.rem(j, 2)], pbuf.at[lax.rem(j, 2)], ds_sem.at[lax.rem(j, 2)], dr_sem.at[lax.rem(j, 2)], partner)

    def part(h):
        return pl.ds(h * half, half)

    def rs_y(j, zb, h):
        return remote(sums.at[j, :, part(h)], ybuf.at[zb, :, part(h)], ys_sem.at[zb, h], yr_sem.at[zb, h], side)

    def rs_end(j, end):
        return remote(sums.at[j, :, part(0)], ebuf.at[end], es_sem.at[end], er_sem.at[end], me + 8 * end - 4)

    def rs_compute(j):
        zb, yb, _ = visit(j)
        b = bid(zb, yb, c)
        bp = bid(zb, yb, 1 - c)

        @pl.when(j >= 2)
        def _():
            give(j).wait_send()

        @pl.loop(0, dim // tile)
        def _(n):
            cols = pl.ds(pl.multiple_of(n * tile, tile), tile)
            r = [dot_nt(jnp.concatenate([act[e, b], act[e, bp]], axis=0), w13[e, cols, :]).astype(BF16) for e in range(2)]
            sums[j, :, cols] = dot_tn(pick[b], jnp.concatenate([r[0][:cap], r[1][:cap]], axis=0))
            dsend[lax.rem(j, 2), :, cols] = dot_tn(pick[bp], jnp.concatenate([r[0][cap:], r[1][cap:]], axis=0))

        @pl.when(j >= 2)
        def _():
            pl.semaphore_wait(credit, 1)
        give(j).start()

    def rs_finish(j):
        give(j).wait_recv()
        sums[j] = sums[j] + pbuf[j % 2]
        if j < 6:
            pl.semaphore_signal(credit, inc=1, device_id={'ep': partner}, device_id_type=pl.DeviceIdType.MESH)

    def end_in(j, end):
        rs_end(j, end).wait_recv()
        sums[j, :, part(0)] = sums[j, :, part(0)] + ebuf[end]

    def chain(k, h, zb, up):
        j = own_slot[k]
        slot, gap = (0, zb - z - 1) if up else (1, z - zb - 1)
        return remote(sums.at[j, :, part(h)], cbuf.at[slot, gap, :, part(h)], cs_sem.at[k, h], cr_sem.at[slot, gap, h], me + (4 if up else -4))

    def chain_in(j, h, slot, gap):
        remote(sums.at[j, :, part(h)], cbuf.at[slot, gap, :, part(h)], cs_sem.at[0, h], cr_sem.at[slot, gap, h], partner).wait_recv()
        sums[j, :, part(h)] = sums[j, :, part(h)] + cbuf[slot, gap, :, part(h)]

    def y_in(j, zb, h):
        rs_y(0, zb, h).wait_recv()
        sums[j, :, part(h)] = sums[j, :, part(h)] + ybuf[zb, :, part(h)]

    def step(k, h, mid):
        zb = order(k)
        j = own_slot[k]
        if h or k == 2 or (k == 1 and not mid):
            y_in(j, zb, h)

        @pl.when(zb > z)
        def _():
            if mid:
                chain_in(j, h, 0, zb - z)
            chain(k, h, zb, True).start()

        @pl.when(zb < z)
        def _():
            if mid:
                chain_in(j, h, 1, z - zb)
            chain(k, h, zb, False).start()

    def act_on(token, mid):
        kind, k, h = token[0], int(token[1]), int(token[2])
        if kind == 'F':
            pass_on(k, h)
        elif kind == 'X':
            rs_finish(k)
        elif kind == 'Y':
            rs_y(other_slot[k], order(k), h).start()
        elif kind == 'S':
            step(k, h, mid)
        elif kind == 'E':
            if mid:
                end_in(other_slot[3], far_end)
            rs_end(other_slot[3], far_end).start()
        elif mid:
            end_in(other_slot[1], near_end)
            rs_end(other_slot[1], near_end).start()
        else:
            end_in(other_slot[0], near_end)
            rs_y(other_slot[0], z, 0).start()

    plans = [gaps(''.join(rows)) for rows in (END_PLAN, MID_PLAN)]

    def between(t, gap):
        for mid in range(2):
            tokens = plans[mid][gap]
            if tokens:
                @pl.when((t == gap // 2) & ((inner > 0) if mid else (inner == 0)))
                def _():
                    for token in tokens:
                        act_on(token, mid)

    @pl.loop(0, 8)
    def _(t):
        for g in range(8):
            between(t, 2 * g)
        compute(t)
        for g in range(8):
            between(t, 2 * g + 1)
        rs_compute(t)

    between(8, 16)
    flush(7, False)
    for h in (1, 0):
        @pl.when(z > 0)
        def _():
            chain_in(0, h, 0, 0)

        @pl.when(z < 3)
        def _():
            chain_in(0, h, 1, 0)
        rs_y(0, z, h).wait_recv()
        total = sums[0, :, part(h)] + ybuf[z, :, part(h)] + sdx[:, part(h)]
        xst[0, :, :, part(h)] = total.astype(BF16).reshape(2, cap, half)
    result = pltpu.make_async_copy(xst.at[0], grad_x, load_sem.at[2])
    result.start()

    for cp in shared_out:
        cp.wait()
    for t in range(8):
        pltpu.make_async_copy(act.at[:, pl.ds(0, 2)], act_all.at[:, pl.ds(0, 2)], out_sem.at[3, t]).wait()
    for zb in range(4):
        for q in range(2):
            if q or zb in (1, 2):
                send_y(q, zb, 0).wait_send()
            else:
                @pl.when(z == zb)
                def _():
                    send_y(q, zb, 0).wait_send()
            for yb in range(2):
                send_d(q, zb, yb, 0).wait_send()

            @pl.when(((zb > z) & (z > 0)) | ((zb < z) & (z < 3)))
            def _():
                send_fwd(q, zb, 0, 1).wait_send()
        for h in range(2):
            if h or zb in (1, 2):
                rs_y(0, zb, h).wait_send()
            else:
                @pl.when(z == zb)
                def _():
                    rs_y(0, zb, h).wait_send()
            if zb:
                remote(sums.at[0, :, part(h)], cbuf.at[0, 0, :, part(h)], cs_sem.at[zb, h], cr_sem.at[0, 0, h], partner).wait_send()

    @pl.when(z < 3)
    def _():
        send_end(0, 1).wait_send()
        for q in range(2):
            send_own(q, 1).wait_send()

    @pl.when(z > 0)
    def _():
        send_end(0, 0).wait_send()
        for q in range(2):
            send_own(q, 0).wait_send()
    rs_end(0, far_end).wait_send()

    @pl.when(inner > 0)
    def _():
        rs_end(0, near_end).wait_send()

    @pl.loop(1, 16)
    def _(d):
        send_table(d).wait_send()
    for j in range(2):
        give(j).wait_send()
    result.wait()


def routed(x_tokens, dy_tokens, ids, gates, slots, w_gate, w_up, w_down, s_gate, s_up, s_down):
    tok, dim = x_tokens.shape
    ff = w_gate.shape[2]
    cap = tok // 2
    dma = pltpu.SemaphoreType.DMA
    shape = jax.ShapeDtypeStruct
    return pl.pallas_call(
        routed_kernel,
        name='routed',
        out_shape=(shape((2, cap, dim), BF16), shape((2, 16, cap, dim), BF16), shape((2, 16, cap, dim), BF16),
                   shape((2, 16, cap, 2 * ff), BF16), shape((2, 16, cap, ff), BF16), shape((tok, 2 * ff), BF16), shape((tok, ff), BF16)),
        in_specs=[ANY] * 11,
        out_specs=(ANY,) * 7,
        scratch_shapes=[
            pltpu.VMEM((16, tok, dim), BF16), pltpu.VMEM((16, tok, dim), BF16)] + [pltpu.VMEM(a.shape, a.dtype) for a in (ids, gates, slots)] + [
            pltpu.VMEM((16, 8, tok), F32), pltpu.VMEM((16, 8, tok), F32), pltpu.VMEM((16, 2 * cap, tok), BF16),
            pltpu.VMEM((2, dim, 2 * ff), BF16), pltpu.VMEM((2, ff, dim), BF16),
            pltpu.VMEM((2, 16, cap, 2 * ff), BF16), pltpu.VMEM((2, 2, cap, ff), BF16), pltpu.VMEM((2, 2, cap, dim), BF16), pltpu.VMEM((2, 2, cap, dim), BF16),
            pltpu.VMEM((tok, 2 * ff), BF16), pltpu.VMEM((tok, ff), BF16), pltpu.VMEM((tok, dim), F32),
            pltpu.VMEM((8, tok, dim), F32), pltpu.VMEM((2, tok, dim), F32), pltpu.VMEM((2, tok, dim), F32),
            pltpu.VMEM((4, tok, dim), F32), pltpu.VMEM((2, 3, tok, dim), F32), pltpu.VMEM((2, tok, dim // 2), F32),
            dma((11,)), dma((4, 8)), dma((16,)), dma((16,)), dma((2, 16)), dma((2, 4)), dma((2, 8)), dma((2, 2)), dma((2, 4)), dma((2,)),
            dma((2,)), dma((2,)), dma((4, 2)), dma((4, 2)), dma((4, 2)), dma((2, 3, 2)), dma((2,)), dma((2,)), pltpu.SemaphoreType.REGULAR,
        ],
        compiler_params=pltpu.CompilerParams(collective_id=0, has_side_effects=True, vmem_limit_bytes=VMEM_LIMIT),
        cost_estimate=pl.CostEstimate(flops=16 * tok * 2 * dim * ff * 5, bytes_accessed=80_000_000, transcendentals=0),
    )(x_tokens, dy_tokens, ids, gates, slots, w_gate, w_up, w_down, s_gate, s_up, s_down)


def grads_kernel(x_in, dy_in, sact_in, shid_in, xr_in, zr_in, act_in, hid_in,
                 s1, s3, s2, g1, g3, g2,
                 x, dy, sact, shid, xr, zr, act, hid, ring, load_sem, tile_sem, ring_sem):
    dim, ff = x.shape[1], shid.shape[1]
    tile = ff
    count = dim // tile
    small = [pltpu.make_async_copy(a, b, load_sem.at[i]) for i, (a, b) in enumerate(((x_in, x), (sact_in, sact), (shid_in, shid), (dy_in, dy)))]

    def part(i):
        return pl.ds(pl.multiple_of(i * tile, tile), tile)

    def whole(e):
        return [pltpu.make_async_copy(a.at[e], b.at[e], load_sem.at[2 * e + 4 + i]) for i, (a, b) in enumerate(((act_in, act), (hid_in, hid)))]

    def tiles(e, i):
        return [pltpu.make_async_copy(a.at[e, :, part(i)], b.at[e, :, part(i)], tile_sem.at[n, e, i]) for n, (a, b) in enumerate(((xr_in, xr), (zr_in, zr)))]

    first = whole(0) + tiles(0, 0)
    for cp in first + small:
        cp.start()
    for i in range(1, count):
        for cp in tiles(0, i):
            cp.start()
    depth = ring.shape[0] - 2

    def drain(slot):
        for i in range(3):
            pltpu.make_async_copy(ring.at[slot, i], g1.at[0, pl.ds(0, ff), :], ring_sem.at[slot, i]).wait()

    def emit(slot, again, rows, acts, hids, dzs, outs):
        @pl.when(again)
        def _():
            drain(slot)
        both = dot_tn(rows, acts)
        ring[slot, 0] = both[:, :ff]
        ring[slot, 1] = both[:, ff:]
        ring[slot, 2] = dot_tn(hids, dzs)
        for i in range(3):
            pltpu.make_async_copy(ring.at[slot, i], outs[i], ring_sem.at[slot, i]).start()

    @pl.loop(0, 2 * count)
    def _(j):
        e = lax.div(j, count)
        i = lax.rem(j, count)

        @pl.when(i == 0)
        def _():
            for cp in whole(e):
                cp.wait()
        for cp in tiles(e, i):
            cp.wait()
        emit(lax.rem(j, depth), j >= depth, xr[e, :, part(i)], act[e], hid[e], zr[e, :, part(i)], (g1.at[e, part(i), :], g3.at[e, part(i), :], g2.at[e, :, part(i)]))

        @pl.when(j == 0)
        def _():
            for cp in small:
                cp.wait()
            for cp in whole(1):
                cp.start()
            for n in range(count):
                for cp in tiles(1, n):
                    cp.start()

        @pl.when(lax.rem(j, 2) == 0)
        def _():
            k = lax.div(j, 2)
            emit(depth + lax.rem(k, 2), k >= 2, x[:, part(k)], sact[...], shid[...], dy[:, part(k)], (s1.at[0, part(k), :], s3.at[0, part(k), :], s2.at[0, :, part(k)]))
    for slot in range(depth + 2):
        drain(slot)


def weight_grads(x, dy, sact, shid, xr, zr, act, hid):
    dim, ff = x.shape[1], shid.shape[1]
    tile = ff
    shape = jax.ShapeDtypeStruct
    ins = (x, dy, sact, shid, xr, zr, act, hid)
    slots = min(6, 2 + 2 * dim // tile)
    dma = pltpu.SemaphoreType.DMA
    return pl.pallas_call(
        grads_kernel,
        name='weight_grads',
        out_shape=tuple(shape((n,) + d, F32) for n in (1, 2) for d in ((dim, ff), (dim, ff), (ff, dim))),
        in_specs=[ANY] * 8,
        out_specs=(ANY,) * 6,
        scratch_shapes=[pltpu.VMEM(a.shape, a.dtype) for a in ins] + [pltpu.VMEM((slots, 3, tile, ff), F32), dma((8,)), dma((2, 2, dim // tile)), dma((slots, 3))],
        compiler_params=pltpu.CompilerParams(vmem_limit_bytes=60_000_000),
        cost_estimate=pl.CostEstimate(flops=6 * dim * ff * (x.shape[0] + 2 * xr.shape[1]), bytes_accessed=2 * sum(a.size for a in ins) + 36 * dim * ff, transcendentals=0),
    )(*ins)


def solution(mesh):
    group = mesh.shape['ep']
    token_spec = P(('dp', 'ep'), None)
    expert_spec = P('ep', None, None)
    whole_spec = P(None, None)
    grad_spec = P(('dp', 'ep'), None, None)

    def local_backward(x_tokens, dy_tokens, expert_ids, gate_vals, slot_pos, w_gate, w_up, w_down, shared_gate, shared_up, shared_down):
        tok, dim = x_tokens.shape
        local_experts = w_gate.shape[0]
        grad_x, x_all, z_all, act_all, hid_all, sact, shid = routed(x_tokens, dy_tokens, expert_ids.T, gate_vals.T, slot_pos.T, w_gate, w_up, w_down, shared_gate, shared_up, shared_down)
        x_all, z_all, act_all, hid_all = [a.reshape(local_experts, -1, a.shape[-1]) for a in (x_all, z_all, act_all, hid_all)]
        grad_shared_gate, grad_shared_up, grad_shared_down, grad_w_gate, grad_w_up, grad_w_down = weight_grads(x_tokens, dy_tokens, sact, shid, x_all, z_all, act_all, hid_all)
        grad_x = grad_x.reshape(tok, dim)
        return grad_x, grad_w_gate, grad_w_up, grad_w_down, grad_shared_gate, grad_shared_up, grad_shared_down

    return jax.shard_map(local_backward, mesh=mesh, in_specs=(token_spec, token_spec, token_spec, token_spec, token_spec, expert_spec, expert_spec, expert_spec, whole_spec, whole_spec, whole_spec), out_specs=(token_spec, grad_spec, grad_spec, grad_spec, grad_spec, grad_spec, grad_spec), check_vma=False)
```

```python
import functools

import jax
import jax.numpy as jnp
from jax import lax
from jax.experimental import pallas as pl
from jax.experimental.pallas import tpu as pltpu
from jax.sharding import PartitionSpec as P

F32 = jnp.float32
BF16 = jnp.bfloat16
ANY = pl.BlockSpec(memory_space=pl.ANY)
VMEM = pl.BlockSpec(memory_space=pltpu.VMEM)
VMEM_LIMIT = 67_000_000


def dot_nn(a, b):
    return lax.dot_general(a, b, (((1,), (0,)), ((), ())), preferred_element_type=F32)


def dot_nt(a, b):
    return lax.dot_general(a, b, (((1,), (1,)), ((), ())), preferred_element_type=F32)


def dot_tn(a, b):
    return lax.dot_general(a, b, (((0,), (0,)), ((), ())), preferred_element_type=F32)


def swiglu_parts(act_gate, act_up, grad_hidden):
    gate_f32 = act_gate.astype(F32)
    up_f32 = act_up.astype(F32)
    sigma = jax.nn.sigmoid(gate_f32)
    silu_gate = gate_f32 * sigma
    hidden = (silu_gate * up_f32).astype(BF16)
    grad_gate = (grad_hidden * up_f32 * sigma * (1.0 + gate_f32 * (1.0 - sigma))).astype(BF16)
    grad_up = (grad_hidden * silu_gate).astype(BF16)
    return hidden, grad_gate, grad_up


END_PLAN = (
    'C00F20F10F11R00X00F21C10R10C20F40X10F30F31R20F41C30R30C40F60',
    'X20X30R40F50F51F61X40C50Y01R50C60X50F70F71S30R60C70R70X60Y20',
    'X70E00Y31Y21Y11Y10S20S31S21S11N00S10',
)
MID_PLAN = (
    'C00F20F10R00F30F11C10F31F50X00F21R10C20F60X10F51F40R20C30R30',
    'F41X20C40R40Y00X30F70C50F61R50X40Y11Y01X50F71C60R60C70R70X60',
    'X70Y20S30Y31E00S10S20N00Y21S31S21S11',
)


def gaps(text):
    found = [[]]
    for i in range(0, len(text), 3):
        token = text[i:i + 3]
        if token[0] in 'CR':
            found.append([])
        else:
            found[-1].append(token)
    return found


def routed_kernel(x_in, dy_in, ids_in, gates_in, slots_in, w_gate, w_up, w_down, s_gate, s_up, s_down,
                  grad_x, x_all, z_all, act_all, hid_all, sact_out, shid_out,
                  xbuf, dybuf, ids, gates, slots, tbuf, table, pick, w13, w2, act, hst, xst, zst, sact, shid, sdx,
                  sums, dsend, pbuf, ybuf, cbuf, ebuf,
                  load_sem, out_sem, gs_sem, gr_sem, recv_sem, sy_sem, sd_sem, sown_sem, sz_sem, sx_sem,
                  ds_sem, dr_sem, ys_sem, yr_sem, cs_sem, cr_sem, es_sem, er_sem, credit):
    tok, dim = x_in.shape
    ff = w2.shape[1]
    cap = xst.shape[2]
    half = dim // 2
    tile = min(512, dim)
    me = lax.axis_index('ep')
    z = lax.div(me, 4)
    y = lax.rem(lax.div(me, 2), 2)
    c = lax.rem(me, 2)
    partner = me + 1 - 2 * c
    side = me + 2 - 4 * y
    inner = z * (3 - z)
    near_end = lax.div(z, 2)
    far_end = 1 - near_end
    bufs = (xbuf, dybuf)
    own_slot = (0, 1, 3, 5)
    other_slot = (2, 4, 6, 7)
    near_first = [(own_slot.index(t), 0) if t in own_slot else (other_slot.index(t), 1) for t in range(8)]

    def bid(zz, yy, cc):
        return zz * 4 + yy * 2 + cc

    def order(k):
        near = lax.div(inner, 2)
        delta = lax.div((1 - k) * (2 - k) * (3 - k), 6) - lax.div(k * (2 - k) * (3 - k), 2)
        base = k + near * delta
        return base + near_end * (3 - 2 * base)

    def visit(t):
        u = t + lax.div(t, 7)
        odd = lax.rem(u, 2)
        first = lax.div(7 - t, 7)
        k = odd * lax.div(u + 1, 2) + (1 - odd) * (lax.div(u, 2) - 1) + first
        col = 1 - odd - first
        return order(k), y + col * (1 - 2 * y), col

    def remote(src, dst, send, recv, dev):
        return pltpu.make_async_remote_copy(src_ref=src, dst_ref=dst, send_sem=send, recv_sem=recv, device_id={'ep': dev}, device_id_type=pl.DeviceIdType.MESH)

    def weights(e, gate, up, down):
        return [pltpu.make_async_copy(gate, w13.at[e, :, pl.ds(0, ff)], load_sem.at[2 + 3 * e]),
                pltpu.make_async_copy(up, w13.at[e, :, pl.ds(ff, ff)], load_sem.at[3 + 3 * e]),
                pltpu.make_async_copy(down, w2.at[e], load_sem.at[4 + 3 * e])]

    own = [pltpu.make_async_copy(x_in, xbuf.at[me], load_sem.at[0]), pltpu.make_async_copy(dy_in, dybuf.at[me], load_sem.at[1])]
    shared_load = weights(1, s_gate, s_up, s_down)
    first_load = weights(0, w_gate.at[0], w_up.at[0], w_down.at[0])
    second_load = weights(1, w_gate.at[1], w_up.at[1], w_down.at[1])
    routing = [pltpu.make_async_copy(a, b, load_sem.at[8 + i]) for i, (a, b) in enumerate(((ids_in, ids), (gates_in, gates), (slots_in, slots)))]
    for cp in own + routing + shared_load + first_load:
        cp.start()

    barrier = pltpu.get_barrier_semaphore()

    @pl.loop(1, 16)
    def _(d):
        pl.semaphore_signal(barrier, inc=1, device_id={'ep': lax.rem(me + d, 16)}, device_id_type=pl.DeviceIdType.MESH)
    pl.semaphore_wait(barrier, 15)

    def send_y(q, zb, b):
        return remote(bufs[q].at[b], bufs[q].at[b], sy_sem.at[q, zb], recv_sem.at[q, b], side)

    def send_d(q, zb, yb, b):
        return remote(bufs[q].at[b], bufs[q].at[b], sd_sem.at[q, zb * 2 + yb], recv_sem.at[q, b], partner)

    def send_own(q, up):
        return remote(bufs[q].at[me], bufs[q].at[me], sown_sem.at[q, up], recv_sem.at[q, me], me + (4 if up else -4))

    def send_fwd(q, zb, b, up):
        return remote(bufs[q].at[b], bufs[q].at[b], sz_sem.at[q, zb], recv_sem.at[q, b], me + (4 if up else -4))

    def send_end(b, up):
        return remote(xbuf.at[b], xbuf.at[b], sx_sem.at[1 - up], recv_sem.at[0, b], me + (4 if up else -4))

    for q in range(2):
        own[q].wait()
        send_y(q, z, me).start()

        @pl.when(z < 3)
        def _():
            send_own(q, 1).start()

        @pl.when(z > 0)
        def _():
            send_own(q, 0).start()
        send_d(q, z, y, me).start()

    for cp in routing:
        cp.wait()
    kept = jnp.where(slots[...] >= 0, ids[...], -1)
    slot_f32 = slots[...].astype(F32) + 1.0
    for dev in range(16):
        hits = [kept == 2 * dev + e for e in range(2)]
        rows = [jnp.sum(jnp.where(hit, gates[...], 0.0), axis=0, keepdims=True) for hit in hits]
        rows += [jnp.sum(jnp.where(hit, slot_f32, 0.0), axis=0, keepdims=True) - 1.0 for hit in hits]
        table[dev] = jnp.concatenate(rows + [jnp.zeros((4, tok), F32)], axis=0)

    def send_table(d):
        dest = lax.rem(me + d, 16)
        return remote(table.at[dest], tbuf.at[me], gs_sem.at[d], gr_sem.at[me], dest)

    @pl.loop(1, 16)
    def _(d):
        send_table(d).start()
    tbuf[me] = table[me]

    def place(t):
        k, col = near_first[t]
        return order(k), y + col * (1 - 2 * y), col

    def pass_on(t, q):
        zb, yb, col = place(t)
        b = bid(zb, yb, c)
        send_d(q, zb, yb, b).wait_recv()
        if col == 0:
            if q:
                send_y(q, zb, b).start()
            else:
                @pl.when(zb * (3 - zb) > 0)
                def _():
                    send_y(q, zb, b).start()

            @pl.when((zb > z) & (z > 0))
            def _():
                send_fwd(q, zb, b, 0).start()

            @pl.when((zb < z) & (z < 3))
            def _():
                send_fwd(q, zb, b, 1).start()
        elif q == 0:
            @pl.when((zb == 3) & (z > 0))
            def _():
                send_end(b, 0).start()

            @pl.when((zb == 0) & (z < 3))
            def _():
                send_end(b, 1).start()
        send_d(q, zb, yb, b).start()

    def flush(t, start):
        zb, yb, _ = visit(t)
        two = pl.ds(bid(zb, yb, 0), 2)
        cps = [pltpu.make_async_copy(xst, x_all.at[:, two], out_sem.at[0, t]),
               pltpu.make_async_copy(zst, z_all.at[:, two], out_sem.at[1, t]),
               pltpu.make_async_copy(hst, hid_all.at[:, two], out_sem.at[2, t]),
               pltpu.make_async_copy(act.at[:, two], act_all.at[:, two], out_sem.at[3, t])]
        if start:
            for cp in cps:
                cp.start()
        else:
            for cp in cps[:3]:
                cp.wait()

    def compute(t):
        zb, yb, _ = visit(t)
        b0 = bid(zb, yb, 0)
        bp = bid(zb, yb, 1 - c)
        for q in range(2):
            send_d(q, zb, yb, bp).wait_recv()
        for p in range(2):
            @pl.when(b0 + p != me)
            def _():
                remote(table.at[0], tbuf.at[b0 + p], gs_sem.at[0], gr_sem.at[b0 + p], partner).wait_recv()

        @pl.when(t > 0)
        def _():
            flush(t - 1, False)
        row = lax.broadcasted_iota(jnp.int32, (2 * cap, tok), 0).astype(F32)
        for p in range(2):
            info = tbuf[b0 + p]
            top = row < cap
            chosen = jnp.where(top, info[2:3, :], info[3:4, :] + cap) == row
            gate = jnp.sum(jnp.where(chosen, jnp.where(top, info[0:1, :], info[1:2, :]), 0.0), axis=1, keepdims=True)
            sel = chosen.astype(BF16)
            pick[b0 + p] = sel
            for n in range(dim // tile):
                cols = slice(n * tile, (n + 1) * tile)
                xr = dot_nn(sel, xbuf[b0 + p, :, cols]).astype(BF16)
                zr = (dot_nn(sel, dybuf[b0 + p, :, cols]) * gate).astype(BF16)
                for e in range(2):
                    xst[e, p, :, cols] = xr[e * cap:(e + 1) * cap]
                    zst[e, p, :, cols] = zr[e * cap:(e + 1) * cap]
        two = pl.ds(b0, 2)
        for e in range(2):
            ab = dot_nn(xst[e].reshape(2 * cap, dim), w13[e]).astype(BF16)
            grad_hidden = dot_nt(zst[e].reshape(2 * cap, dim), w2[e])
            hidden, grad_gate, grad_up = swiglu_parts(ab[:, :ff], ab[:, ff:], grad_hidden)
            hst[e] = hidden.reshape(2, cap, ff)
            act[e, two, :, :ff] = grad_gate.reshape(2, cap, ff)
            act[e, two, :, ff:] = grad_up.reshape(2, cap, ff)
        flush(t, True)

    for cp in shared_load:
        cp.wait()
    ab = dot_nn(xbuf[me], w13[1]).astype(BF16)
    hidden, grad_gate, grad_up = swiglu_parts(ab[:, :ff], ab[:, ff:], dot_nt(dybuf[me], w2[1]))
    shid[...] = hidden
    sact[:, :ff] = grad_gate
    sact[:, ff:] = grad_up
    for n in range(dim // tile):
        cols = slice(n * tile, (n + 1) * tile)
        sdx[:, cols] = dot_nt(sact[...], w13[1, cols, :])
    shared_out = [pltpu.make_async_copy(sact, sact_out, load_sem.at[0]), pltpu.make_async_copy(shid, shid_out, load_sem.at[1])]
    for cp in shared_out + second_load:
        cp.start()
    for cp in first_load + second_load:
        cp.wait()
    def give(j):
        return remote(dsend.at[lax.rem(j, 2)], pbuf.at[lax.rem(j, 2)], ds_sem.at[lax.rem(j, 2)], dr_sem.at[lax.rem(j, 2)], partner)

    def part(h):
        return pl.ds(h * half, half)

    def rs_y(j, zb, h):
        return remote(sums.at[j, :, part(h)], ybuf.at[zb, :, part(h)], ys_sem.at[zb, h], yr_sem.at[zb, h], side)

    def rs_end(j, end):
        return remote(sums.at[j, :, part(0)], ebuf.at[end], es_sem.at[end], er_sem.at[end], me + 8 * end - 4)

    def rs_compute(j):
        zb, yb, _ = visit(j)
        b = bid(zb, yb, c)
        bp = bid(zb, yb, 1 - c)

        @pl.when(j >= 2)
        def _():
            give(j).wait_send()

        @pl.loop(0, dim // tile)
        def _(n):
            cols = pl.ds(pl.multiple_of(n * tile, tile), tile)
            r = [dot_nt(jnp.concatenate([act[e, b], act[e, bp]], axis=0), w13[e, cols, :]).astype(BF16) for e in range(2)]
            sums[j, :, cols] = dot_tn(pick[b], jnp.concatenate([r[0][:cap], r[1][:cap]], axis=0))
            dsend[lax.rem(j, 2), :, cols] = dot_tn(pick[bp], jnp.concatenate([r[0][cap:], r[1][cap:]], axis=0))

        @pl.when(j >= 2)
        def _():
            pl.semaphore_wait(credit, 1)
        give(j).start()

    def rs_finish(j):
        give(j).wait_recv()
        sums[j] = sums[j] + pbuf[j % 2]
        if j < 6:
            pl.semaphore_signal(credit, inc=1, device_id={'ep': partner}, device_id_type=pl.DeviceIdType.MESH)

    def end_in(j, end):
        rs_end(j, end).wait_recv()
        sums[j, :, part(0)] = sums[j, :, part(0)] + ebuf[end]

    def chain(k, h, zb, up):
        j = own_slot[k]
        slot, gap = (0, zb - z - 1) if up else (1, z - zb - 1)
        return remote(sums.at[j, :, part(h)], cbuf.at[slot, gap, :, part(h)], cs_sem.at[k, h], cr_sem.at[slot, gap, h], me + (4 if up else -4))

    def chain_in(j, h, slot, gap):
        remote(sums.at[j, :, part(h)], cbuf.at[slot, gap, :, part(h)], cs_sem.at[0, h], cr_sem.at[slot, gap, h], partner).wait_recv()
        sums[j, :, part(h)] = sums[j, :, part(h)] + cbuf[slot, gap, :, part(h)]

    def y_in(j, zb, h):
        rs_y(0, zb, h).wait_recv()
        sums[j, :, part(h)] = sums[j, :, part(h)] + ybuf[zb, :, part(h)]

    def step(k, h, mid):
        zb = order(k)
        j = own_slot[k]
        if h or k == 2 or (k == 1 and not mid):
            y_in(j, zb, h)

        @pl.when(zb > z)
        def _():
            if mid:
                chain_in(j, h, 0, zb - z)
            chain(k, h, zb, True).start()

        @pl.when(zb < z)
        def _():
            if mid:
                chain_in(j, h, 1, z - zb)
            chain(k, h, zb, False).start()

    def act_on(token, mid):
        kind, k, h = token[0], int(token[1]), int(token[2])
        if kind == 'F':
            pass_on(k, h)
        elif kind == 'X':
            rs_finish(k)
        elif kind == 'Y':
            rs_y(other_slot[k], order(k), h).start()
        elif kind == 'S':
            step(k, h, mid)
        elif kind == 'E':
            if mid:
                end_in(other_slot[3], far_end)
            rs_end(other_slot[3], far_end).start()
        elif mid:
            end_in(other_slot[1], near_end)
            rs_end(other_slot[1], near_end).start()
        else:
            end_in(other_slot[0], near_end)
            rs_y(other_slot[0], z, 0).start()

    plans = [gaps(''.join(rows)) for rows in (END_PLAN, MID_PLAN)]

    def between(t, gap):
        for mid in range(2):
            tokens = plans[mid][gap]
            if tokens:
                @pl.when((t == gap // 2) & ((inner > 0) if mid else (inner == 0)))
                def _():
                    for token in tokens:
                        act_on(token, mid)

    @pl.loop(0, 8)
    def _(t):
        for g in range(8):
            between(t, 2 * g)
        compute(t)
        for g in range(8):
            between(t, 2 * g + 1)
        rs_compute(t)

    between(8, 16)
    flush(7, False)
    for h in (1, 0):
        @pl.when(z > 0)
        def _():
            chain_in(0, h, 0, 0)

        @pl.when(z < 3)
        def _():
            chain_in(0, h, 1, 0)
        rs_y(0, z, h).wait_recv()
        total = sums[0, :, part(h)] + ybuf[z, :, part(h)] + sdx[:, part(h)]
        xst[0, :, :, part(h)] = total.astype(BF16).reshape(2, cap, half)
    result = pltpu.make_async_copy(xst.at[0], grad_x, load_sem.at[2])
    result.start()

    for cp in shared_out:
        cp.wait()
    for t in range(8):
        pltpu.make_async_copy(act.at[:, pl.ds(0, 2)], act_all.at[:, pl.ds(0, 2)], out_sem.at[3, t]).wait()
    for zb in range(4):
        for q in range(2):
            if q or zb in (1, 2):
                send_y(q, zb, 0).wait_send()
            else:
                @pl.when(z == zb)
                def _():
                    send_y(q, zb, 0).wait_send()
            for yb in range(2):
                send_d(q, zb, yb, 0).wait_send()

            @pl.when(((zb > z) & (z > 0)) | ((zb < z) & (z < 3)))
            def _():
                send_fwd(q, zb, 0, 1).wait_send()
        for h in range(2):
            if h or zb in (1, 2):
                rs_y(0, zb, h).wait_send()
            else:
                @pl.when(z == zb)
                def _():
                    rs_y(0, zb, h).wait_send()
            if zb:
                remote(sums.at[0, :, part(h)], cbuf.at[0, 0, :, part(h)], cs_sem.at[zb, h], cr_sem.at[0, 0, h], partner).wait_send()

    @pl.when(z < 3)
    def _():
        send_end(0, 1).wait_send()
        for q in range(2):
            send_own(q, 1).wait_send()

    @pl.when(z > 0)
    def _():
        send_end(0, 0).wait_send()
        for q in range(2):
            send_own(q, 0).wait_send()
    rs_end(0, far_end).wait_send()

    @pl.when(inner > 0)
    def _():
        rs_end(0, near_end).wait_send()

    @pl.loop(1, 16)
    def _(d):
        send_table(d).wait_send()
    for j in range(2):
        give(j).wait_send()
    result.wait()


def routed(x_tokens, dy_tokens, ids, gates, slots, w_gate, w_up, w_down, s_gate, s_up, s_down):
    tok, dim = x_tokens.shape
    ff = w_gate.shape[2]
    cap = tok // 2
    dma = pltpu.SemaphoreType.DMA
    shape = jax.ShapeDtypeStruct
    return pl.pallas_call(
        routed_kernel,
        name='routed',
        out_shape=(shape((2, cap, dim), BF16), shape((2, 16, cap, dim), BF16), shape((2, 16, cap, dim), BF16),
                   shape((2, 16, cap, 2 * ff), BF16), shape((2, 16, cap, ff), BF16), shape((tok, 2 * ff), BF16), shape((tok, ff), BF16)),
        in_specs=[ANY] * 11,
        out_specs=(ANY,) * 7,
        scratch_shapes=[
            pltpu.VMEM((16, tok, dim), BF16), pltpu.VMEM((16, tok, dim), BF16)] + [pltpu.VMEM(a.shape, a.dtype) for a in (ids, gates, slots)] + [
            pltpu.VMEM((16, 8, tok), F32), pltpu.VMEM((16, 8, tok), F32), pltpu.VMEM((16, 2 * cap, tok), BF16),
            pltpu.VMEM((2, dim, 2 * ff), BF16), pltpu.VMEM((2, ff, dim), BF16),
            pltpu.VMEM((2, 16, cap, 2 * ff), BF16), pltpu.VMEM((2, 2, cap, ff), BF16), pltpu.VMEM((2, 2, cap, dim), BF16), pltpu.VMEM((2, 2, cap, dim), BF16),
            pltpu.VMEM((tok, 2 * ff), BF16), pltpu.VMEM((tok, ff), BF16), pltpu.VMEM((tok, dim), F32),
            pltpu.VMEM((8, tok, dim), F32), pltpu.VMEM((2, tok, dim), F32), pltpu.VMEM((2, tok, dim), F32),
            pltpu.VMEM((4, tok, dim), F32), pltpu.VMEM((2, 3, tok, dim), F32), pltpu.VMEM((2, tok, dim // 2), F32),
            dma((11,)), dma((4, 8)), dma((16,)), dma((16,)), dma((2, 16)), dma((2, 4)), dma((2, 8)), dma((2, 2)), dma((2, 4)), dma((2,)),
            dma((2,)), dma((2,)), dma((4, 2)), dma((4, 2)), dma((4, 2)), dma((2, 3, 2)), dma((2,)), dma((2,)), pltpu.SemaphoreType.REGULAR,
        ],
        compiler_params=pltpu.CompilerParams(collective_id=0, has_side_effects=True, vmem_limit_bytes=VMEM_LIMIT),
        cost_estimate=pl.CostEstimate(flops=16 * tok * 2 * dim * ff * 5, bytes_accessed=80_000_000, transcendentals=0),
    )(x_tokens, dy_tokens, ids, gates, slots, w_gate, w_up, w_down, s_gate, s_up, s_down)


def grads_kernel(x_in, dy_in, sact_in, shid_in, xr_in, zr_in, act_in, hid_in,
                 s1, s3, s2, g1, g3, g2,
                 x, dy, sact, shid, xr, zr, act, hid, hid_t, ring, load_sem, tile_sem, ring_sem):
    dim, ff = x.shape[1], shid.shape[1]
    tile = ff
    count = dim // tile
    small = [pltpu.make_async_copy(a, b, load_sem.at[i]) for i, (a, b) in enumerate(((x_in, x), (sact_in, sact), (shid_in, shid), (dy_in, dy)))]

    def part(i):
        return pl.ds(pl.multiple_of(i * tile, tile), tile)

    def whole(e):
        return [pltpu.make_async_copy(a.at[e], b.at[e], load_sem.at[2 * e + 4 + i]) for i, (a, b) in enumerate(((act_in, act), (hid_in, hid)))]

    def tiles(e, i):
        return [pltpu.make_async_copy(a.at[e, :, part(i)], b.at[e, :, part(i)], tile_sem.at[n, e, i]) for n, (a, b) in enumerate(((xr_in, xr), (zr_in, zr)))]

    def load(e):
        for cp in whole(e):
            cp.start()
        for i in range(count):
            for cp in tiles(e, i):
                cp.start()

    for cp in small:
        cp.start()
    load(0)
    depth = ring.shape[0]

    def drain(slot):
        for i in range(3):
            pltpu.make_async_copy(ring.at[slot, i, pl.ds(0, ff), pl.ds(0, ff)], g1.at[0, pl.ds(0, ff), :], ring_sem.at[slot, i]).wait()

    def emit(job, rows, acts, down, outs):
        slot = lax.rem(job, depth)

        @pl.when(job >= depth)
        def _():
            drain(slot)
        both = dot_tn(rows, acts)
        ring[slot, 0] = both[:, :ff]
        ring[slot, 1] = both[:, ff:]
        ring[slot, 2] = down()
        for i in range(3):
            pltpu.make_async_copy(ring.at[slot, i], outs[i], ring_sem.at[slot, i]).start()

    for cp in small:
        cp.wait()

    @pl.loop(0, count)
    def _(i):
        emit(i, x[:, part(i)], sact[...], lambda: dot_tn(shid[...], dy[:, part(i)]), (s1.at[0, part(i), :], s3.at[0, part(i), :], s2.at[0, :, part(i)]))
    load(1)

    @pl.loop(0, 2 * count)
    def _(j):
        e = lax.div(j, count)
        i = lax.rem(j, count)

        @pl.when(i == 0)
        def _():
            for cp in whole(e):
                cp.wait()
            hid_t[...] = hid[e].T
        for cp in tiles(e, i):
            cp.wait()
        emit(j + count, xr[e, :, part(i)], act[e], lambda: dot_nn(hid_t[...], zr[e, :, part(i)]), (g1.at[e, part(i), :], g3.at[e, part(i), :], g2.at[e, :, part(i)]))
    for slot in range(depth):
        drain(slot)


def weight_grads(x, dy, sact, shid, xr, zr, act, hid):
    dim, ff = x.shape[1], shid.shape[1]
    tile = ff
    shape = jax.ShapeDtypeStruct
    ins = (x, dy, sact, shid, xr, zr, act, hid)
    dma = pltpu.SemaphoreType.DMA
    return pl.pallas_call(
        grads_kernel,
        name='weight_grads',
        out_shape=tuple(shape((n,) + d, F32) for n in (1, 2) for d in ((dim, ff), (dim, ff), (ff, dim))),
        in_specs=[ANY] * 8,
        out_specs=(ANY,) * 6,
        scratch_shapes=[pltpu.VMEM(a.shape, a.dtype) for a in ins] + [pltpu.VMEM((ff, hid.shape[1]), BF16), pltpu.VMEM((4, 3, tile, ff), F32), dma((8,)), dma((2, 2, dim // tile)), dma((4, 3))],
        compiler_params=pltpu.CompilerParams(vmem_limit_bytes=60_000_000),
        cost_estimate=pl.CostEstimate(flops=6 * dim * ff * (x.shape[0] + 2 * xr.shape[1]), bytes_accessed=2 * sum(a.size for a in ins) + 36 * dim * ff, transcendentals=0),
    )(*ins)


def solution(mesh):
    group = mesh.shape['ep']
    token_spec = P(('dp', 'ep'), None)
    expert_spec = P('ep', None, None)
    whole_spec = P(None, None)
    grad_spec = P(('dp', 'ep'), None, None)

    def local_backward(x_tokens, dy_tokens, expert_ids, gate_vals, slot_pos, w_gate, w_up, w_down, shared_gate, shared_up, shared_down):
        tok, dim = x_tokens.shape
        local_experts = w_gate.shape[0]
        grad_x, x_all, z_all, act_all, hid_all, sact, shid = routed(x_tokens, dy_tokens, expert_ids.T, gate_vals.T, slot_pos.T, w_gate, w_up, w_down, shared_gate, shared_up, shared_down)
        x_all, z_all, act_all, hid_all = [a.reshape(local_experts, -1, a.shape[-1]) for a in (x_all, z_all, act_all, hid_all)]
        grad_shared_gate, grad_shared_up, grad_shared_down, grad_w_gate, grad_w_up, grad_w_down = weight_grads(x_tokens, dy_tokens, sact, shid, x_all, z_all, act_all, hid_all)
        grad_x = grad_x.reshape(tok, dim)
        return grad_x, grad_w_gate, grad_w_up, grad_w_down, grad_shared_gate, grad_shared_up, grad_shared_down

    return jax.shard_map(local_backward, mesh=mesh, in_specs=(token_spec, token_spec, token_spec, token_spec, token_spec, expert_spec, expert_spec, expert_spec, whole_spec, whole_spec, whole_spec), out_specs=(token_spec, grad_spec, grad_spec, grad_spec, grad_spec, grad_spec, grad_spec), check_vma=False)
```
